512 devices in a mesh: batch: 8 (over y_lo, x), rows: 8 (over z), chan: 8 (over y_hi, core).
Axes of the slice: x: 4, y: 8 (y_hi: 4, y_lo: 2; y = y_hi * 2 + y_lo), z: 8, core: 2. Of those that a mesh axis runs over, the one named last changes fastest.
Arguments:
- images: float32 [64, 24, 64, 32], P('batch', None, ('rows', 'chan')), may hold values from -6 to 6
- shift_mid: float32 [3, 24], replicated, may hold values from -1.75 to 1.75
- gain_mid: float32 [3, 24], replicated, may hold values from -0.3 to 0.3
- lower_mid: float32 [3, 24, 24], replicated, may hold values from -1.25 to 1.25
- upper_mid: float32 [3, 24, 24], replicated, may hold values from -1.25 to 1.25
- diag_mid: float32 [3, 24], replicated, may hold values from -0.3 to 0.3
- first_mid: bfloat16 [3, 9, 12, 512], replicated, may hold values from -0.625 to 0.625
- first_bias_mid: bfloat16 [3, 512], replicated, may hold values from -3 to 3
- second_mid: bfloat16 [3, 512, 512], replicated, may hold values from -0.25 to 0.25
- second_bias_mid: float32 [3, 512], replicated, may hold values from -3 to 3
- third_mid: bfloat16 [3, 9, 512, 24], replicated, may hold values from -0.09375 to 0.09375
- third_bias_mid: float32 [3, 24], replicated, may hold values from -3 to 3
- shift_top: float32 [2, 48], replicated, may hold values from -1.75 to 1.75
- gain_top: float32 [2, 48], replicated, may hold values from -0.3 to 0.3
- lower_top: float32 [2, 48, 48], replicated, may hold values from -0.875 to 0.875
- upper_top: float32 [2, 48, 48], replicated, may hold values from -0.875 to 0.875
- diag_top: float32 [2, 48], replicated, may hold values from -0.3 to 0.3
- first_top: bfloat16 [2, 9, 24, 512], replicated, may hold values from -0.4375 to 0.4375
- first_bias_top: bfloat16 [2, 512], replicated, may hold values from -3 to 3
- second_top: bfloat16 [2, 512, 512], replicated, may hold values from -0.25 to 0.25
- second_bias_top: float32 [2, 512], replicated, may hold values from -3 to 3
- third_top: bfloat16 [2, 9, 512, 48], replicated, may hold values from -0.09375 to 0.09375
- third_bias_top: float32 [2, 48], replicated, may hold values from -3 to 3
Outputs:
- latent_mid: float32 [64, 12, 64, 32], P('batch', None, ('rows', 'chan'))
- latent_top: float32 [64, 48, 32, 16], P(('batch', 'chan'), None, 'rows')
- loglik: float32 [64], P(('batch', 'chan'))
The draws below stay inside these ranges and needn't reach their ends.
All inputs are finite; a program needn't handle non-finite values.
Results may differ from the reference program's by a relative error of at most 0.008.
Values may be sent and summed in bfloat16 or wider, within the bound.
A program may use at most 64 MiB of HBM per device.

```python
import math
import jax
import jax.numpy as jnp
from jax import lax

HID = 512
C2 = 24
W2 = 32
STEPS2 = 3
STEPS3 = 2
B = 64
H2 = 64
C3 = 48


def level_of(rng, extent, split, least, high):
    gain, own = 1.0, jax.random.fold_in(rng, 6)
    for axis_at, shards_of in split:
        draws = jnp.exp(jax.random.uniform(jax.random.fold_in(own, axis_at), (shards_of,), jnp.float32, least / len(split), high / len(split)))
        gain = gain * jnp.repeat(draws, extent[axis_at] // shards_of).reshape([-1 if axis == axis_at else 1 for axis in range(len(extent))])
    return gain


def centred(rng, dims, width, bound, shards=(), held_as=jnp.bfloat16):
    array = width * jax.random.normal(rng, dims, jnp.float32)
    if shards:
        array = array * level_of(rng, dims, shards, -0.22, 0.18)
    return jnp.clip(array, -bound, bound).astype(held_as)


def setup_inputs(seed: int = 0) -> dict:
    keys = jax.random.split(jax.random.key(seed), 24)
    return {
        "images": centred(keys[0], (B, C2, H2, W2), 1.0, 6.0, ((0, 8), (2, 64)), jnp.float32),
        "shift_mid": centred(keys[1], (STEPS2, C2), 0.3, 1.75, (), jnp.float32),
        "gain_mid": jnp.clip(jax.random.uniform(keys[2], (STEPS2, C2), jnp.float32, -0.3, 0.3), -0.3, 0.3),
        "lower_mid": centred(keys[3], (STEPS2, C2, C2), C2 ** -0.5, 1.25, (), jnp.float32),
        "upper_mid": centred(keys[4], (STEPS2, C2, C2), C2 ** -0.5, 1.25, (), jnp.float32),
        "diag_mid": jnp.clip(jax.random.uniform(keys[5], (STEPS2, C2), jnp.float32, -0.3, 0.3), -0.3, 0.3),
        "first_mid": centred(keys[6], (STEPS2, 9, C2 // 2, HID), (9 * C2 // 2) ** -0.5, 0.625),
        "first_bias_mid": centred(keys[7], (STEPS2, HID), 0.5, 3.0),
        "second_mid": centred(keys[8], (STEPS2, HID, HID), HID ** -0.5, 0.25),
        "second_bias_mid": centred(keys[9], (STEPS2, HID), 0.5, 3.0, (), jnp.float32),
        "third_mid": centred(keys[10], (STEPS2, 9, HID, C2), (9 * HID) ** -0.5, 0.09375),
        "third_bias_mid": centred(keys[11], (STEPS2, C2), 0.5, 3.0, (), jnp.float32),
        "shift_top": centred(keys[12], (STEPS3, C3), 0.3, 1.75, (), jnp.float32),
        "gain_top": jnp.clip(jax.random.uniform(keys[13], (STEPS3, C3), jnp.float32, -0.3, 0.3), -0.3, 0.3),
        "lower_top": centred(keys[14], (STEPS3, C3, C3), C3 ** -0.5, 0.875, (), jnp.float32),
        "upper_top": centred(keys[15], (STEPS3, C3, C3), C3 ** -0.5, 0.875, (), jnp.float32),
        "diag_top": jnp.clip(jax.random.uniform(keys[16], (STEPS3, C3), jnp.float32, -0.3, 0.3), -0.3, 0.3),
        "first_top": centred(keys[17], (STEPS3, 9, C2, HID), (9 * C2) ** -0.5, 0.4375),
        "first_bias_top": centred(keys[18], (STEPS3, HID), 0.5, 3.0),
        "second_top": centred(keys[19], (STEPS3, HID, HID), HID ** -0.5, 0.25),
        "second_bias_top": centred(keys[20], (STEPS3, HID), 0.5, 3.0, (), jnp.float32),
        "third_top": centred(keys[21], (STEPS3, 9, HID, C3), (9 * HID) ** -0.5, 0.09375),
        "third_bias_top": centred(keys[22], (STEPS3, C3), 0.5, 3.0, (), jnp.float32),
    }


log_two_pi = math.log(2.0 * math.pi)


def spatial_conv(source, weights):
    height = source.shape[1]
    columns = source.shape[2]
    padded = jnp.pad(source, ((0, 0), (1, 1), (1, 1))).astype(jnp.float32)
    summed = jnp.zeros((weights.shape[2], height, columns), jnp.float32)
    for tap_idx in range(9):
        row_off = tap_idx // 3
        col_off = tap_idx % 3
        window = padded[:, row_off:row_off + height, col_off:col_off + columns]
        summed = summed + jnp.einsum('chw,co->ohw', window, weights[tap_idx].astype(jnp.float32))
    return summed


def flow_step(flow_state, params):
    shift_vec, gain_vec, lower_raw, upper_raw, diag_log, first_w, first_b, second_w, second_b, third_w, third_b = params
    channels = flow_state.shape[0]
    half_chan = channels // 2
    cell_count = flow_state.shape[1] * flow_state.shape[2]
    mixed_state = (flow_state + shift_vec[:, None, None]) * jnp.exp(gain_vec)[:, None, None]
    lower_mat = jnp.tril(lower_raw, -1) + jnp.eye(channels, dtype=jnp.float32)
    upper_mat = jnp.triu(upper_raw, 1) + jnp.diag(jnp.exp(diag_log))
    matrix = jnp.dot(lower_mat, upper_mat, precision=lax.Precision.HIGHEST)
    mixed_state = jnp.einsum('oc,chw->ohw', matrix, mixed_state, precision=lax.Precision.HIGHEST)
    part_a = mixed_state[:half_chan]
    part_b = mixed_state[half_chan:]
    coupled = part_a.astype(jnp.bfloat16)
    inner = jax.nn.relu(spatial_conv(coupled, first_w) + first_b.astype(jnp.float32)[:, None, None]).astype(jnp.bfloat16)
    middle = jnp.einsum('chw,co->ohw', inner.astype(jnp.float32), second_w.astype(jnp.float32))
    middle = jax.nn.relu(middle + second_b[:, None, None]).astype(jnp.bfloat16)
    output = spatial_conv(middle, third_w) + third_b[:, None, None]
    gate_pre = output[:half_chan] + 2.0
    updated = (part_b + output[half_chan:]) * jax.nn.sigmoid(gate_pre)
    step_term = cell_count * (jnp.sum(gain_vec) + jnp.sum(diag_log)) + jnp.sum(jax.nn.log_sigmoid(gate_pre))
    return jnp.concatenate([part_a, updated], axis=0), step_term


def image_flow(picture, params_mid, params_top):
    flow_state = picture
    logdet = jnp.zeros((), jnp.float32)
    for step_num in range(params_mid[0].shape[0]):
        flow_state, step_term = flow_step(flow_state, tuple(p[step_num] for p in params_mid))
        logdet = logdet + step_term
    half_chan = flow_state.shape[0] // 2
    latent_mid = flow_state[:half_chan]
    kept_chan = flow_state[half_chan:]
    count_chan, height, columns = kept_chan.shape
    squeezed = kept_chan.reshape(count_chan, height // 2, 2, columns // 2, 2).transpose(0, 2, 4, 1, 3)
    flow_state = squeezed.reshape(count_chan * 4, height // 2, columns // 2)
    for step_num in range(params_top[0].shape[0]):
        flow_state, step_term = flow_step(flow_state, tuple(p[step_num] for p in params_top))
        logdet = logdet + step_term
    latent_top = flow_state
    latent_count = latent_mid.size + latent_top.size
    logprob = -0.5 * (jnp.sum(latent_mid * latent_mid) + jnp.sum(latent_top * latent_top)) - 0.5 * log_two_pi * latent_count
    total_dims = picture.shape[0] * picture.shape[1] * picture.shape[2]
    return latent_mid, latent_top, (logprob + logdet) / total_dims


def reference(images, shift_mid, gain_mid, lower_mid, upper_mid, diag_mid, first_mid, first_bias_mid, second_mid, second_bias_mid, third_mid, third_bias_mid, shift_top, gain_top, lower_top, upper_top, diag_top, first_top, first_bias_top, second_top, second_bias_top, third_top, third_bias_top):
    params_mid = (shift_mid, gain_mid, lower_mid, upper_mid, diag_mid, first_mid, first_bias_mid, second_mid, second_bias_mid, third_mid, third_bias_mid)
    params_top = (shift_top, gain_top, lower_top, upper_top, diag_top, first_top, first_bias_top, second_top, second_bias_top, third_top, third_bias_top)
    latent_mid, latent_top, loglik = lax.map(lambda picture: image_flow(picture, params_mid, params_top), images)
    return (latent_mid, latent_top, loglik)
```

```python
import functools
import math

import jax
import jax.numpy as jnp
from jax import lax
from jax.experimental import pallas as pl
from jax.experimental.pallas import tpu as pltpu
from jax.sharding import PartitionSpec as P

MESH = pl.DeviceIdType.MESH
F32 = jnp.float32
BF16 = jnp.bfloat16
HI = lax.Precision.HIGHEST
log_two_pi = math.log(2.0 * math.pi)


def iota2(shape, dim):
    return lax.broadcasted_iota(jnp.int32, shape, dim)


def mixing(lower, upper, diag, gain, shift, spread, place, split_at):
    n = lower.shape[0]
    r, c = iota2((n, n), 0), iota2((n, n), 1)
    low = jnp.where(r > c, lower, jnp.where(r == c, 1.0, 0.0))
    up = jnp.where(c > r, upper, jnp.where(r == c, jnp.exp(diag), 0.0)) * jnp.exp(gain)
    both = jnp.dot(low, up, precision=HI, preferred_element_type=F32)
    if spread is not None:
        both = jnp.dot(spread, both, precision=HI, preferred_element_type=F32)
    const = jnp.sum(both * shift, axis=1, keepdims=True)
    wide = jnp.dot(both, place, precision=HI, preferred_element_type=F32)
    high = wide.astype(BF16).astype(F32)
    lane = iota2(wide.shape, 1)
    return jnp.where(lane < split_at, high, wide - high).astype(BF16), const


def column(row):
    n = row.shape[1]
    eye = iota2((n, n), 0) == iota2((n, n), 1)
    return jnp.sum(jnp.where(eye, jnp.broadcast_to(row, (n, n)), 0.0), axis=1, keepdims=True)


def apply_mix(state, mix, const):
    high = state.astype(BF16)
    low = (state - high.astype(F32)).astype(BF16)
    stacked = jnp.concatenate([high, low, high], axis=0)
    return jnp.dot(mix, stacked, preferred_element_type=F32) + const


def coupling(u, half, pad, w1t, w2t, bias2, w3, bias3, left_ok, right_ok, up_ok, down_ok, cols, tile, extra):
    length = u.shape[1]
    ua, ub = u[:pad], u[pad : 2 * pad]
    q = ua.astype(BF16).astype(F32)
    sides = (
        jnp.where(left_ok, pltpu.roll(q, 1, 1), 0.0),
        q,
        jnp.where(right_ok, pltpu.roll(q, length - 1, 1), 0.0),
    )
    above = [jnp.where(up_ok, pltpu.roll(s, cols, 1), 0.0) for s in sides]
    below = [jnp.where(down_ok, pltpu.roll(s, length - cols, 1), 0.0) for s in sides]
    stack = [*above, *sides, *below]
    if extra:
        stack.append(jnp.ones((8, length), F32))
    patches = jnp.concatenate(stack, axis=0).astype(BF16)
    pieces = []
    for at in range(0, length, tile):
        h = jnp.dot(w1t[...], patches[:, at : at + tile], preferred_element_type=F32)
        h = jnp.maximum(h, 0.0).astype(BF16)
        h = jnp.dot(w2t[...], h, preferred_element_type=F32)
        b = bias2[...]
        b = jnp.concatenate([b] * (tile // 128), axis=1)
        h = jnp.maximum(h + b, 0.0).astype(BF16)
        pieces.append(jnp.dot(w3[...], h, preferred_element_type=F32))
    taps = jnp.concatenate(pieces, axis=1) if len(pieces) > 1 else pieces[0]
    both = 2 * half
    rows = []
    for dr in range(3):
        a, b, c = (taps[(dr * 3 + dc) * both : (dr * 3 + dc + 1) * both] for dc in range(3))
        rows.append(
            b
            + jnp.where(left_ok, pltpu.roll(a, 1, 1), 0.0)
            + jnp.where(right_ok, pltpu.roll(c, length - 1, 1), 0.0)
        )
    out = (
        rows[1]
        + jnp.where(up_ok, pltpu.roll(rows[0], cols, 1), 0.0)
        + jnp.where(down_ok, pltpu.roll(rows[2], length - cols, 1), 0.0)
        + bias3
    )
    g, t = out[:half] + 2.0, out[half:]
    if pad > half:
        zeros = jnp.zeros((pad - half, length), F32)
        g, t = jnp.concatenate([g, zeros], axis=0), jnp.concatenate([t, zeros], axis=0)
    return ua, (ub + t) * jax.nn.sigmoid(g), g


def log_sigmoid(g):
    return jnp.minimum(g, 0.0) - jnp.log1p(jnp.exp(-jnp.abs(g)))


def kernel(
    n_rows,
    n_chan,
    images,
    shift_mid,
    gain_mid,
    lower_mid,
    upper_mid,
    diag_mid,
    first_mid,
    first_bias_mid,
    second_mid,
    second_bias_mid,
    third_mid,
    third_bias_mid,
    shift_top,
    gain_top,
    lower_top,
    upper_top,
    diag_top,
    first_top,
    first_bias_top,
    second_top,
    second_bias_top,
    third_top,
    third_bias_top,
    latent_mid,
    latent_top,
    loglik,
    img_v,
    w1m,
    w2m,
    w3m,
    w1p,
    w2p,
    w3p,
    w1f_m,
    w1f_p,
    w1m_t,
    w2m_t,
    w1p_t,
    w2p_t,
    b2m,
    b2p,
    mix_m,
    mix_p0,
    mix_p1,
    const_m,
    const_p,
    y_out,
    y_in,
    z_out,
    z_in,
    back_out,
    back_in,
    ll_out,
    ll_in,
    load_sem,
    ys_sem,
    yr_sem,
    zs_sem,
    zr_sem,
    bs_sem,
    br_sem,
    ls_sem,
    lr_sem,
):
    me_row, me_chan = lax.axis_index("rows"), lax.axis_index("chan")
    steps_m, steps_p = shift_mid.shape[0], shift_top.shape[0]
    n_img, c_mid, width = img_v.shape
    half_m = c_mid // 2
    c_top = shift_top.shape[1]
    half_p = c_top // 2

    loads = [
        pltpu.make_async_copy(src, dst, load_sem.at[k])
        for k, (src, dst) in enumerate(
            (
                (images, img_v),
                (first_mid, w1m),
                (second_mid, w2m),
                (third_mid, w3m),
                (first_top, w1p),
                (second_top, w2p),
                (third_top, w3p),
            )
        )
    ]
    for load in loads:
        load.start()

    barrier = pltpu.get_barrier_semaphore()
    chan_peers = [lax.rem(me_chan + k, n_chan) for k in range(1, n_chan)]
    row_peers = [lax.rem(me_row + k, n_rows) for k in range(1, n_rows)]
    for peer in chan_peers:
        pl.semaphore_signal(barrier, inc=1, device_id={"chan": peer}, device_id_type=MESH)
    for peer in row_peers:
        pl.semaphore_signal(barrier, inc=1, device_id={"rows": peer}, device_id_type=MESH)

    loads[0].wait()
    for i in range(n_img):
        row = img_v[i]
        packed = [row[8 * k : 8 * k + 8] for k in range(c_mid // 8)]
        packed.append(jnp.zeros((8, 128 - width * (c_mid // 8)), F32))
        y_out[i] = jnp.concatenate(packed, axis=1)
    y_in[me_chan] = y_out[me_chan]

    spread = jnp.where(
        iota2((32, c_mid), 0)
        == iota2((32, c_mid), 1) + jnp.where(iota2((32, c_mid), 1) >= half_m, 16 - half_m, 0),
        1.0,
        0.0,
    )
    src, lane = iota2((c_mid, 96), 0), lax.rem(iota2((c_mid, 96), 1), 32)
    plain = jnp.where(src == lane, 1.0, 0.0)
    padded = jnp.where(src + jnp.where(src >= half_m, 16 - half_m, 0) == lane, 1.0, 0.0)
    for s in range(steps_m):
        mix, const = mixing(
            lower_mid[s],
            upper_mid[s],
            diag_mid[s : s + 1],
            gain_mid[s : s + 1],
            shift_mid[s : s + 1],
            spread,
            plain if s == 0 else padded,
            64,
        )
        mix_m[s] = mix
        const_m[s] = jnp.where(iota2((32, 1), 0) == half_m, 1.0, const)
    src, lane = iota2((c_top, 192), 0), lax.rem(iota2((c_top, 192), 1), 64)
    squeezed_place = jnp.where(
        jnp.logical_and(lax.rem(lane, 16) < half_m, src == 4 * lax.rem(lane, 16) + lax.div(lane, 16)), 1.0, 0.0
    )
    src, lane = iota2((c_top, 144), 0), lax.rem(iota2((c_top, 144), 1), 48)
    top_place = jnp.where(src == lane, 1.0, 0.0)
    for s in range(steps_p):
        mix, const = mixing(
            lower_top[s],
            upper_top[s],
            diag_top[s : s + 1],
            gain_top[s : s + 1],
            shift_top[s : s + 1],
            None,
            squeezed_place if s == 0 else top_place,
            128 if s == 0 else 96,
        )
        if s == 0:
            mix_p0[...] = mix
        else:
            mix_p1[s - 1] = mix
        const_p[s] = const

    pl.semaphore_wait(barrier, n_chan + n_rows - 2)
    y_copies = []
    for k, peer in enumerate(chan_peers):
        copy = pltpu.make_async_remote_copy(
            src_ref=y_out.at[peer],
            dst_ref=y_in.at[me_chan],
            send_sem=ys_sem.at[k],
            recv_sem=yr_sem.at[n_chan - 2 - k],
            device_id={"chan": peer},
            device_id_type=MESH,
        )
        copy.start()
        y_copies.append(copy)

    def prepare_mid(s):
        w1f_m[...] = jnp.zeros_like(w1f_m)
        for t in range(9):
            w1f_m[16 * t : 16 * t + half_m] = w1m[s, t].astype(F32)
        w1f_m[64 + half_m : 65 + half_m] = first_bias_mid[s : s + 1].astype(F32)
        w1m_t[s] = w1f_m[...].T.astype(BF16)
        w2m_t[s] = w2m[s].T
        b2m[s] = jnp.broadcast_to(second_bias_mid[s : s + 1], (128, b2m.shape[1])).T

    def prepare_top(s):
        w1f_p[9 * half_p :] = jnp.zeros((8, w1f_p.shape[1]), F32)
        w1f_p[: 9 * half_p] = w1p[s].astype(F32)
        w1f_p[9 * half_p : 9 * half_p + 1] = first_bias_top[s : s + 1].astype(F32)
        w1p_t[s] = w1f_p[...].T.astype(BF16)
        w2p_t[s] = w2p[s].T
        b2p[s] = jnp.broadcast_to(second_bias_top[s : s + 1], (128, b2p.shape[1])).T

    loads[1].wait()
    loads[2].wait()
    prepare_mid(0)

    for copy in y_copies:
        copy.wait_recv()
    groups = []
    for k in range(c_mid // 8):
        groups.append(jnp.concatenate([y_in[c][:, width * k : width * (k + 1)] for c in range(n_chan)], axis=1))
    own = jnp.concatenate([*groups, jnp.zeros((32 - c_mid, n_chan * width), F32)], axis=0)
    z_out[...] = own.astype(BF16)
    z_copies = []
    for k, d in enumerate((1, -1, 2, -2)):
        copy = pltpu.make_async_remote_copy(
            src_ref=z_out,
            dst_ref=z_in.at[k],
            send_sem=zs_sem.at[k],
            recv_sem=zr_sem.at[k],
            device_id={"rows": lax.rem(me_row + d + n_rows, n_rows)},
            device_id_type=MESH,
        )
        copy.start()
        z_copies.append(copy)
    for s in range(1, steps_m):
        prepare_mid(s)
    for load in loads[3:]:
        load.wait()
    for s in range(steps_p):
        prepare_top(s)
    bias3_m = [column(third_bias_mid[s : s + 1]) for s in range(steps_m)]
    bias3_p = [column(third_bias_top[s : s + 1]) for s in range(steps_p)]
    for copy in z_copies:
        copy.wait_recv()
    state = jnp.concatenate([z_in[2].astype(F32), z_in[0].astype(F32), own, z_in[1].astype(F32), z_in[3].astype(F32)], axis=1)

    height = n_rows * n_chan
    partial = jnp.zeros((8, 128), F32)

    def folded(x):
        total = None
        for i in range(0, x.shape[0], 8):
            for j in range(0, x.shape[1], 128):
                piece = x[i : i + 8, j : j + 128]
                total = piece if total is None else total + piece
        return total

    first_row = me_row * n_chan - 2 * n_chan
    own_at = 2 * n_chan * width
    own_lanes = n_chan * width
    valid_m = iota2((16, own_lanes), 0) < half_m
    for s in range(steps_m):
        if s == 1:
            state = state[:, 4 * width : 36 * width]
            first_row = first_row + 4
            own_at = own_at - 4 * width
        length = state.shape[1]
        lane = iota2((1, length), 1)
        col, row = lax.rem(lane, width), lax.div(lane, width) + first_row
        u = apply_mix(state, mix_m[s], const_m[s])
        ua, updated, g = coupling(
            u,
            half_m,
            16,
            w1m_t.at[s],
            w2m_t.at[s],
            b2m.at[s],
            w3m.at[s],
            bias3_m[s],
            col >= 1,
            col <= width - 2,
            row >= 1,
            row <= height - 2,
            width,
            256,
            False,
        )
        state = jnp.concatenate([ua, updated], axis=0)
        mine = g[:, own_at : own_at + own_lanes]
        partial = partial + folded(jnp.where(valid_m, log_sigmoid(mine), 0.0))
    latent = jnp.where(valid_m, state[:16, own_at : own_at + own_lanes], 0.0)
    partial = partial + folded(-0.5 * latent * latent)

    for c in range(n_chan):
        piece = latent[:, width * c : width * (c + 1)]
        back_out[c] = jnp.concatenate([piece[:8], piece[8:], jnp.zeros((8, 128 - 2 * width), F32)], axis=1)
    back_in[me_chan] = back_out[me_chan]
    back_copies = []
    for k, peer in enumerate(chan_peers):
        copy = pltpu.make_async_remote_copy(
            src_ref=back_out.at[peer],
            dst_ref=back_in.at[me_chan],
            send_sem=bs_sem.at[k],
            recv_sem=br_sem.at[n_chan - 2 - k],
            device_id={"chan": peer},
            device_id_type=MESH,
        )
        copy.start()
        back_copies.append(copy)

    kept = state[16:, 4 * width : 28 * width]
    cols_p = width // 2
    lane = iota2((16, 128), 1)
    phase, rest = lax.div(lane, 32), lax.rem(lane, 32)
    pick = (2 * lax.div(rest, cols_p) + lax.div(phase, 2)) * width + 2 * lax.rem(rest, cols_p) + lax.rem(phase, 2)
    blocks = [
        jnp.take_along_axis(kept[:, 128 * k : 128 * k + 128], pick, axis=1) for k in range(kept.shape[1] // 128)
    ]
    phases = []
    for p in range(4):
        parts = [b[:, 32 * p : 32 * p + 32] for b in blocks]
        parts.append(jnp.zeros((16, 256 - 32 * len(blocks)), F32))
        phases.append(jnp.concatenate(parts, axis=1))
    state = jnp.concatenate(phases, axis=0)

    rows_p = n_chan // 2
    first_row = me_row * rows_p - rows_p
    length = state.shape[1]
    lane = iota2((1, length), 1)
    col, row = lax.rem(lane, cols_p), lax.div(lane, cols_p) + first_row
    own_at = rows_p * cols_p
    mine_p = jnp.logical_and(lane >= own_at, lane < 2 * own_at)
    for s in range(steps_p):
        u = apply_mix(state, mix_p0[...] if s == 0 else mix_p1[s - 1], const_p[s])
        ua, updated, g = coupling(
            u,
            half_p,
            half_p,
            w1p_t.at[s],
            w2p_t.at[s],
            b2p.at[s],
            w3p.at[s],
            bias3_p[s],
            col >= 1,
            col <= cols_p - 2,
            row >= 1,
            row <= height // 2 - 2,
            cols_p,
            256,
            True,
        )
        state = jnp.concatenate([ua, updated], axis=0)
        partial = partial + folded(jnp.where(mine_p, log_sigmoid(g), 0.0))
    partial = partial + folded(jnp.where(mine_p, -0.5 * state * state, 0.0))
    ll_out[...] = jnp.sum(partial, axis=0, keepdims=True)
    ll_copies = []
    for k, peer in enumerate(row_peers):
        copy = pltpu.make_async_remote_copy(
            src_ref=ll_out,
            dst_ref=ll_in.at[n_rows - 2 - k],
            send_sem=ls_sem.at[k],
            recv_sem=lr_sem.at[n_rows - 2 - k],
            device_id={"rows": peer},
            device_id_type=MESH,
        )
        copy.start()
        ll_copies.append(copy)

    latent_top[...] = state[:, :128].T[own_at : 2 * own_at]
    for copy in back_copies:
        copy.wait_recv()
    for c in range(n_img):
        piece = back_in[c]
        latent_mid[c, :8] = piece[:, :width]
        latent_mid[c, 8:half_m] = piece[: half_m - 8, width : 2 * width]
    cells = height * width
    const = sum(
        (
            cells * (jnp.sum(gain_mid[...]) + jnp.sum(diag_mid[...])),
            (cells // 4) * (jnp.sum(gain_top[...]) + jnp.sum(diag_top[...])),
        )
    )
    for copy in ll_copies:
        copy.wait_recv()
    total = ll_out[...]
    for k in range(n_rows - 1):
        total = total + ll_in[k]
    scale = 1.0 / (c_mid * cells)
    loglik[...] = jnp.broadcast_to((jnp.sum(total) + const) * scale - 0.5 * log_two_pi, (1, 128))
    for copy in (*y_copies, *z_copies, *back_copies, *ll_copies):
        copy.wait_send()


def body(
    images,
    shift_mid,
    gain_mid,
    lower_mid,
    upper_mid,
    diag_mid,
    first_mid,
    first_bias_mid,
    second_mid,
    second_bias_mid,
    third_mid,
    third_bias_mid,
    shift_top,
    gain_top,
    lower_top,
    upper_top,
    diag_top,
    first_top,
    first_bias_top,
    second_top,
    second_bias_top,
    third_top,
    third_bias_top,
):
    n_rows, n_chan = lax.axis_size("rows"), lax.axis_size("chan")
    n_img, c_mid, _, width = images.shape
    hid = second_mid.shape[1]
    steps_m, steps_p = shift_mid.shape[0], shift_top.shape[0]
    c_top = shift_top.shape[1]
    half_m, half_p = c_mid // 2, c_top // 2
    images = images.reshape(n_img, c_mid, width)
    third_mid = third_mid.transpose(0, 1, 3, 2).reshape(steps_m, 9 * c_mid, hid)
    third_top = third_top.transpose(0, 1, 3, 2).reshape(steps_p, 9 * c_top, hid)
    first_top = first_top.reshape(steps_p, 9 * half_p, hid)
    big = pl.BlockSpec(memory_space=pl.ANY)
    small = pl.BlockSpec(memory_space=pltpu.VMEM)
    where = [big] + [small] * 5 + [big, small] * 2 + [big, small] + [small] * 5 + [big, small] * 3
    rows_p = n_chan // 2
    vmem = pltpu.VMEM
    dma = pltpu.SemaphoreType.DMA
    latent_mid, latent_top, loglik = pl.pallas_call(
        functools.partial(kernel, n_rows, n_chan),
        out_shape=(
            jax.ShapeDtypeStruct((n_img, half_m, width), F32),
            jax.ShapeDtypeStruct((rows_p * width // 2, c_top), F32),
            jax.ShapeDtypeStruct((1, 128), F32),
        ),
        in_specs=where,
        out_specs=(small, small, small),
        scratch_shapes=[
            vmem((n_img, c_mid, width), F32),
            vmem((steps_m, 9, half_m, hid), BF16),
            vmem((steps_m, hid, hid), BF16),
            vmem((steps_m, 9 * c_mid, hid), BF16),
            vmem((steps_p, 9 * half_p, hid), BF16),
            vmem((steps_p, hid, hid), BF16),
            vmem((steps_p, 9 * c_top, hid), BF16),
            vmem((144, hid), F32),
            vmem((9 * half_p + 8, hid), F32),
            vmem((steps_m, hid, 144), BF16),
            vmem((steps_m, hid, hid), BF16),
            vmem((steps_p, hid, 9 * half_p + 8), BF16),
            vmem((steps_p, hid, hid), BF16),
            vmem((steps_m, hid, 128), F32),
            vmem((steps_p, hid, 128), F32),
            vmem((steps_m, 32, 96), BF16),
            vmem((c_top, 192), BF16),
            vmem((steps_p - 1, c_top, 144), BF16),
            vmem((steps_m, 32, 1), F32),
            vmem((steps_p, c_top, 1), F32),
            vmem((n_chan, 8, 128), F32),
            vmem((n_chan, 8, 128), F32),
            vmem((32, n_chan * width), BF16),
            vmem((4, 32, n_chan * width), BF16),
            vmem((n_chan, 8, 128), F32),
            vmem((n_chan, 8, 128), F32),
            vmem((1, 128), F32),
            vmem((n_rows - 1, 1, 128), F32),
            dma((7,)),
            dma((n_chan - 1,)),
            dma((n_chan - 1,)),
            dma((4,)),
            dma((4,)),
            dma((n_chan - 1,)),
            dma((n_chan - 1,)),
            dma((n_rows - 1,)),
            dma((n_rows - 1,)),
        ],
        compiler_params=pltpu.CompilerParams(
            collective_id=0, has_side_effects=True, vmem_limit_bytes=66 * 1000 * 1000
        ),
    )(
        images,
        shift_mid,
        gain_mid,
        lower_mid,
        upper_mid,
        diag_mid,
        first_mid,
        first_bias_mid,
        second_mid,
        second_bias_mid,
        third_mid,
        third_bias_mid,
        shift_top,
        gain_top,
        lower_top,
        upper_top,
        diag_top,
        first_top,
        first_bias_top,
        second_top,
        second_bias_top,
        third_top,
        third_bias_top,
    )
    latent_mid = latent_mid.reshape(n_img, half_m, 1, width)
    latent_top = latent_top.reshape(1, rows_p, width // 2, c_top).transpose(0, 3, 1, 2)
    return latent_mid, latent_top, loglik[0, :1]


def solution(mesh):
    placed = (P("batch", None, ("rows", "chan"), None),) + (P(),) * 22
    return jax.shard_map(
        body,
        mesh=mesh,
        in_specs=placed,
        out_specs=(
            P("batch", None, ("rows", "chan"), None),
            P(("batch", "chan"), None, "rows", None),
            P(("batch", "chan")),
        ),
        check_vma=False,
    )
```

```python
import functools
import math

import jax
import jax.numpy as jnp
from jax import lax
from jax.experimental import pallas as pl
from jax.experimental.pallas import tpu as pltpu
from jax.sharding import PartitionSpec as P

MESH = pl.DeviceIdType.MESH
F32 = jnp.float32
BF16 = jnp.bfloat16
HI = lax.Precision.HIGHEST
log_two_pi = math.log(2.0 * math.pi)


def iota2(shape, dim):
    return lax.broadcasted_iota(jnp.int32, shape, dim)


def mixing(lower, upper, diag, gain, shift, spread, place, split_at):
    n = lower.shape[0]
    r, c = iota2((n, n), 0), iota2((n, n), 1)
    low = jnp.where(r > c, lower, jnp.where(r == c, 1.0, 0.0))
    up = jnp.where(c > r, upper, jnp.where(r == c, jnp.exp(diag), 0.0)) * jnp.exp(gain)
    both = jnp.dot(low, up, precision=HI, preferred_element_type=F32)
    if spread is not None:
        both = jnp.dot(spread, both, precision=HI, preferred_element_type=F32)
    const = jnp.sum(both * shift, axis=1, keepdims=True)
    wide = jnp.dot(both, place, precision=HI, preferred_element_type=F32)
    high = wide.astype(BF16).astype(F32)
    lane = iota2(wide.shape, 1)
    return jnp.where(lane < split_at, high, wide - high).astype(BF16), const


def column(row):
    n = row.shape[1]
    eye = iota2((n, n), 0) == iota2((n, n), 1)
    return jnp.sum(jnp.where(eye, jnp.broadcast_to(row, (n, n)), 0.0), axis=1, keepdims=True)


def apply_mix(state, mix, const):
    high = state.astype(BF16)
    low = (state - high.astype(F32)).astype(BF16)
    stacked = jnp.concatenate([high, low, high], axis=0)
    return jnp.dot(mix, stacked, preferred_element_type=F32) + const


def dot(w, x):
    if x.shape[1] > 256:
        return jnp.dot(w[...], x, preferred_element_type=F32)
    rows = w.shape[0]
    cut = rows // 16 // 2 * 16
    return jnp.concatenate(
        [
            jnp.dot(w[:cut], x, preferred_element_type=F32),
            jnp.dot(w[cut:], x, preferred_element_type=F32),
        ],
        axis=0,
    )


def coupling(u, half, pad, w1t, w2t, bias2, w3, bias3, left_ok, right_ok, up_ok, down_ok, cols, tile, extra):
    length = u.shape[1]
    ua, ub = u[:pad], u[pad : 2 * pad]
    q = ua.astype(BF16).astype(F32)
    sides = (
        jnp.where(left_ok, pltpu.roll(q, 1, 1), 0.0),
        q,
        jnp.where(right_ok, pltpu.roll(q, length - 1, 1), 0.0),
    )
    above = [jnp.where(up_ok, pltpu.roll(s, cols, 1), 0.0) for s in sides]
    below = [jnp.where(down_ok, pltpu.roll(s, length - cols, 1), 0.0) for s in sides]
    stack = [*above, *sides, *below]
    if extra:
        stack.append(jnp.ones((8, length), F32))
    patches = jnp.concatenate(stack, axis=0).astype(BF16)
    pieces = []
    for at in range(0, length, tile):
        size = min(tile, length - at)
        h = dot(w1t, patches[:, at : at + size])
        h = jnp.maximum(h, 0.0).astype(BF16)
        h = dot(w2t, h)
        b = bias2[...]
        b = jnp.concatenate([b] * (size // 128), axis=1)
        h = jnp.maximum(h + b, 0.0).astype(BF16)
        pieces.append(dot(w3, h))
    taps = jnp.concatenate(pieces, axis=1) if len(pieces) > 1 else pieces[0]
    both = 2 * half
    rows = []
    for dr in range(3):
        a, b, c = (taps[(dr * 3 + dc) * both : (dr * 3 + dc + 1) * both] for dc in range(3))
        rows.append(
            b
            + jnp.where(left_ok, pltpu.roll(a, 1, 1), 0.0)
            + jnp.where(right_ok, pltpu.roll(c, length - 1, 1), 0.0)
        )
    out = (
        rows[1]
        + jnp.where(up_ok, pltpu.roll(rows[0], cols, 1), 0.0)
        + jnp.where(down_ok, pltpu.roll(rows[2], length - cols, 1), 0.0)
        + bias3
    )
    g, t = out[:half] + 2.0, out[half:]
    if pad > half:
        zeros = jnp.zeros((pad - half, length), F32)
        g, t = jnp.concatenate([g, zeros], axis=0), jnp.concatenate([t, zeros], axis=0)
    return ua, (ub + t) * jax.nn.sigmoid(g), g


def log_sigmoid(g):
    return jnp.minimum(g, 0.0) - jnp.log1p(jnp.exp(-jnp.abs(g)))


def kernel(
    n_rows,
    n_chan,
    images,
    shift_mid_h,
    gain_mid_h,
    lower_mid_h,
    upper_mid_h,
    diag_mid_h,
    first_mid,
    first_bias_mid_h,
    second_mid,
    second_bias_mid_h,
    third_mid,
    third_bias_mid_h,
    shift_top_h,
    gain_top_h,
    lower_top_h,
    upper_top_h,
    diag_top_h,
    first_top,
    first_bias_top_h,
    second_top,
    second_bias_top_h,
    third_top,
    third_bias_top_h,
    latent_mid,
    latent_top,
    loglik,
    img_v,
    w1m,
    w2m,
    w3m,
    w1p,
    w2p,
    w3p,
    w1f_m,
    w1f_p,
    w1m_t,
    w2m_t,
    w1p_t,
    w2p_t,
    b2m,
    b2p,
    mix_m,
    mix_p0,
    mix_p1,
    const_m,
    const_p,
    y_out,
    y_in,
    z_out,
    z_in,
    back_out,
    back_in,
    ll_out,
    ll_in,
    shift_mid,
    gain_mid,
    lower_mid,
    upper_mid,
    diag_mid,
    first_bias_mid,
    second_bias_mid,
    third_bias_mid,
    shift_top,
    gain_top,
    lower_top,
    upper_top,
    diag_top,
    first_bias_top,
    second_bias_top,
    third_bias_top,
    load_sem,
    small_sem,
    ys_sem,
    yr_sem,
    zs_sem,
    zr_sem,
    bs_sem,
    br_sem,
    ls_sem,
    lr_sem,
):
    me_row, me_chan = lax.axis_index("rows"), lax.axis_index("chan")
    steps_m, steps_p = shift_mid.shape[0], shift_top.shape[0]
    n_img, c_mid, width = img_v.shape
    half_m = c_mid // 2
    c_top = shift_top.shape[1]
    half_p = c_top // 2

    barrier = pltpu.get_barrier_semaphore()
    chan_peers = [lax.rem(me_chan + k, n_chan) for k in range(1, n_chan)]
    row_peers = [lax.rem(me_row + k, n_rows) for k in range(1, n_rows)]
    for peer in chan_peers:
        pl.semaphore_signal(barrier, inc=1, device_id={"chan": peer}, device_id_type=MESH)
    for peer in row_peers:
        pl.semaphore_signal(barrier, inc=1, device_id={"rows": peer}, device_id_type=MESH)

    loads = [
        pltpu.make_async_copy(src, dst, load_sem.at[k])
        for k, (src, dst) in enumerate(
            (
                (images, img_v),
                (first_mid, w1m),
                (second_mid, w2m),
                (third_mid, w3m),
                (first_top, w1p),
                (second_top, w2p),
                (third_top, w3p),
            )
        )
    ]
    smalls = [
        pltpu.make_async_copy(src, dst, small_sem.at[k])
        for k, (src, dst) in enumerate(
            (
                (shift_mid_h, shift_mid),
                (gain_mid_h, gain_mid),
                (lower_mid_h, lower_mid),
                (upper_mid_h, upper_mid),
                (diag_mid_h, diag_mid),
                (first_bias_mid_h, first_bias_mid),
                (second_bias_mid_h, second_bias_mid),
                (third_bias_mid_h, third_bias_mid),
                (shift_top_h, shift_top),
                (gain_top_h, gain_top),
                (lower_top_h, lower_top),
                (upper_top_h, upper_top),
                (diag_top_h, diag_top),
                (first_bias_top_h, first_bias_top),
                (second_bias_top_h, second_bias_top),
                (third_bias_top_h, third_bias_top),
            )
        )
    ]
    for load in (loads[0], *smalls, *loads[1:]):
        load.start()

    loads[0].wait()
    for i in range(n_img):
        row = img_v[i]
        packed = [row[8 * k : 8 * k + 8] for k in range(c_mid // 8)]
        packed.append(jnp.zeros((8, 128 - width * (c_mid // 8)), F32))
        y_out[i] = jnp.concatenate(packed, axis=1)
    y_in[me_chan] = y_out[me_chan]

    pl.semaphore_wait(barrier, n_chan + n_rows - 2)
    y_copies = []
    for k, peer in enumerate(chan_peers):
        copy = pltpu.make_async_remote_copy(
            src_ref=y_out.at[peer],
            dst_ref=y_in.at[me_chan],
            send_sem=ys_sem.at[k],
            recv_sem=yr_sem.at[n_chan - 2 - k],
            device_id={"chan": peer},
            device_id_type=MESH,
        )
        copy.start()
        y_copies.append(copy)

    for load in smalls:
        load.wait()
    spread = jnp.where(
        iota2((32, c_mid), 0)
        == iota2((32, c_mid), 1) + jnp.where(iota2((32, c_mid), 1) >= half_m, 16 - half_m, 0),
        1.0,
        0.0,
    )
    src, lane = iota2((c_mid, 96), 0), lax.rem(iota2((c_mid, 96), 1), 32)
    plain = jnp.where(src == lane, 1.0, 0.0)
    padded = jnp.where(src + jnp.where(src >= half_m, 16 - half_m, 0) == lane, 1.0, 0.0)
    for s in range(steps_m):
        mix, const = mixing(
            lower_mid[s],
            upper_mid[s],
            diag_mid[s : s + 1],
            gain_mid[s : s + 1],
            shift_mid[s : s + 1],
            spread,
            plain if s == 0 else padded,
            64,
        )
        mix_m[s] = mix
        const_m[s] = jnp.where(iota2((32, 1), 0) == half_m, 1.0, const)
    src, lane = iota2((c_top, 192), 0), lax.rem(iota2((c_top, 192), 1), 64)
    squeezed_place = jnp.where(
        jnp.logical_and(lax.rem(lane, 16) < half_m, src == 4 * lax.rem(lane, 16) + lax.div(lane, 16)), 1.0, 0.0
    )
    src, lane = iota2((c_top, 144), 0), lax.rem(iota2((c_top, 144), 1), 48)
    top_place = jnp.where(src == lane, 1.0, 0.0)
    for s in range(steps_p):
        mix, const = mixing(
            lower_top[s],
            upper_top[s],
            diag_top[s : s + 1],
            gain_top[s : s + 1],
            shift_top[s : s + 1],
            None,
            squeezed_place if s == 0 else top_place,
            128 if s == 0 else 96,
        )
        if s == 0:
            mix_p0[...] = mix
        else:
            mix_p1[s - 1] = mix
        const_p[s] = const

    def prepare_mid(s):
        w1f_m[...] = jnp.zeros_like(w1f_m)
        for t in range(9):
            w1f_m[16 * t : 16 * t + half_m] = w1m[s, t].astype(F32)
        w1f_m[64 + half_m : 65 + half_m] = first_bias_mid[s : s + 1].astype(F32)
        w1m_t[s] = w1f_m[...].T.astype(BF16)
        w2m_t[s] = w2m[s].T
        b2m[s] = jnp.broadcast_to(second_bias_mid[s : s + 1], (128, b2m.shape[1])).T

    def prepare_top(s):
        w1f_p[9 * half_p :] = jnp.zeros((8, w1f_p.shape[1]), F32)
        w1f_p[: 9 * half_p] = w1p[s].astype(F32)
        w1f_p[9 * half_p : 9 * half_p + 1] = first_bias_top[s : s + 1].astype(F32)
        w1p_t[s] = w1f_p[...].T.astype(BF16)
        w2p_t[s] = w2p[s].T
        b2p[s] = jnp.broadcast_to(second_bias_top[s : s + 1], (128, b2p.shape[1])).T

    for load in loads[1:]:
        load.wait()
    for s in range(steps_m):
        prepare_mid(s)
    for s in range(steps_p):
        prepare_top(s)
    bias3_m = [column(third_bias_mid[s : s + 1]) for s in range(steps_m)]
    bias3_p = [column(third_bias_top[s : s + 1]) for s in range(steps_p)]

    for copy in y_copies:
        copy.wait_recv()
    groups = []
    for k in range(c_mid // 8):
        groups.append(jnp.concatenate([y_in[c][:, width * k : width * (k + 1)] for c in range(n_chan)], axis=1))
    own = jnp.concatenate([*groups, jnp.zeros((32 - c_mid, n_chan * width), F32)], axis=0)
    z_out[...] = own.astype(BF16)
    z_copies = []
    for k, d in enumerate((1, -1, 2, -2)):
        copy = pltpu.make_async_remote_copy(
            src_ref=z_out,
            dst_ref=z_in.at[k],
            send_sem=zs_sem.at[k],
            recv_sem=zr_sem.at[k],
            device_id={"rows": lax.rem(me_row + d + n_rows, n_rows)},
            device_id_type=MESH,
        )
        copy.start()
        z_copies.append(copy)
    for copy in z_copies:
        copy.wait_recv()
    state = jnp.concatenate([z_in[2].astype(F32), z_in[0].astype(F32), own, z_in[1].astype(F32), z_in[3].astype(F32)], axis=1)

    height = n_rows * n_chan
    partial = jnp.zeros((8, 128), F32)

    def folded(x):
        total = None
        for i in range(0, x.shape[0], 8):
            for j in range(0, x.shape[1], 128):
                piece = x[i : i + 8, j : j + 128]
                total = piece if total is None else total + piece
        return total

    first_row = me_row * n_chan - 2 * n_chan
    own_at = 2 * n_chan * width
    own_lanes = n_chan * width
    valid_m = iota2((16, own_lanes), 0) < half_m
    for s in range(steps_m):
        if s == 1:
            state = state[:, 4 * width : 36 * width]
            first_row = first_row + 4
            own_at = own_at - 4 * width
        length = state.shape[1]
        lane = iota2((1, length), 1)
        col, row = lax.rem(lane, width), lax.div(lane, width) + first_row
        u = apply_mix(state, mix_m[s], const_m[s])
        ua, updated, g = coupling(
            u,
            half_m,
            16,
            w1m_t.at[s],
            w2m_t.at[s],
            b2m.at[s],
            w3m.at[s],
            bias3_m[s],
            col >= 1,
            col <= width - 2,
            row >= 1,
            row <= height - 2,
            width,
            512,
            False,
        )
        state = jnp.concatenate([ua, updated], axis=0)
        mine = g[:, own_at : own_at + own_lanes]
        partial = partial + folded(jnp.where(valid_m, log_sigmoid(mine), 0.0))
    latent = jnp.where(valid_m, state[:16, own_at : own_at + own_lanes], 0.0)
    partial = partial + folded(-0.5 * latent * latent)

    for c in range(n_chan):
        piece = latent[:, width * c : width * (c + 1)]
        back_out[c] = jnp.concatenate([piece[:8], piece[8:], jnp.zeros((8, 128 - 2 * width), F32)], axis=1)
    back_in[me_chan] = back_out[me_chan]
    back_copies = []
    for k, peer in enumerate(chan_peers):
        copy = pltpu.make_async_remote_copy(
            src_ref=back_out.at[peer],
            dst_ref=back_in.at[me_chan],
            send_sem=bs_sem.at[k],
            recv_sem=br_sem.at[n_chan - 2 - k],
            device_id={"chan": peer},
            device_id_type=MESH,
        )
        copy.start()
        back_copies.append(copy)

    kept = state[16:, 4 * width : 28 * width]
    cols_p = width // 2
    lane = iota2((16, 128), 1)
    phase, rest = lax.div(lane, 32), lax.rem(lane, 32)
    pick = (2 * lax.div(rest, cols_p) + lax.div(phase, 2)) * width + 2 * lax.rem(rest, cols_p) + lax.rem(phase, 2)
    blocks = [
        jnp.take_along_axis(kept[:, 128 * k : 128 * k + 128], pick, axis=1) for k in range(kept.shape[1] // 128)
    ]
    phases = []
    for p in range(4):
        parts = [b[:, 32 * p : 32 * p + 32] for b in blocks]
        parts.append(jnp.zeros((16, 256 - 32 * len(blocks)), F32))
        phases.append(jnp.concatenate(parts, axis=1))
    state = jnp.concatenate(phases, axis=0)

    rows_p = n_chan // 2
    first_row = me_row * rows_p - rows_p
    length = state.shape[1]
    lane = iota2((1, length), 1)
    col, row = lax.rem(lane, cols_p), lax.div(lane, cols_p) + first_row
    own_at = rows_p * cols_p
    mine_p = jnp.logical_and(lane >= own_at, lane < 2 * own_at)
    for s in range(steps_p):
        u = apply_mix(state, mix_p0[...] if s == 0 else mix_p1[s - 1], const_p[s])
        ua, updated, g = coupling(
            u,
            half_p,
            half_p,
            w1p_t.at[s],
            w2p_t.at[s],
            b2p.at[s],
            w3p.at[s],
            bias3_p[s],
            col >= 1,
            col <= cols_p - 2,
            row >= 1,
            row <= height // 2 - 2,
            cols_p,
            256,
            True,
        )
        state = jnp.concatenate([ua, updated], axis=0)
        partial = partial + folded(jnp.where(mine_p, log_sigmoid(g), 0.0))
    partial = partial + folded(jnp.where(mine_p, -0.5 * state * state, 0.0))
    ll_out[...] = jnp.sum(partial, axis=0, keepdims=True)
    ll_copies = []
    for k, peer in enumerate(row_peers):
        copy = pltpu.make_async_remote_copy(
            src_ref=ll_out,
            dst_ref=ll_in.at[n_rows - 2 - k],
            send_sem=ls_sem.at[k],
            recv_sem=lr_sem.at[n_rows - 2 - k],
            device_id={"rows": peer},
            device_id_type=MESH,
        )
        copy.start()
        ll_copies.append(copy)

    latent_top[...] = state[:, :128].T[own_at : 2 * own_at]
    for copy in back_copies:
        copy.wait_recv()
    for c in range(n_img):
        piece = back_in[c]
        latent_mid[half_m * c : half_m * c + 8] = piece[:, :width]
        latent_mid[half_m * c + 8 : half_m * (c + 1)] = piece[: half_m - 8, width : 2 * width]
    cells = height * width
    const = sum(
        (
            cells * (jnp.sum(gain_mid[...]) + jnp.sum(diag_mid[...])),
            (cells // 4) * (jnp.sum(gain_top[...]) + jnp.sum(diag_top[...])),
        )
    )
    for copy in ll_copies:
        copy.wait_recv()
    total = ll_out[...]
    for k in range(n_rows - 1):
        total = total + ll_in[k]
    scale = 1.0 / (c_mid * cells)
    loglik[...] = jnp.broadcast_to((jnp.sum(total) + const) * scale - 0.5 * log_two_pi, (1, 128))
    for copy in (*y_copies, *z_copies, *back_copies, *ll_copies):
        copy.wait_send()


def write_out(*refs):
    sem = refs[-1]
    copies = [pltpu.make_async_copy(refs[k], refs[3 + k], sem.at[k]) for k in range(3)]
    for copy in copies:
        copy.start()
    for copy in copies:
        copy.wait()


def body(
    images,
    shift_mid,
    gain_mid,
    lower_mid,
    upper_mid,
    diag_mid,
    first_mid,
    first_bias_mid,
    second_mid,
    second_bias_mid,
    third_mid,
    third_bias_mid,
    shift_top,
    gain_top,
    lower_top,
    upper_top,
    diag_top,
    first_top,
    first_bias_top,
    second_top,
    second_bias_top,
    third_top,
    third_bias_top,
):
    n_rows, n_chan = lax.axis_size("rows"), lax.axis_size("chan")
    n_img, c_mid, _, width = images.shape
    hid = second_mid.shape[1]
    steps_m, steps_p = shift_mid.shape[0], shift_top.shape[0]
    c_top = shift_top.shape[1]
    half_m, half_p = c_mid // 2, c_top // 2
    images = images.reshape(n_img, c_mid, width)
    third_mid = third_mid.transpose(0, 1, 3, 2).reshape(steps_m, 9 * c_mid, hid)
    third_top = third_top.transpose(0, 1, 3, 2).reshape(steps_p, 9 * c_top, hid)
    first_top = first_top.reshape(steps_p, 9 * half_p, hid)
    big = pl.BlockSpec(memory_space=pltpu.HBM)
    small = pl.BlockSpec(memory_space=pltpu.VMEM)
    rows_p = n_chan // 2
    vmem = pltpu.VMEM
    small_args = (shift_mid, gain_mid, lower_mid, upper_mid, diag_mid, first_bias_mid, second_bias_mid, third_bias_mid, shift_top, gain_top, lower_top, upper_top, diag_top, first_bias_top, second_bias_top, third_bias_top)
    dma = pltpu.SemaphoreType.DMA
    found = pl.pallas_call(
        functools.partial(kernel, n_rows, n_chan),
        out_shape=(
            vmem((n_img * half_m, width), F32),
            vmem((rows_p * width // 2, c_top), F32),
            vmem((1, 128), F32),
        ),
        in_specs=[big] * 23,
        out_specs=(small, small, small),
        scratch_shapes=[
            vmem((n_img, c_mid, width), F32),
            vmem((steps_m, 9, half_m, hid), BF16),
            vmem((steps_m, hid, hid), BF16),
            vmem((steps_m, 9 * c_mid, hid), BF16),
            vmem((steps_p, 9 * half_p, hid), BF16),
            vmem((steps_p, hid, hid), BF16),
            vmem((steps_p, 9 * c_top, hid), BF16),
            vmem((144, hid), F32),
            vmem((9 * half_p + 8, hid), F32),
            vmem((steps_m, hid, 144), BF16),
            vmem((steps_m, hid, hid), BF16),
            vmem((steps_p, hid, 9 * half_p + 8), BF16),
            vmem((steps_p, hid, hid), BF16),
            vmem((steps_m, hid, 128), F32),
            vmem((steps_p, hid, 128), F32),
            vmem((steps_m, 32, 96), BF16),
            vmem((c_top, 192), BF16),
            vmem((steps_p - 1, c_top, 144), BF16),
            vmem((steps_m, 32, 1), F32),
            vmem((steps_p, c_top, 1), F32),
            vmem((n_chan, 8, 128), F32),
            vmem((n_chan, 8, 128), F32),
            vmem((32, n_chan * width), BF16),
            vmem((4, 32, n_chan * width), BF16),
            vmem((n_chan, 8, 128), F32),
            vmem((n_chan, 8, 128), F32),
            vmem((1, 128), F32),
            vmem((n_rows - 1, 1, 128), F32),
            *(vmem(a.shape, a.dtype) for a in small_args),
            dma((7,)),
            dma((len(small_args),)),
            dma((n_chan - 1,)),
            dma((n_chan - 1,)),
            dma((4,)),
            dma((4,)),
            dma((n_chan - 1,)),
            dma((n_chan - 1,)),
            dma((n_rows - 1,)),
            dma((n_rows - 1,)),
        ],
        compiler_params=pltpu.CompilerParams(
            collective_id=0, has_side_effects=True, vmem_limit_bytes=67043328 - 100 * 1024
        ),
    )(
        images,
        shift_mid,
        gain_mid,
        lower_mid,
        upper_mid,
        diag_mid,
        first_mid,
        first_bias_mid,
        second_mid,
        second_bias_mid,
        third_mid,
        third_bias_mid,
        shift_top,
        gain_top,
        lower_top,
        upper_top,
        diag_top,
        first_top,
        first_bias_top,
        second_top,
        second_bias_top,
        third_top,
        third_bias_top,
    )
    latent_mid, latent_top, loglik = pl.pallas_call(
        write_out,
        out_shape=tuple(jax.ShapeDtypeStruct(x.shape, x.dtype) for x in found),
        in_specs=[small] * 3,
        out_specs=(pl.BlockSpec(memory_space=pltpu.HBM),) * 3,
        scratch_shapes=[dma((3,))],
        compiler_params=pltpu.CompilerParams(vmem_limit_bytes=1024 * 1024),
    )(*found)
    latent_mid = latent_mid.reshape(n_img, half_m, 1, width)
    latent_top = latent_top.reshape(1, rows_p, width // 2, c_top).transpose(0, 3, 1, 2)
    return latent_mid, latent_top, loglik[0, :1]


def solution(mesh):
    placed = (P("batch", None, ("rows", "chan"), None),) + (P(),) * 22
    return jax.shard_map(
        body,
        mesh=mesh,
        in_specs=placed,
        out_specs=(
            P("batch", None, ("rows", "chan"), None),
            P(("batch", "chan"), None, "rows", None),
            P(("batch", "chan")),
        ),
        check_vma=False,
    )
```

```python
import functools
import math

import jax
import jax.numpy as jnp
from jax import lax
from jax.experimental import pallas as pl
from jax.experimental.pallas import tpu as pltpu
from jax.sharding import PartitionSpec as P

MESH = pl.DeviceIdType.MESH
F32 = jnp.float32
BF16 = jnp.bfloat16
HI = lax.Precision.HIGHEST
log_two_pi = math.log(2.0 * math.pi)


def iota2(shape, dim):
    return lax.broadcasted_iota(jnp.int32, shape, dim)


def mixing(lower, upper, diag, gain, shift, spread, place, split_at):
    n = lower.shape[0]
    r, c = iota2((n, n), 0), iota2((n, n), 1)
    low = jnp.where(r > c, lower, jnp.where(r == c, 1.0, 0.0))
    up = jnp.where(c > r, upper, jnp.where(r == c, jnp.exp(diag), 0.0)) * jnp.exp(gain)
    both = jnp.dot(low, up, precision=HI, preferred_element_type=F32)
    if spread is not None:
        both = jnp.dot(spread, both, precision=HI, preferred_element_type=F32)
    const = jnp.sum(both * shift, axis=1, keepdims=True)
    wide = jnp.dot(both, place, precision=HI, preferred_element_type=F32)
    high = wide.astype(BF16).astype(F32)
    lane = iota2(wide.shape, 1)
    return jnp.where(lane < split_at, high, wide - high).astype(BF16), const


def column(row):
    n = row.shape[1]
    eye = iota2((n, n), 0) == iota2((n, n), 1)
    return jnp.sum(jnp.where(eye, jnp.broadcast_to(row, (n, n)), 0.0), axis=1, keepdims=True)


def apply_mix(state, mix, const):
    high = state.astype(BF16)
    low = (state - high.astype(F32)).astype(BF16)
    stacked = jnp.concatenate([high, low, high], axis=0)
    return jnp.dot(mix, stacked, preferred_element_type=F32) + const


def dot(w, x):
    if x.shape[1] > 256:
        return jnp.dot(w[...], x, preferred_element_type=F32)
    rows = w.shape[0]
    cut = rows // 16 // 2 * 16
    return jnp.concatenate(
        [
            jnp.dot(w[:cut], x, preferred_element_type=F32),
            jnp.dot(w[cut:], x, preferred_element_type=F32),
        ],
        axis=0,
    )


def shifted(x, by, ok):
    pieces = [pltpu.roll(x[:, at : at + 128], by, 1) for at in range(0, x.shape[1], 128)]
    return jnp.where(ok, jnp.concatenate(pieces, axis=1), 0.0)


def from_left(x, ok):
    return shifted(x, 1, ok)


def from_right(x, ok):
    return shifted(x, 127, ok)


def coupling(u, half, pad, w1t, w2t, bias2, w3, bias3, left_ok, right_ok, up_ok, down_ok, inside, cols, tile, extra):
    length = u.shape[1]
    ua, ub = u[:pad], u[pad : 2 * pad]
    q = jnp.where(inside, ua.astype(BF16).astype(F32), 0.0)
    sides = (from_left(q, left_ok), q, from_right(q, right_ok))
    above = [pltpu.roll(s, cols, 1) for s in sides]
    below = [pltpu.roll(s, length - cols, 1) for s in sides]
    stack = [*above, *sides, *below]
    if extra:
        stack.append(jnp.ones((8, length), F32))
    patches = jnp.concatenate(stack, axis=0).astype(BF16)
    pieces = []
    for at in range(0, length, tile):
        size = min(tile, length - at)
        h = dot(w1t, patches[:, at : at + size])
        h = jnp.maximum(h, 0.0).astype(BF16)
        h = dot(w2t, h)
        b = bias2[...]
        b = jnp.concatenate([b] * (size // 128), axis=1)
        h = jnp.maximum(h + b, 0.0).astype(BF16)
        pieces.append(dot(w3, h))
    taps = jnp.concatenate(pieces, axis=1) if len(pieces) > 1 else pieces[0]
    both = 2 * half
    rows = []
    for dr in range(3):
        a, b, c = (taps[(dr * 3 + dc) * both : (dr * 3 + dc + 1) * both] for dc in range(3))
        rows.append(
            b
            + from_left(a, left_ok)
            + from_right(c, right_ok)
        )
    out = (
        rows[1]
        + jnp.where(up_ok, pltpu.roll(rows[0], cols, 1), 0.0)
        + jnp.where(down_ok, pltpu.roll(rows[2], length - cols, 1), 0.0)
        + bias3
    )
    g, t = out[:half] + 2.0, out[half:]
    if pad > half:
        zeros = jnp.zeros((pad - half, length), F32)
        g, t = jnp.concatenate([g, zeros], axis=0), jnp.concatenate([t, zeros], axis=0)
    return ua, (ub + t) * jax.nn.sigmoid(g), g


def log_sigmoid(g):
    return jnp.minimum(g, 0.0) - jnp.log1p(jnp.exp(-jnp.abs(g)))


def kernel(
    n_rows,
    n_chan,
    images,
    shift_mid_h,
    gain_mid_h,
    lower_mid_h,
    upper_mid_h,
    diag_mid_h,
    first_mid,
    first_bias_mid_h,
    second_mid,
    second_bias_mid_h,
    third_mid,
    third_bias_mid_h,
    shift_top_h,
    gain_top_h,
    lower_top_h,
    upper_top_h,
    diag_top_h,
    first_top,
    first_bias_top_h,
    second_top,
    second_bias_top_h,
    third_top,
    third_bias_top_h,
    latent_mid,
    latent_top,
    loglik,
    img_v,
    w1m,
    w2m,
    w3m,
    w1p,
    w2p,
    w3p,
    w1f_m,
    w1f_p,
    w1m_t,
    w2m_t,
    w1p_t,
    w2p_t,
    b2m,
    b2p,
    mix_m,
    mix_p0,
    mix_p1,
    const_m,
    const_p,
    y_out,
    y_in,
    z_out,
    z_in,
    k_out,
    k_in,
    back_out,
    back_in,
    ll_out,
    ll_in,
    shift_mid,
    gain_mid,
    lower_mid,
    upper_mid,
    diag_mid,
    first_bias_mid,
    second_bias_mid,
    third_bias_mid,
    shift_top,
    gain_top,
    lower_top,
    upper_top,
    diag_top,
    first_bias_top,
    second_bias_top,
    third_bias_top,
    load_sem,
    image_sem,
    small_sem,
    ys_sem,
    yr_sem,
    zs_sem,
    zr_sem,
    ks_sem,
    kr_sem,
    bs_sem,
    br_sem,
    ls_sem,
    lr_sem,
):
    me_row, me_chan = lax.axis_index("rows"), lax.axis_index("chan")
    steps_m, steps_p = shift_mid.shape[0], shift_top.shape[0]
    n_img, c_mid, width = img_v.shape
    half_m = c_mid // 2
    c_top = shift_top.shape[1]
    half_p = c_top // 2

    image_load = pltpu.make_async_copy(images, img_v, image_sem)
    image_load.start()
    barrier = pltpu.get_barrier_semaphore()
    far = sorted(range(1, n_chan), key=lambda k: -min(k, n_chan - k))
    chan_peers = [lax.rem(me_chan + k, n_chan) for k in range(1, n_chan)]
    row_peers = [lax.rem(me_row + k, n_rows) for k in range(1, n_rows)]
    near = sorted({d % n_rows for d in (1, -1, 2, -2)} - {0})
    for k in far:
        pl.semaphore_signal(barrier, inc=1, device_id={"chan": chan_peers[k - 1]}, device_id_type=MESH)
    for d in near:
        pl.semaphore_signal(barrier, inc=1, device_id={"rows": row_peers[d - 1]}, device_id_type=MESH)

    loads = [
        pltpu.make_async_copy(src, dst, load_sem.at[k])
        for k, (src, dst) in enumerate(
            (
                (first_mid, w1m),
                (second_mid, w2m),
                (third_mid, w3m),
                (first_top, w1p),
                (second_top, w2p),
                (third_top, w3p),
            )
        )
    ]
    smalls = [
        pltpu.make_async_copy(src, dst, small_sem.at[k])
        for k, (src, dst) in enumerate(
            (
                (shift_mid_h, shift_mid),
                (gain_mid_h, gain_mid),
                (lower_mid_h, lower_mid),
                (upper_mid_h, upper_mid),
                (diag_mid_h, diag_mid),
                (first_bias_mid_h, first_bias_mid),
                (second_bias_mid_h, second_bias_mid),
                (third_bias_mid_h, third_bias_mid),
                (shift_top_h, shift_top),
                (gain_top_h, gain_top),
                (lower_top_h, lower_top),
                (upper_top_h, upper_top),
                (diag_top_h, diag_top),
                (first_bias_top_h, first_bias_top),
                (second_bias_top_h, second_bias_top),
                (third_bias_top_h, third_bias_top),
            )
        )
    ]
    for load in (*smalls, *loads):
        load.start()

    image_load.wait()
    for i in range(n_img):
        row = img_v[i]
        packed = [row[8 * k : 8 * k + 8] for k in range(c_mid // 8)]
        packed.append(jnp.zeros((8, 128 - width * (c_mid // 8)), F32))
        y_out[i] = jnp.concatenate(packed, axis=1)
    y_in[me_chan] = y_out[me_chan]

    pl.semaphore_wait(barrier, n_chan - 1 + len(near))
    y_copies = []
    for k, peer in enumerate(chan_peers):
        copy = pltpu.make_async_remote_copy(
            src_ref=y_out.at[peer],
            dst_ref=y_in.at[me_chan],
            send_sem=ys_sem.at[k],
            recv_sem=yr_sem.at[n_chan - 2 - k],
            device_id={"chan": peer},
            device_id_type=MESH,
        )
        copy.start()
        y_copies.append(copy)

    for load in smalls:
        load.wait()
    spread = jnp.where(
        iota2((32, c_mid), 0)
        == iota2((32, c_mid), 1) + jnp.where(iota2((32, c_mid), 1) >= half_m, 16 - half_m, 0),
        1.0,
        0.0,
    )
    src, lane = iota2((c_mid, 96), 0), lax.rem(iota2((c_mid, 96), 1), 32)
    plain = jnp.where(src == lane, 1.0, 0.0)
    padded = jnp.where(src + jnp.where(src >= half_m, 16 - half_m, 0) == lane, 1.0, 0.0)
    for s in range(steps_m):
        mix, const = mixing(
            lower_mid[s],
            upper_mid[s],
            diag_mid[s : s + 1],
            gain_mid[s : s + 1],
            shift_mid[s : s + 1],
            spread,
            plain if s == 0 else padded,
            64,
        )
        mix_m[s] = mix
        const_m[s] = jnp.where(iota2((32, 1), 0) == half_m, 1.0, const)
    src, lane = iota2((c_top, 192), 0), lax.rem(iota2((c_top, 192), 1), 64)
    squeezed_place = jnp.where(
        jnp.logical_and(lax.rem(lane, 16) < half_m, src == 4 * lax.rem(lane, 16) + lax.div(lane, 16)), 1.0, 0.0
    )
    src, lane = iota2((c_top, 144), 0), lax.rem(iota2((c_top, 144), 1), 48)
    top_place = jnp.where(src == lane, 1.0, 0.0)
    for s in range(steps_p):
        mix, const = mixing(
            lower_top[s],
            upper_top[s],
            diag_top[s : s + 1],
            gain_top[s : s + 1],
            shift_top[s : s + 1],
            None,
            squeezed_place if s == 0 else top_place,
            128 if s == 0 else 96,
        )
        if s == 0:
            mix_p0[...] = mix
        else:
            mix_p1[s - 1] = mix
        const_p[s] = const

    def prepare_mid(s):
        w1f_m[...] = jnp.zeros_like(w1f_m)
        for t in range(9):
            w1f_m[16 * t : 16 * t + half_m] = w1m[s, t].astype(F32)
        w1f_m[64 + half_m : 65 + half_m] = first_bias_mid[s : s + 1].astype(F32)
        w1m_t[s] = w1f_m[...].T.astype(BF16)
        w2m_t[s] = w2m[s].T
        b2m[s] = jnp.broadcast_to(second_bias_mid[s : s + 1], (128, b2m.shape[1])).T

    def prepare_top(s):
        w1f_p[9 * half_p :] = jnp.zeros((8, w1f_p.shape[1]), F32)
        w1f_p[: 9 * half_p] = w1p[s].astype(F32)
        w1f_p[9 * half_p : 9 * half_p + 1] = first_bias_top[s : s + 1].astype(F32)
        w1p_t[s] = w1f_p[...].T.astype(BF16)
        w2p_t[s] = w2p[s].T
        b2p[s] = jnp.broadcast_to(second_bias_top[s : s + 1], (128, b2p.shape[1])).T

    for load in loads:
        load.wait()
    for s in range(steps_m):
        prepare_mid(s)
    for s in range(steps_p):
        prepare_top(s)
    bias3_m = [column(third_bias_mid[s : s + 1]) for s in range(steps_m)]
    bias3_p = [column(third_bias_top[s : s + 1]) for s in range(steps_p)]

    for copy in y_copies:
        copy.wait_recv()
    groups = []
    for k in range(c_mid // 8):
        groups.append(jnp.concatenate([y_in[c][:, width * k : width * (k + 1)] for c in range(n_chan)], axis=1))
    own = jnp.concatenate([*groups, jnp.zeros((32 - c_mid, n_chan * width), F32)], axis=0)
    z_out[...] = own.astype(BF16)
    z_copies = []
    for k, d in enumerate((1, -1)):
        copy = pltpu.make_async_remote_copy(
            src_ref=z_out,
            dst_ref=z_in.at[k],
            send_sem=zs_sem.at[k],
            recv_sem=zr_sem.at[k],
            device_id={"rows": lax.rem(me_row + d + n_rows, n_rows)},
            device_id_type=MESH,
        )
        copy.start()
        z_copies.append(copy)
    for copy in z_copies:
        copy.wait_recv()
    state = jnp.concatenate([z_in[0].astype(F32), own, z_in[1].astype(F32)], axis=1)

    height = n_rows * n_chan
    partial = jnp.zeros((8, 128), F32)

    def folded(x):
        total = None
        for i in range(0, x.shape[0], 8):
            for j in range(0, x.shape[1], 128):
                piece = x[i : i + 8, j : j + 128]
                total = piece if total is None else total + piece
        return total

    first_row = me_row * n_chan - n_chan
    own_at = n_chan * width
    own_lanes = n_chan * width
    valid_m = iota2((16, own_lanes), 0) < half_m
    for s in range(steps_m):
        if s == 1:
            state = state[:, 4 * width : 20 * width]
            first_row = first_row + 4
            own_at = own_at - 4 * width
        length = state.shape[1]
        lane = iota2((1, length), 1)
        col, row = lax.rem(lane, width), lax.div(lane, width) + first_row
        u = apply_mix(state, mix_m[s], const_m[s])
        ua, updated, g = coupling(
            u,
            half_m,
            16,
            w1m_t.at[s],
            w2m_t.at[s],
            b2m.at[s],
            w3m.at[s],
            bias3_m[s],
            col >= 1,
            col <= width - 2,
            row >= 1,
            row <= height - 2,
            jnp.logical_and(row >= 0, row < height),
            width,
            512,
            False,
        )
        state = jnp.concatenate([ua, updated], axis=0)
        mine = g[:, own_at : own_at + own_lanes]
        partial = partial + folded(jnp.where(valid_m, log_sigmoid(mine), 0.0))
    kept = state[16:, own_at : own_at + own_lanes]
    k_out[...] = kept.astype(BF16)
    k_copies = []
    for k, d in enumerate((1, -1)):
        copy = pltpu.make_async_remote_copy(
            src_ref=k_out,
            dst_ref=k_in.at[k],
            send_sem=ks_sem.at[k],
            recv_sem=kr_sem.at[k],
            device_id={"rows": lax.rem(me_row + d + n_rows, n_rows)},
            device_id_type=MESH,
        )
        copy.start()
        k_copies.append(copy)
    latent = jnp.where(valid_m, state[:16, own_at : own_at + own_lanes], 0.0)
    partial = partial + folded(-0.5 * latent * latent)

    for c in range(n_chan):
        piece = latent[:, width * c : width * (c + 1)]
        back_out[c] = jnp.concatenate([piece[:8], piece[8:], jnp.zeros((8, 128 - 2 * width), F32)], axis=1)
    back_in[me_chan] = back_out[me_chan]
    back_copies = []
    for k, peer in enumerate(chan_peers):
        copy = pltpu.make_async_remote_copy(
            src_ref=back_out.at[peer],
            dst_ref=back_in.at[me_chan],
            send_sem=bs_sem.at[k],
            recv_sem=br_sem.at[n_chan - 2 - k],
            device_id={"chan": peer},
            device_id_type=MESH,
        )
        copy.start()
        back_copies.append(copy)

    cols_p = width // 2
    lane = iota2((16, 128), 1)
    phase, rest = lax.div(lane, 32), lax.rem(lane, 32)
    pick = (2 * lax.div(rest, cols_p) + lax.div(phase, 2)) * width + 2 * lax.rem(rest, cols_p) + lax.rem(phase, 2)
    for copy in k_copies:
        copy.wait_recv()
    kept = jnp.concatenate([k_in[0].astype(F32), kept, k_in[1].astype(F32)], axis=1)
    blocks = [
        jnp.take_along_axis(kept[:, 128 * k : 128 * k + 128], pick, axis=1) for k in range(kept.shape[1] // 128)
    ]
    phases = []
    for p in range(4):
        parts = [b[:, 32 * p : 32 * p + 32] for b in blocks]
        parts.append(jnp.zeros((16, 256 - 32 * len(blocks)), F32))
        phases.append(jnp.concatenate(parts, axis=1))
    state = jnp.concatenate(phases, axis=0)

    rows_p = n_chan // 2
    first_row = me_row * rows_p - rows_p
    length = state.shape[1]
    lane = iota2((1, length), 1)
    col, row = lax.rem(lane, cols_p), lax.div(lane, cols_p) + first_row
    own_at = rows_p * cols_p
    mine_p = jnp.logical_and(lane >= own_at, lane < 2 * own_at)
    for s in range(steps_p):
        u = apply_mix(state, mix_p0[...] if s == 0 else mix_p1[s - 1], const_p[s])
        ua, updated, g = coupling(
            u,
            half_p,
            half_p,
            w1p_t.at[s],
            w2p_t.at[s],
            b2p.at[s],
            w3p.at[s],
            bias3_p[s],
            col >= 1,
            col <= cols_p - 2,
            row >= 1,
            row <= height // 2 - 2,
            jnp.logical_and(row >= 0, row < height // 2),
            cols_p,
            256,
            True,
        )
        state = jnp.concatenate([ua, updated], axis=0)
        partial = partial + folded(jnp.where(mine_p, log_sigmoid(g), 0.0))
    partial = partial + folded(jnp.where(mine_p, -0.5 * state * state, 0.0))
    ll_out[...] = jnp.sum(partial, axis=0, keepdims=True)
    ll_copies = []
    for k, peer in enumerate(row_peers):
        copy = pltpu.make_async_remote_copy(
            src_ref=ll_out,
            dst_ref=ll_in.at[n_rows - 2 - k],
            send_sem=ls_sem.at[k],
            recv_sem=lr_sem.at[n_rows - 2 - k],
            device_id={"rows": peer},
            device_id_type=MESH,
        )
        copy.start()
        ll_copies.append(copy)

    latent_top[...] = state[:, :128].T[own_at : 2 * own_at]
    for copy in back_copies:
        copy.wait_recv()
    for c in range(n_img):
        piece = back_in[c]
        latent_mid[half_m * c : half_m * c + 8] = piece[:, :width]
        latent_mid[half_m * c + 8 : half_m * (c + 1)] = piece[: half_m - 8, width : 2 * width]
    cells = height * width
    const = sum(
        (
            cells * (jnp.sum(gain_mid[...]) + jnp.sum(diag_mid[...])),
            (cells // 4) * (jnp.sum(gain_top[...]) + jnp.sum(diag_top[...])),
        )
    )
    for copy in ll_copies:
        copy.wait_recv()
    total = ll_out[...]
    for k in range(n_rows - 1):
        total = total + ll_in[k]
    scale = 1.0 / (c_mid * cells)
    loglik[...] = jnp.broadcast_to((jnp.sum(total) + const) * scale - 0.5 * log_two_pi, (1, 128))
    for copy in (*y_copies, *z_copies, *k_copies, *back_copies, *ll_copies):
        copy.wait_send()


def write_out(*refs):
    sem = refs[-1]
    copies = [pltpu.make_async_copy(refs[k], refs[3 + k], sem.at[k]) for k in range(3)]
    for copy in copies:
        copy.start()
    for copy in copies:
        copy.wait()


def body(
    images,
    shift_mid,
    gain_mid,
    lower_mid,
    upper_mid,
    diag_mid,
    first_mid,
    first_bias_mid,
    second_mid,
    second_bias_mid,
    third_mid,
    third_bias_mid,
    shift_top,
    gain_top,
    lower_top,
    upper_top,
    diag_top,
    first_top,
    first_bias_top,
    second_top,
    second_bias_top,
    third_top,
    third_bias_top,
):
    n_rows, n_chan = lax.axis_size("rows"), lax.axis_size("chan")
    n_img, c_mid, _, width = images.shape
    hid = second_mid.shape[1]
    steps_m, steps_p = shift_mid.shape[0], shift_top.shape[0]
    c_top = shift_top.shape[1]
    half_m, half_p = c_mid // 2, c_top // 2
    images = images.reshape(n_img, c_mid, width)
    third_mid = third_mid.transpose(0, 1, 3, 2).reshape(steps_m, 9 * c_mid, hid)
    third_top = third_top.transpose(0, 1, 3, 2).reshape(steps_p, 9 * c_top, hid)
    first_top = first_top.reshape(steps_p, 9 * half_p, hid)
    big = pl.BlockSpec(memory_space=pltpu.HBM)
    small = pl.BlockSpec(memory_space=pltpu.VMEM)
    rows_p = n_chan // 2
    vmem = pltpu.VMEM
    small_args = (shift_mid, gain_mid, lower_mid, upper_mid, diag_mid, first_bias_mid, second_bias_mid, third_bias_mid, shift_top, gain_top, lower_top, upper_top, diag_top, first_bias_top, second_bias_top, third_bias_top)
    dma = pltpu.SemaphoreType.DMA
    found = pl.pallas_call(
        functools.partial(kernel, n_rows, n_chan),
        out_shape=(
            vmem((n_img * half_m, width), F32),
            vmem((rows_p * width // 2, c_top), F32),
            vmem((1, 128), F32),
        ),
        in_specs=[big] * 23,
        out_specs=(small, small, small),
        scratch_shapes=[
            vmem((n_img, c_mid, width), F32),
            vmem((steps_m, 9, half_m, hid), BF16),
            vmem((steps_m, hid, hid), BF16),
            vmem((steps_m, 9 * c_mid, hid), BF16),
            vmem((steps_p, 9 * half_p, hid), BF16),
            vmem((steps_p, hid, hid), BF16),
            vmem((steps_p, 9 * c_top, hid), BF16),
            vmem((144, hid), F32),
            vmem((9 * half_p + 8, hid), F32),
            vmem((steps_m, hid, 144), BF16),
            vmem((steps_m, hid, hid), BF16),
            vmem((steps_p, hid, 9 * half_p + 8), BF16),
            vmem((steps_p, hid, hid), BF16),
            vmem((steps_m, hid, 128), F32),
            vmem((steps_p, hid, 128), F32),
            vmem((steps_m, 32, 96), BF16),
            vmem((c_top, 192), BF16),
            vmem((steps_p - 1, c_top, 144), BF16),
            vmem((steps_m, 32, 1), F32),
            vmem((steps_p, c_top, 1), F32),
            vmem((n_chan, 8, 128), F32),
            vmem((n_chan, 8, 128), F32),
            vmem((32, n_chan * width), BF16),
            vmem((2, 32, n_chan * width), BF16),
            vmem((16, n_chan * width), BF16),
            vmem((2, 16, n_chan * width), BF16),
            vmem((n_chan, 8, 128), F32),
            vmem((n_chan, 8, 128), F32),
            vmem((1, 128), F32),
            vmem((n_rows - 1, 1, 128), F32),
            *(vmem(a.shape, a.dtype) for a in small_args),
            dma((6,)),
            dma(()),
            dma((len(small_args),)),
            dma((n_chan - 1,)),
            dma((n_chan - 1,)),
            dma((2,)),
            dma((2,)),
            dma((2,)),
            dma((2,)),
            dma((n_chan - 1,)),
            dma((n_chan - 1,)),
            dma((n_rows - 1,)),
            dma((n_rows - 1,)),
        ],
        compiler_params=pltpu.CompilerParams(
            collective_id=0, has_side_effects=True, vmem_limit_bytes=67043328 - 100 * 1024
        ),
    )(
        images,
        shift_mid,
        gain_mid,
        lower_mid,
        upper_mid,
        diag_mid,
        first_mid,
        first_bias_mid,
        second_mid,
        second_bias_mid,
        third_mid,
        third_bias_mid,
        shift_top,
        gain_top,
        lower_top,
        upper_top,
        diag_top,
        first_top,
        first_bias_top,
        second_top,
        second_bias_top,
        third_top,
        third_bias_top,
    )
    latent_mid, latent_top, loglik = pl.pallas_call(
        write_out,
        out_shape=tuple(jax.ShapeDtypeStruct(x.shape, x.dtype) for x in found),
        in_specs=[small] * 3,
        out_specs=(pl.BlockSpec(memory_space=pltpu.HBM),) * 3,
        scratch_shapes=[dma((3,))],
        compiler_params=pltpu.CompilerParams(vmem_limit_bytes=1024 * 1024),
    )(*found)
    latent_mid = latent_mid.reshape(n_img, half_m, 1, width)
    latent_top = latent_top.reshape(1, rows_p, width // 2, c_top).transpose(0, 3, 1, 2)
    return latent_mid, latent_top, loglik[0, :1]


def solution(mesh):
    placed = (P("batch", None, ("rows", "chan"), None),) + (P(),) * 22
    return jax.shard_map(
        body,
        mesh=mesh,
        in_specs=placed,
        out_specs=(
            P("batch", None, ("rows", "chan"), None),
            P(("batch", "chan"), None, "rows", None),
            P(("batch", "chan")),
        ),
        check_vma=False,
    )
```

```python
import functools
import math

import jax
import jax.numpy as jnp
from jax import lax
from jax.experimental import pallas as pl
from jax.experimental.pallas import tpu as pltpu
from jax.sharding import PartitionSpec as P

MESH = pl.DeviceIdType.MESH
F32 = jnp.float32
BF16 = jnp.bfloat16
HI = lax.Precision.HIGHEST
log_two_pi = math.log(2.0 * math.pi)


def iota2(shape, dim):
    return lax.broadcasted_iota(jnp.int32, shape, dim)


def mixing(lower, upper, diag, gain, shift, spread, place, split_at):
    n = lower.shape[0]
    r, c = iota2((n, n), 0), iota2((n, n), 1)
    low = jnp.where(r > c, lower, jnp.where(r == c, 1.0, 0.0))
    up = jnp.where(c > r, upper, jnp.where(r == c, jnp.exp(diag), 0.0)) * jnp.exp(gain)
    both = jnp.dot(low, up, precision=HI, preferred_element_type=F32)
    if spread is not None:
        both = jnp.dot(spread, both, precision=HI, preferred_element_type=F32)
    const = jnp.sum(both * shift, axis=1, keepdims=True)
    wide = jnp.dot(both, place, precision=HI, preferred_element_type=F32)
    high = wide.astype(BF16).astype(F32)
    lane = iota2(wide.shape, 1)
    return jnp.where(lane < split_at, high, wide - high).astype(BF16), const


def column(row):
    n = row.shape[1]
    eye = iota2((n, n), 0) == iota2((n, n), 1)
    return jnp.sum(jnp.where(eye, jnp.broadcast_to(row, (n, n)), 0.0), axis=1, keepdims=True)


def apply_mix(state, mix, const):
    high = state.astype(BF16)
    low = (state - high.astype(F32)).astype(BF16)
    stacked = jnp.concatenate([high, low, high], axis=0)
    return jnp.dot(mix, stacked, preferred_element_type=F32) + const


def dot(w, x):
    if x.shape[1] > 256:
        return jnp.dot(w[...], x, preferred_element_type=F32)
    rows = w.shape[0]
    cut = rows // 16 // 2 * 16
    return jnp.concatenate(
        [
            jnp.dot(w[:cut], x, preferred_element_type=F32),
            jnp.dot(w[cut:], x, preferred_element_type=F32),
        ],
        axis=0,
    )


def shifted(x, by, ok):
    pieces = [pltpu.roll(x[:, at : at + 128], by, 1) for at in range(0, x.shape[1], 128)]
    return jnp.where(ok, jnp.concatenate(pieces, axis=1), 0.0)


def from_left(x, ok):
    return shifted(x, 1, ok)


def from_right(x, ok):
    return shifted(x, 127, ok)


def coupling(u, half, pad, w1t, w2t, bias2, w3, bias3, left_ok, right_ok, up_ok, down_ok, inside, cols, tile, extra):
    length = u.shape[1]
    ua, ub = u[:pad], u[pad : 2 * pad]
    q = jnp.where(inside, ua.astype(BF16).astype(F32), 0.0)
    sides = (from_left(q, left_ok), q, from_right(q, right_ok))
    above = [pltpu.roll(s, cols, 1) for s in sides]
    below = [pltpu.roll(s, length - cols, 1) for s in sides]
    stack = [*above, *sides, *below]
    if extra:
        stack.append(jnp.ones((8, length), F32))
    patches = jnp.concatenate(stack, axis=0).astype(BF16)
    pieces = []
    for at in range(0, length, tile):
        size = min(tile, length - at)
        h = dot(w1t, patches[:, at : at + size])
        h = jnp.maximum(h, 0.0).astype(BF16)
        h = dot(w2t, h)
        b = bias2[...]
        b = jnp.concatenate([b] * (size // 128), axis=1)
        h = jnp.maximum(h + b, 0.0).astype(BF16)
        pieces.append(dot(w3, h))
    taps = jnp.concatenate(pieces, axis=1) if len(pieces) > 1 else pieces[0]
    both = 2 * half
    rows = []
    for dr in range(3):
        a, b, c = (taps[(dr * 3 + dc) * both : (dr * 3 + dc + 1) * both] for dc in range(3))
        rows.append(
            b
            + from_left(a, left_ok)
            + from_right(c, right_ok)
        )
    out = (
        rows[1]
        + jnp.where(up_ok, pltpu.roll(rows[0], cols, 1), 0.0)
        + jnp.where(down_ok, pltpu.roll(rows[2], length - cols, 1), 0.0)
        + bias3
    )
    g, t = out[:half] + 2.0, out[half:]
    if pad > half:
        zeros = jnp.zeros((pad - half, length), F32)
        g, t = jnp.concatenate([g, zeros], axis=0), jnp.concatenate([t, zeros], axis=0)
    return ua, (ub + t) * jax.nn.sigmoid(g), g


def log_sigmoid(g):
    return jnp.minimum(g, 0.0) - jnp.log1p(jnp.exp(-jnp.abs(g)))


def kernel(
    n_rows,
    n_chan,
    images,
    shift_mid_h,
    gain_mid_h,
    lower_mid_h,
    upper_mid_h,
    diag_mid_h,
    first_mid,
    first_bias_mid_h,
    second_mid,
    second_bias_mid_h,
    third_mid,
    third_bias_mid_h,
    shift_top_h,
    gain_top_h,
    lower_top_h,
    upper_top_h,
    diag_top_h,
    first_top,
    first_bias_top_h,
    second_top,
    second_bias_top_h,
    third_top,
    third_bias_top_h,
    latent_mid,
    latent_top,
    loglik,
    img_v,
    w1m,
    w2m,
    w3m,
    w1p,
    w2p,
    w3p,
    w1f_m,
    w1f_p,
    w1m_t,
    w2m_t,
    w1p_t,
    w2p_t,
    b2m,
    b2p,
    mix_m,
    mix_p0,
    mix_p1,
    const_m,
    const_p,
    y_out,
    y_in,
    z_out,
    z_in,
    k_out,
    k_in,
    back_out,
    back_in,
    ll_out,
    ll_in,
    shift_mid,
    gain_mid,
    lower_mid,
    upper_mid,
    diag_mid,
    first_bias_mid,
    second_bias_mid,
    third_bias_mid,
    shift_top,
    gain_top,
    lower_top,
    upper_top,
    diag_top,
    first_bias_top,
    second_bias_top,
    third_bias_top,
    load_sem,
    image_sem,
    small_sem,
    ys_sem,
    yr_sem,
    zs_sem,
    zr_sem,
    ks_sem,
    kr_sem,
    bs_sem,
    br_sem,
    ls_sem,
    lr_sem,
    token_sem,
):
    me_row, me_chan = lax.axis_index("rows"), lax.axis_index("chan")
    steps_m, steps_p = shift_mid.shape[0], shift_top.shape[0]
    n_img, c_mid, width = img_v.shape
    half_m = c_mid // 2
    c_top = shift_top.shape[1]
    half_p = c_top // 2

    def has_row(d):
        return jnp.logical_and(me_row + d >= 0, me_row + d < n_rows)

    def to_neighbours(src, dst, send_sem, recv_sem):
        copies = []
        for k, d in enumerate((1, -1)):
            copy = pltpu.make_async_remote_copy(
                src_ref=src,
                dst_ref=dst.at[k],
                send_sem=send_sem.at[k],
                recv_sem=recv_sem.at[k],
                device_id={"rows": lax.rem(me_row + d + n_rows, n_rows)},
                device_id_type=MESH,
            )
            pl.when(has_row(d))(copy.start)
            copies.append((copy, d))
        return copies

    def from_neighbours(copies):
        for copy, d in copies:
            pl.when(has_row(-d))(copy.wait_recv)

    def tell_rows(sem, by):
        for d in (by, -by):

            @pl.when(has_row(d))
            def _():
                pl.semaphore_signal(sem, inc=1, device_id={"rows": lax.rem(me_row + d + n_rows, n_rows)}, device_id_type=MESH)

    def rows_off(by):
        return has_row(by).astype(jnp.int32) + has_row(-by).astype(jnp.int32)

    image_load = pltpu.make_async_copy(images, img_v, image_sem)
    image_load.start()
    barrier = pltpu.get_barrier_semaphore()
    far = sorted(range(1, n_chan), key=lambda k: -min(k, n_chan - k))
    chan_peers = [lax.rem(me_chan + k, n_chan) for k in range(1, n_chan)]
    row_peers = [lax.rem(me_row + k, n_rows) for k in range(1, n_rows)]
    for k in far:
        pl.semaphore_signal(barrier, inc=1, device_id={"chan": chan_peers[k - 1]}, device_id_type=MESH)
    tell_rows(barrier, 1)

    loads = [
        pltpu.make_async_copy(src, dst, load_sem.at[k])
        for k, (src, dst) in enumerate(
            (
                (first_mid, w1m),
                (second_mid, w2m),
                (third_mid, w3m),
                (first_top, w1p),
                (second_top, w2p),
                (third_top, w3p),
            )
        )
    ]
    smalls = [
        pltpu.make_async_copy(src, dst, small_sem.at[k])
        for k, (src, dst) in enumerate(
            (
                (shift_mid_h, shift_mid),
                (gain_mid_h, gain_mid),
                (lower_mid_h, lower_mid),
                (upper_mid_h, upper_mid),
                (diag_mid_h, diag_mid),
                (first_bias_mid_h, first_bias_mid),
                (second_bias_mid_h, second_bias_mid),
                (third_bias_mid_h, third_bias_mid),
                (shift_top_h, shift_top),
                (gain_top_h, gain_top),
                (lower_top_h, lower_top),
                (upper_top_h, upper_top),
                (diag_top_h, diag_top),
                (first_bias_top_h, first_bias_top),
                (second_bias_top_h, second_bias_top),
                (third_bias_top_h, third_bias_top),
            )
        )
    ]
    for load in (*smalls, *loads):
        load.start()

    image_load.wait()
    for i in range(n_img):
        row = img_v[i]
        packed = [row[8 * k : 8 * k + 8] for k in range(c_mid // 8)]
        packed.append(jnp.zeros((8, 128 - width * (c_mid // 8)), F32))
        y_out[i] = jnp.concatenate(packed, axis=1)
    y_in[me_chan] = y_out[me_chan]

    pl.semaphore_wait(barrier, n_chan - 1 + rows_off(1))
    tell_rows(token_sem.at[0], 1)
    y_copies = []
    for k, peer in enumerate(chan_peers):
        copy = pltpu.make_async_remote_copy(
            src_ref=y_out.at[peer],
            dst_ref=y_in.at[me_chan],
            send_sem=ys_sem.at[k],
            recv_sem=yr_sem.at[n_chan - 2 - k],
            device_id={"chan": peer},
            device_id_type=MESH,
        )
        copy.start()
        y_copies.append(copy)

    for load in smalls:
        load.wait()
    spread = jnp.where(
        iota2((32, c_mid), 0)
        == iota2((32, c_mid), 1) + jnp.where(iota2((32, c_mid), 1) >= half_m, 16 - half_m, 0),
        1.0,
        0.0,
    )
    src, lane = iota2((c_mid, 96), 0), lax.rem(iota2((c_mid, 96), 1), 32)
    plain = jnp.where(src == lane, 1.0, 0.0)
    padded = jnp.where(src + jnp.where(src >= half_m, 16 - half_m, 0) == lane, 1.0, 0.0)
    for s in range(steps_m):
        mix, const = mixing(
            lower_mid[s],
            upper_mid[s],
            diag_mid[s : s + 1],
            gain_mid[s : s + 1],
            shift_mid[s : s + 1],
            spread,
            plain if s == 0 else padded,
            64,
        )
        mix_m[s] = mix
        const_m[s] = jnp.where(iota2((32, 1), 0) == half_m, 1.0, const)
    src, lane = iota2((c_top, 192), 0), lax.rem(iota2((c_top, 192), 1), 64)
    squeezed_place = jnp.where(
        jnp.logical_and(lax.rem(lane, 16) < half_m, src == 4 * lax.rem(lane, 16) + lax.div(lane, 16)), 1.0, 0.0
    )
    src, lane = iota2((c_top, 144), 0), lax.rem(iota2((c_top, 144), 1), 48)
    top_place = jnp.where(src == lane, 1.0, 0.0)
    for s in range(steps_p):
        mix, const = mixing(
            lower_top[s],
            upper_top[s],
            diag_top[s : s + 1],
            gain_top[s : s + 1],
            shift_top[s : s + 1],
            None,
            squeezed_place if s == 0 else top_place,
            128 if s == 0 else 96,
        )
        if s == 0:
            mix_p0[...] = mix
        else:
            mix_p1[s - 1] = mix
        const_p[s] = const

    def prepare_mid(s):
        w1f_m[...] = jnp.zeros_like(w1f_m)
        for t in range(9):
            w1f_m[16 * t : 16 * t + half_m] = w1m[s, t].astype(F32)
        w1f_m[64 + half_m : 65 + half_m] = first_bias_mid[s : s + 1].astype(F32)
        w1m_t[s] = w1f_m[...].T.astype(BF16)
        w2m_t[s] = w2m[s].T
        b2m[s] = jnp.broadcast_to(second_bias_mid[s : s + 1], (128, b2m.shape[1])).T

    def prepare_top(s):
        w1f_p[9 * half_p :] = jnp.zeros((8, w1f_p.shape[1]), F32)
        w1f_p[: 9 * half_p] = w1p[s].astype(F32)
        w1f_p[9 * half_p : 9 * half_p + 1] = first_bias_top[s : s + 1].astype(F32)
        w1p_t[s] = w1f_p[...].T.astype(BF16)
        w2p_t[s] = w2p[s].T
        b2p[s] = jnp.broadcast_to(second_bias_top[s : s + 1], (128, b2p.shape[1])).T

    for load in loads:
        load.wait()
    for s in range(steps_m):
        prepare_mid(s)
    for s in range(steps_p):
        prepare_top(s)
    bias3_m = [column(third_bias_mid[s : s + 1]) for s in range(steps_m)]
    bias3_p = [column(third_bias_top[s : s + 1]) for s in range(steps_p)]

    for copy in y_copies:
        copy.wait_recv()
    groups = []
    for k in range(c_mid // 8):
        groups.append(jnp.concatenate([y_in[c][:, width * k : width * (k + 1)] for c in range(n_chan)], axis=1))
    own = jnp.concatenate([*groups, jnp.zeros((32 - c_mid, n_chan * width), F32)], axis=0)
    z_out[...] = own.astype(BF16)
    z_copies = to_neighbours(z_out, z_in, zs_sem, zr_sem)
    pl.semaphore_wait(token_sem.at[0], rows_off(1))
    tell_rows(token_sem.at[1], 2)
    from_neighbours(z_copies)
    zero = jnp.zeros_like(own)
    state = jnp.concatenate(
        [
            jnp.where(has_row(-1), z_in[0].astype(F32), zero),
            own,
            jnp.where(has_row(1), z_in[1].astype(F32), zero),
        ],
        axis=1,
    )

    height = n_rows * n_chan
    partial = jnp.zeros((8, 128), F32)

    def folded(x):
        total = None
        for i in range(0, x.shape[0], 8):
            for j in range(0, x.shape[1], 128):
                piece = x[i : i + 8, j : j + 128]
                total = piece if total is None else total + piece
        return total

    first_row = me_row * n_chan - n_chan
    own_at = n_chan * width
    own_lanes = n_chan * width
    valid_m = iota2((16, own_lanes), 0) < half_m
    for s in range(steps_m):
        if s == 1:
            state = state[:, 4 * width : 20 * width]
            first_row = first_row + 4
            own_at = own_at - 4 * width
        length = state.shape[1]
        lane = iota2((1, length), 1)
        col, row = lax.rem(lane, width), lax.div(lane, width) + first_row
        u = apply_mix(state, mix_m[s], const_m[s])
        ua, updated, g = coupling(
            u,
            half_m,
            16,
            w1m_t.at[s],
            w2m_t.at[s],
            b2m.at[s],
            w3m.at[s],
            bias3_m[s],
            col >= 1,
            col <= width - 2,
            row >= 1,
            row <= height - 2,
            jnp.logical_and(row >= 0, row < height),
            width,
            512,
            False,
        )
        state = jnp.concatenate([ua, updated], axis=0)
        mine = g[:, own_at : own_at + own_lanes]
        partial = partial + folded(jnp.where(valid_m, log_sigmoid(mine), 0.0))
    kept = state[16:, own_at : own_at + own_lanes]
    k_out[...] = kept.astype(BF16)
    k_copies = to_neighbours(k_out, k_in, ks_sem, kr_sem)
    latent = jnp.where(valid_m, state[:16, own_at : own_at + own_lanes], 0.0)
    partial = partial + folded(-0.5 * latent * latent)

    for c in range(n_chan):
        piece = latent[:, width * c : width * (c + 1)]
        back_out[c] = jnp.concatenate([piece[:8], piece[8:], jnp.zeros((8, 128 - 2 * width), F32)], axis=1)
    back_in[me_chan] = back_out[me_chan]
    back_copies = []
    for k, peer in enumerate(chan_peers):
        copy = pltpu.make_async_remote_copy(
            src_ref=back_out.at[peer],
            dst_ref=back_in.at[me_chan],
            send_sem=bs_sem.at[k],
            recv_sem=br_sem.at[n_chan - 2 - k],
            device_id={"chan": peer},
            device_id_type=MESH,
        )
        copy.start()
        back_copies.append(copy)

    cols_p = width // 2
    lane = iota2((16, 128), 1)
    phase, rest = lax.div(lane, 32), lax.rem(lane, 32)
    pick = (2 * lax.div(rest, cols_p) + lax.div(phase, 2)) * width + 2 * lax.rem(rest, cols_p) + lax.rem(phase, 2)
    pl.semaphore_wait(token_sem.at[1], rows_off(2))
    tell_rows(token_sem.at[2], 4)
    from_neighbours(k_copies)
    zero = jnp.zeros_like(kept)
    kept = jnp.concatenate(
        [
            jnp.where(has_row(-1), k_in[0].astype(F32), zero),
            kept,
            jnp.where(has_row(1), k_in[1].astype(F32), zero),
        ],
        axis=1,
    )
    blocks = [
        jnp.take_along_axis(kept[:, 128 * k : 128 * k + 128], pick, axis=1) for k in range(kept.shape[1] // 128)
    ]
    phases = []
    for p in range(4):
        parts = [b[:, 32 * p : 32 * p + 32] for b in blocks]
        parts.append(jnp.zeros((16, 256 - 32 * len(blocks)), F32))
        phases.append(jnp.concatenate(parts, axis=1))
    state = jnp.concatenate(phases, axis=0)

    rows_p = n_chan // 2
    first_row = me_row * rows_p - rows_p
    own_at = rows_p * cols_p
    for s in range(steps_p):
        if s == steps_p - 1:
            state = pltpu.roll(state, state.shape[1] - 2 * cols_p, 1)[:, :128]
            first_row, own_at = first_row + 2, own_at - 2 * cols_p
        lane = iota2((1, state.shape[1]), 1)
        col, row = lax.rem(lane, cols_p), lax.div(lane, cols_p) + first_row
        mine_p = jnp.logical_and(lane >= own_at, lane < own_at + rows_p * cols_p)
        u = apply_mix(state, mix_p0[...] if s == 0 else mix_p1[s - 1], const_p[s])
        ua, updated, g = coupling(
            u,
            half_p,
            half_p,
            w1p_t.at[s],
            w2p_t.at[s],
            b2p.at[s],
            w3p.at[s],
            bias3_p[s],
            col >= 1,
            col <= cols_p - 2,
            row >= 1,
            row <= height // 2 - 2,
            jnp.logical_and(row >= 0, row < height // 2),
            cols_p,
            256,
            True,
        )
        state = jnp.concatenate([ua, updated], axis=0)
        partial = partial + folded(jnp.where(mine_p, log_sigmoid(g), 0.0))
    partial = partial + folded(jnp.where(mine_p, -0.5 * state * state, 0.0))
    ll_out[...] = jnp.sum(partial, axis=0, keepdims=True)
    pl.semaphore_wait(token_sem.at[2], rows_off(4))
    ll_copies = []
    for k, peer in enumerate(row_peers):
        copy = pltpu.make_async_remote_copy(
            src_ref=ll_out,
            dst_ref=ll_in.at[n_rows - 2 - k],
            send_sem=ls_sem.at[k],
            recv_sem=lr_sem.at[n_rows - 2 - k],
            device_id={"rows": peer},
            device_id_type=MESH,
        )
        copy.start()
        ll_copies.append(copy)

    latent_top[...] = state.T[own_at : own_at + rows_p * cols_p]
    for copy in back_copies:
        copy.wait_recv()
    for c in range(n_img):
        piece = back_in[c]
        latent_mid[half_m * c : half_m * c + 8] = piece[:, :width]
        latent_mid[half_m * c + 8 : half_m * (c + 1)] = piece[: half_m - 8, width : 2 * width]
    cells = height * width
    const = sum(
        (
            cells * (jnp.sum(gain_mid[...]) + jnp.sum(diag_mid[...])),
            (cells // 4) * (jnp.sum(gain_top[...]) + jnp.sum(diag_top[...])),
        )
    )
    for copy in ll_copies:
        copy.wait_recv()
    total = ll_out[...]
    for k in range(n_rows - 1):
        total = total + ll_in[k]
    scale = 1.0 / (c_mid * cells)
    loglik[...] = jnp.broadcast_to((jnp.sum(total) + const) * scale - 0.5 * log_two_pi, (1, 128))
    for copy in (*y_copies, *back_copies, *ll_copies):
        copy.wait_send()
    for copies in (z_copies, k_copies):
        for copy, d in copies:
            pl.when(has_row(d))(copy.wait_send)


def write_out(*refs):
    sem = refs[-1]
    copies = [pltpu.make_async_copy(refs[k], refs[3 + k], sem.at[k]) for k in range(3)]
    for copy in copies:
        copy.start()
    for copy in copies:
        copy.wait()


def body(
    images,
    shift_mid,
    gain_mid,
    lower_mid,
    upper_mid,
    diag_mid,
    first_mid,
    first_bias_mid,
    second_mid,
    second_bias_mid,
    third_mid,
    third_bias_mid,
    shift_top,
    gain_top,
    lower_top,
    upper_top,
    diag_top,
    first_top,
    first_bias_top,
    second_top,
    second_bias_top,
    third_top,
    third_bias_top,
):
    n_rows, n_chan = lax.axis_size("rows"), lax.axis_size("chan")
    n_img, c_mid, _, width = images.shape
    hid = second_mid.shape[1]
    steps_m, steps_p = shift_mid.shape[0], shift_top.shape[0]
    c_top = shift_top.shape[1]
    half_m, half_p = c_mid // 2, c_top // 2
    images = images.reshape(n_img, c_mid, width)
    third_mid = third_mid.transpose(0, 1, 3, 2).reshape(steps_m, 9 * c_mid, hid)
    third_top = third_top.transpose(0, 1, 3, 2).reshape(steps_p, 9 * c_top, hid)
    first_top = first_top.reshape(steps_p, 9 * half_p, hid)
    big = pl.BlockSpec(memory_space=pltpu.HBM)
    small = pl.BlockSpec(memory_space=pltpu.VMEM)
    rows_p = n_chan // 2
    vmem = pltpu.VMEM
    small_args = (shift_mid, gain_mid, lower_mid, upper_mid, diag_mid, first_bias_mid, second_bias_mid, third_bias_mid, shift_top, gain_top, lower_top, upper_top, diag_top, first_bias_top, second_bias_top, third_bias_top)
    dma = pltpu.SemaphoreType.DMA
    found = pl.pallas_call(
        functools.partial(kernel, n_rows, n_chan),
        out_shape=(
            vmem((n_img * half_m, width), F32),
            vmem((rows_p * width // 2, c_top), F32),
            vmem((1, 128), F32),
        ),
        in_specs=[big] * 23,
        out_specs=(small, small, small),
        scratch_shapes=[
            vmem((n_img, c_mid, width), F32),
            vmem((steps_m, 9, half_m, hid), BF16),
            vmem((steps_m, hid, hid), BF16),
            vmem((steps_m, 9 * c_mid, hid), BF16),
            vmem((steps_p, 9 * half_p, hid), BF16),
            vmem((steps_p, hid, hid), BF16),
            vmem((steps_p, 9 * c_top, hid), BF16),
            vmem((144, hid), F32),
            vmem((9 * half_p + 8, hid), F32),
            vmem((steps_m, hid, 144), BF16),
            vmem((steps_m, hid, hid), BF16),
            vmem((steps_p, hid, 9 * half_p + 8), BF16),
            vmem((steps_p, hid, hid), BF16),
            vmem((steps_m, hid, 128), F32),
            vmem((steps_p, hid, 128), F32),
            vmem((steps_m, 32, 96), BF16),
            vmem((c_top, 192), BF16),
            vmem((steps_p - 1, c_top, 144), BF16),
            vmem((steps_m, 32, 1), F32),
            vmem((steps_p, c_top, 1), F32),
            vmem((n_chan, 8, 128), F32),
            vmem((n_chan, 8, 128), F32),
            vmem((32, n_chan * width), BF16),
            vmem((2, 32, n_chan * width), BF16),
            vmem((16, n_chan * width), BF16),
            vmem((2, 16, n_chan * width), BF16),
            vmem((n_chan, 8, 128), F32),
            vmem((n_chan, 8, 128), F32),
            vmem((1, 128), F32),
            vmem((n_rows - 1, 1, 128), F32),
            *(vmem(a.shape, a.dtype) for a in small_args),
            dma((6,)),
            dma(()),
            dma((len(small_args),)),
            dma((n_chan - 1,)),
            dma((n_chan - 1,)),
            dma((2,)),
            dma((2,)),
            dma((2,)),
            dma((2,)),
            dma((n_chan - 1,)),
            dma((n_chan - 1,)),
            dma((n_rows - 1,)),
            dma((n_rows - 1,)),
            pltpu.SemaphoreType.REGULAR((3,)),
        ],
        compiler_params=pltpu.CompilerParams(
            collective_id=0, has_side_effects=True, vmem_limit_bytes=67043328 - 100 * 1024
        ),
    )(
        images,
        shift_mid,
        gain_mid,
        lower_mid,
        upper_mid,
        diag_mid,
        first_mid,
        first_bias_mid,
        second_mid,
        second_bias_mid,
        third_mid,
        third_bias_mid,
        shift_top,
        gain_top,
        lower_top,
        upper_top,
        diag_top,
        first_top,
        first_bias_top,
        second_top,
        second_bias_top,
        third_top,
        third_bias_top,
    )
    latent_mid, latent_top, loglik = pl.pallas_call(
        write_out,
        out_shape=tuple(jax.ShapeDtypeStruct(x.shape, x.dtype) for x in found),
        in_specs=[small] * 3,
        out_specs=(pl.BlockSpec(memory_space=pltpu.HBM),) * 3,
        scratch_shapes=[dma((3,))],
        compiler_params=pltpu.CompilerParams(vmem_limit_bytes=1024 * 1024),
    )(*found)
    latent_mid = latent_mid.reshape(n_img, half_m, 1, width)
    latent_top = latent_top.reshape(1, rows_p, width // 2, c_top).transpose(0, 3, 1, 2)
    return latent_mid, latent_top, loglik[0, :1]


def solution(mesh):
    placed = (P("batch", None, ("rows", "chan"), None),) + (P(),) * 22
    return jax.shard_map(
        body,
        mesh=mesh,
        in_specs=placed,
        out_specs=(
            P("batch", None, ("rows", "chan"), None),
            P(("batch", "chan"), None, "rows", None),
            P(("batch", "chan")),
        ),
        check_vma=False,
    )
```

```python
import functools
import math

import jax
import jax.numpy as jnp
from jax import lax
from jax.experimental import pallas as pl
from jax.experimental.pallas import tpu as pltpu
from jax.sharding import PartitionSpec as P

MESH = pl.DeviceIdType.MESH
F32 = jnp.float32
BF16 = jnp.bfloat16
HI = lax.Precision.HIGHEST
log_two_pi = math.log(2.0 * math.pi)


def iota2(shape, dim):
    return lax.broadcasted_iota(jnp.int32, shape, dim)


def mixing(lower, upper, diag, gain, shift, spread, place, split_at):
    n = lower.shape[0]
    r, c = iota2((n, n), 0), iota2((n, n), 1)
    low = jnp.where(r > c, lower, jnp.where(r == c, 1.0, 0.0))
    up = jnp.where(c > r, upper, jnp.where(r == c, jnp.exp(diag), 0.0)) * jnp.exp(gain)
    both = jnp.dot(low, up, precision=HI, preferred_element_type=F32)
    if spread is not None:
        both = jnp.dot(spread, both, precision=HI, preferred_element_type=F32)
    const = jnp.sum(both * shift, axis=1, keepdims=True)
    wide = jnp.dot(both, place, precision=HI, preferred_element_type=F32)
    high = wide.astype(BF16).astype(F32)
    lane = iota2(wide.shape, 1)
    return jnp.where(lane < split_at, high, wide - high).astype(BF16), const


def column(row):
    n = row.shape[1]
    eye = iota2((n, n), 0) == iota2((n, n), 1)
    return jnp.sum(jnp.where(eye, jnp.broadcast_to(row, (n, n)), 0.0), axis=1, keepdims=True)


def apply_mix(state, mix, const):
    high = state.astype(BF16)
    low = (state - high.astype(F32)).astype(BF16)
    stacked = jnp.concatenate([high, low, high], axis=0)
    return jnp.dot(mix, stacked, preferred_element_type=F32) + const


def dot(w, x):
    if x.shape[1] > 256:
        return jnp.dot(w[...], x, preferred_element_type=F32)
    rows = w.shape[0]
    cut = rows // 16 // 2 * 16
    return jnp.concatenate(
        [
            jnp.dot(w[:cut], x, preferred_element_type=F32),
            jnp.dot(w[cut:], x, preferred_element_type=F32),
        ],
        axis=0,
    )


def shifted(x, by, ok):
    pieces = [pltpu.roll(x[:, at : at + 128], by, 1) for at in range(0, x.shape[1], 128)]
    return jnp.where(ok, jnp.concatenate(pieces, axis=1), 0.0)


def from_left(x, ok):
    return shifted(x, 1, ok)


def from_right(x, ok):
    return shifted(x, 127, ok)


def coupling(u, half, pad, w1t, w2t, bias2, w3, bias3, left_ok, right_ok, up_ok, down_ok, inside, cols, tile, extra):
    length = u.shape[1]
    ua, ub = u[:pad], u[pad : 2 * pad]
    q = jnp.where(inside, ua.astype(BF16).astype(F32), 0.0)
    sides = (from_left(q, left_ok), q, from_right(q, right_ok))
    above = [pltpu.roll(s, cols, 1) for s in sides]
    below = [pltpu.roll(s, length - cols, 1) for s in sides]
    stack = [*above, *sides, *below]
    if extra:
        stack.append(jnp.ones((8, length), F32))
    patches = jnp.concatenate(stack, axis=0).astype(BF16)
    pieces = []
    for at in range(0, length, tile):
        size = min(tile, length - at)
        h = dot(w1t, patches[:, at : at + size])
        h = jnp.maximum(h, 0.0).astype(BF16)
        h = dot(w2t, h)
        b = bias2[...]
        b = jnp.concatenate([b] * (size // 128), axis=1)
        h = jnp.maximum(h + b, 0.0).astype(BF16)
        pieces.append(dot(w3, h))
    taps = jnp.concatenate(pieces, axis=1) if len(pieces) > 1 else pieces[0]
    both = 2 * half
    rows = []
    for dr in range(3):
        a, b, c = (taps[(dr * 3 + dc) * both : (dr * 3 + dc + 1) * both] for dc in range(3))
        rows.append(
            b
            + from_left(a, left_ok)
            + from_right(c, right_ok)
        )
    out = (
        rows[1]
        + jnp.where(up_ok, pltpu.roll(rows[0], cols, 1), 0.0)
        + jnp.where(down_ok, pltpu.roll(rows[2], length - cols, 1), 0.0)
        + bias3
    )
    g, t = out[:half] + 2.0, out[half:]
    if pad > half:
        zeros = jnp.zeros((pad - half, length), F32)
        g, t = jnp.concatenate([g, zeros], axis=0), jnp.concatenate([t, zeros], axis=0)
    return ua, (ub + t) * jax.nn.sigmoid(g), g


def log_sigmoid(g):
    return jnp.minimum(g, 0.0) - jnp.log1p(jnp.exp(-jnp.abs(g)))


def kernel(
    n_rows,
    n_chan,
    images,
    shift_mid_h,
    gain_mid_h,
    lower_mid_h,
    upper_mid_h,
    diag_mid_h,
    first_mid,
    first_bias_mid_h,
    second_mid,
    second_bias_mid_h,
    third_mid,
    third_bias_mid_h,
    shift_top_h,
    gain_top_h,
    lower_top_h,
    upper_top_h,
    diag_top_h,
    first_top,
    first_bias_top_h,
    second_top,
    second_bias_top_h,
    third_top,
    third_bias_top_h,
    latent_mid,
    latent_top,
    loglik,
    img_v,
    w1m,
    w2m,
    w3m,
    w1p,
    w2p,
    w3p,
    w1f_m,
    w1f_p,
    w1m_t,
    w2m_t,
    w1p_t,
    w2p_t,
    b2m,
    b2p,
    mix_m,
    mix_p0,
    mix_p1,
    const_m,
    const_p,
    y_out,
    y_in,
    z_in,
    k_out,
    k_in,
    back_out,
    back_in,
    ll_out,
    ll_in,
    shift_mid,
    gain_mid,
    lower_mid,
    upper_mid,
    diag_mid,
    first_bias_mid,
    second_bias_mid,
    third_bias_mid,
    shift_top,
    gain_top,
    lower_top,
    upper_top,
    diag_top,
    first_bias_top,
    second_bias_top,
    third_bias_top,
    load_sem,
    image_sem,
    small_sem,
    ys_sem,
    yr_sem,
    zs_sem,
    zr_sem,
    ks_sem,
    kr_sem,
    bs_sem,
    br_sem,
    ls_sem,
    lr_sem,
    token_sem,
):
    me_row, me_chan = lax.axis_index("rows"), lax.axis_index("chan")
    steps_m, steps_p = shift_mid.shape[0], shift_top.shape[0]
    n_img, c_mid, width = img_v.shape
    halo = 2 * steps_m
    half_m = c_mid // 2
    c_top = shift_top.shape[1]
    half_p = c_top // 2

    def has_row(d):
        return jnp.logical_and(me_row + d >= 0, me_row + d < n_rows)

    def to_neighbours(src, dst, send_sem, recv_sem):
        copies = []
        for k, d in enumerate((1, -1)):
            copy = pltpu.make_async_remote_copy(
                src_ref=src,
                dst_ref=dst.at[k],
                send_sem=send_sem.at[k],
                recv_sem=recv_sem.at[k],
                device_id={"rows": lax.rem(me_row + d + n_rows, n_rows)},
                device_id_type=MESH,
            )
            pl.when(has_row(d))(copy.start)
            copies.append((copy, d))
        return copies

    def from_neighbours(copies):
        for copy, d in copies:
            pl.when(has_row(-d))(copy.wait_recv)

    def tell_rows(sem, by):
        for d in (by, -by):

            @pl.when(has_row(d))
            def _():
                pl.semaphore_signal(sem, inc=1, device_id={"rows": lax.rem(me_row + d + n_rows, n_rows)}, device_id_type=MESH)

    def rows_off(by):
        return has_row(by).astype(jnp.int32) + has_row(-by).astype(jnp.int32)

    image_load = pltpu.make_async_copy(images, img_v, image_sem)
    image_load.start()
    barrier = pltpu.get_barrier_semaphore()
    far = sorted(range(1, n_chan), key=lambda k: (-(k // 2 == 2), -(k > 1)))
    chan_peers = [me_chan ^ k for k in range(1, n_chan)]
    row_peers = [lax.rem(me_row + k, n_rows) for k in range(1, n_rows)]
    far_rows = sorted(range(1, n_rows), key=lambda k: -min(k, n_rows - k))
    for k in far:
        pl.semaphore_signal(barrier, inc=1, device_id={"chan": chan_peers[k - 1]}, device_id_type=MESH)
    tell_rows(barrier, 1)

    loads = [
        pltpu.make_async_copy(src, dst, load_sem.at[k])
        for k, (src, dst) in enumerate(
            (
                (first_mid, w1m),
                (second_mid, w2m),
                (third_mid, w3m),
                (first_top, w1p),
                (second_top, w2p),
                (third_top, w3p),
            )
        )
    ]
    smalls = [
        pltpu.make_async_copy(src, dst, small_sem.at[k])
        for k, (src, dst) in enumerate(
            (
                (shift_mid_h, shift_mid),
                (gain_mid_h, gain_mid),
                (lower_mid_h, lower_mid),
                (upper_mid_h, upper_mid),
                (diag_mid_h, diag_mid),
                (first_bias_mid_h, first_bias_mid),
                (second_bias_mid_h, second_bias_mid),
                (third_bias_mid_h, third_bias_mid),
                (shift_top_h, shift_top),
                (gain_top_h, gain_top),
                (lower_top_h, lower_top),
                (upper_top_h, upper_top),
                (diag_top_h, diag_top),
                (first_bias_top_h, first_bias_top),
                (second_bias_top_h, second_bias_top),
                (third_bias_top_h, third_bias_top),
            )
        )
    ]
    for load in (*smalls, *loads):
        load.start()

    image_load.wait()
    for i in range(n_img):
        row = img_v[i]
        packed = [row[8 * k : 8 * k + 8] for k in range(c_mid // 8)]
        packed.append(jnp.zeros((8, 128 - width * (c_mid // 8)), F32))
        y_out[i] = jnp.concatenate(packed, axis=1)
    y_in[me_chan] = y_out[me_chan]

    pl.semaphore_wait(barrier, n_chan - 1 + rows_off(1))
    tell_rows(token_sem.at[0], 1)
    y_copies = []
    for k in far:
        peer = chan_peers[k - 1]
        copy = pltpu.make_async_remote_copy(
            src_ref=y_out.at[peer],
            dst_ref=y_in.at[me_chan],
            send_sem=ys_sem.at[k - 1],
            recv_sem=yr_sem.at[k - 1],
            device_id={"chan": peer},
            device_id_type=MESH,
        )
        copy.start()
        y_copies.append(copy)

    for load in smalls:
        load.wait()
    spread = jnp.where(
        iota2((32, c_mid), 0)
        == iota2((32, c_mid), 1) + jnp.where(iota2((32, c_mid), 1) >= half_m, 16 - half_m, 0),
        1.0,
        0.0,
    )
    src, lane = iota2((c_mid, 96), 0), lax.rem(iota2((c_mid, 96), 1), 32)
    plain = jnp.where(src == lane, 1.0, 0.0)
    padded = jnp.where(src + jnp.where(src >= half_m, 16 - half_m, 0) == lane, 1.0, 0.0)
    for s in range(steps_m):
        mix, const = mixing(
            lower_mid[s],
            upper_mid[s],
            diag_mid[s : s + 1],
            gain_mid[s : s + 1],
            shift_mid[s : s + 1],
            spread,
            plain if s == 0 else padded,
            64,
        )
        mix_m[s] = mix
        const_m[s] = jnp.where(iota2((32, 1), 0) == half_m, 1.0, const)
    src, lane = iota2((c_top, 192), 0), lax.rem(iota2((c_top, 192), 1), 64)
    squeezed_place = jnp.where(
        jnp.logical_and(lax.rem(lane, 16) < half_m, src == 4 * lax.rem(lane, 16) + lax.div(lane, 16)), 1.0, 0.0
    )
    src, lane = iota2((c_top, 144), 0), lax.rem(iota2((c_top, 144), 1), 48)
    top_place = jnp.where(src == lane, 1.0, 0.0)
    for s in range(steps_p):
        mix, const = mixing(
            lower_top[s],
            upper_top[s],
            diag_top[s : s + 1],
            gain_top[s : s + 1],
            shift_top[s : s + 1],
            None,
            squeezed_place if s == 0 else top_place,
            128 if s == 0 else 96,
        )
        if s == 0:
            mix_p0[...] = mix
        else:
            mix_p1[s - 1] = mix
        const_p[s] = const

    def prepare_mid(s):
        w1f_m[...] = jnp.zeros_like(w1f_m)
        for t in range(9):
            w1f_m[16 * t : 16 * t + half_m] = w1m[s, t].astype(F32)
        w1f_m[64 + half_m : 65 + half_m] = first_bias_mid[s : s + 1].astype(F32)
        w1m_t[s] = w1f_m[...].T.astype(BF16)
        w2m_t[s] = w2m[s].T
        b2m[s] = jnp.broadcast_to(second_bias_mid[s : s + 1], (128, b2m.shape[1])).T

    def prepare_top(s):
        w1f_p[9 * half_p :] = jnp.zeros((8, w1f_p.shape[1]), F32)
        w1f_p[: 9 * half_p] = w1p[s].astype(F32)
        w1f_p[9 * half_p : 9 * half_p + 1] = first_bias_top[s : s + 1].astype(F32)
        w1p_t[s] = w1f_p[...].T.astype(BF16)
        w2p_t[s] = w2p[s].T
        b2p[s] = jnp.broadcast_to(second_bias_top[s : s + 1], (128, b2p.shape[1])).T

    for load in loads:
        load.wait()
    for s in range(steps_m):
        prepare_mid(s)
    for s in range(steps_p):
        prepare_top(s)
    bias3_m = [column(third_bias_mid[s : s + 1]) for s in range(steps_m)]
    bias3_p = [column(third_bias_top[s : s + 1]) for s in range(steps_p)]

    z_copies = []

    def forward(c):
        for k, (d, needed) in enumerate(((1, c >= n_chan - halo), (-1, c < halo))):
            copy = pltpu.make_async_remote_copy(
                src_ref=y_in.at[c],
                dst_ref=z_in.at[k, c],
                send_sem=zs_sem.at[k, c],
                recv_sem=zr_sem.at[k, c],
                device_id={"rows": lax.rem(me_row + d + n_rows, n_rows)},
                device_id_type=MESH,
            )
            there = jnp.logical_and(has_row(d), needed)
            pl.when(there)(copy.start)
            z_copies.append((copy, there))

    forward(me_chan)
    for copy, k in sorted(zip(y_copies, far), key=lambda pair: -far.index(pair[1])):
        copy.wait_recv()
        forward(chan_peers[k - 1])

    def block(rows):
        groups = [
            jnp.concatenate([r[:, width * k : width * (k + 1)] for r in rows], axis=1) for k in range(c_mid // 8)
        ]
        return jnp.concatenate([*groups, jnp.zeros((32 - c_mid, n_chan * width), F32)], axis=0)

    own = block([y_in[c] for c in range(n_chan)])
    pl.semaphore_wait(token_sem.at[0], rows_off(1))
    tell_rows(token_sem.at[1], 2)
    for k, (d, needed) in enumerate(((1, range(n_chan - halo, n_chan)), (-1, range(halo)))):

        @pl.when(has_row(-d))
        def _():
            for c in needed:
                pltpu.make_async_remote_copy(
                    src_ref=y_in.at[c],
                    dst_ref=z_in.at[k, c],
                    send_sem=zs_sem.at[k, c],
                    recv_sem=zr_sem.at[k, c],
                    device_id={"rows": lax.rem(me_row + d + n_rows, n_rows)},
                    device_id_type=MESH,
                ).wait_recv()

    zero = jnp.zeros_like(own)
    blank = jnp.zeros((8, 128), F32)
    state = jnp.concatenate(
        [
            jnp.where(has_row(-1), block([blank] * (n_chan - halo) + [z_in[0, c] for c in range(n_chan - halo, n_chan)]), zero),
            own,
            jnp.where(has_row(1), block([z_in[1, c] for c in range(halo)] + [blank] * (n_chan - halo)), zero),
        ],
        axis=1,
    )

    height = n_rows * n_chan
    partial = jnp.zeros((8, 128), F32)

    def folded(x):
        total = None
        for i in range(0, x.shape[0], 8):
            for j in range(0, x.shape[1], 128):
                piece = x[i : i + 8, j : j + 128]
                total = piece if total is None else total + piece
        return total

    first_row = me_row * n_chan - n_chan
    own_at = n_chan * width
    own_lanes = n_chan * width
    valid_m = iota2((16, own_lanes), 0) < half_m
    for s in range(steps_m):
        if s == 1:
            state = state[:, 4 * width : 20 * width]
            first_row = first_row + 4
            own_at = own_at - 4 * width
        length = state.shape[1]
        lane = iota2((1, length), 1)
        col, row = lax.rem(lane, width), lax.div(lane, width) + first_row
        u = apply_mix(state, mix_m[s], const_m[s])
        ua, updated, g = coupling(
            u,
            half_m,
            16,
            w1m_t.at[s],
            w2m_t.at[s],
            b2m.at[s],
            w3m.at[s],
            bias3_m[s],
            col >= 1,
            col <= width - 2,
            row >= 1,
            row <= height - 2,
            jnp.logical_and(row >= 0, row < height),
            width,
            512,
            False,
        )
        state = jnp.concatenate([ua, updated], axis=0)
        mine = g[:, own_at : own_at + own_lanes]
        partial = partial + folded(jnp.where(valid_m, log_sigmoid(mine), 0.0))
    kept = state[16:, own_at : own_at + own_lanes]
    k_out[...] = kept.astype(BF16)
    k_copies = to_neighbours(k_out, k_in, ks_sem, kr_sem)
    latent = jnp.where(valid_m, state[:16, own_at : own_at + own_lanes], 0.0)
    partial = partial + folded(-0.5 * latent * latent)

    for c in range(n_chan):
        piece = latent[:, width * c : width * (c + 1)]
        back_out[c] = jnp.concatenate([piece[:8], piece[8:], jnp.zeros((8, 128 - 2 * width), F32)], axis=1)
    back_in[me_chan] = back_out[me_chan]
    back_copies = []
    for k in far:
        peer = chan_peers[k - 1]
        copy = pltpu.make_async_remote_copy(
            src_ref=back_out.at[peer],
            dst_ref=back_in.at[me_chan],
            send_sem=bs_sem.at[k - 1],
            recv_sem=br_sem.at[k - 1],
            device_id={"chan": peer},
            device_id_type=MESH,
        )
        copy.start()
        back_copies.append(copy)

    cols_p = width // 2
    lane = iota2((16, 128), 1)
    phase, rest = lax.div(lane, 32), lax.rem(lane, 32)
    pick = (2 * lax.div(rest, cols_p) + lax.div(phase, 2)) * width + 2 * lax.rem(rest, cols_p) + lax.rem(phase, 2)
    pl.semaphore_wait(token_sem.at[1], rows_off(2))
    tell_rows(token_sem.at[2], 4)
    from_neighbours(k_copies)
    zero = jnp.zeros_like(kept)
    kept = jnp.concatenate(
        [
            jnp.where(has_row(-1), k_in[0].astype(F32), zero),
            kept,
            jnp.where(has_row(1), k_in[1].astype(F32), zero),
        ],
        axis=1,
    )
    blocks = [
        jnp.take_along_axis(kept[:, 128 * k : 128 * k + 128], pick, axis=1) for k in range(kept.shape[1] // 128)
    ]
    phases = []
    for p in range(4):
        parts = [b[:, 32 * p : 32 * p + 32] for b in blocks]
        parts.append(jnp.zeros((16, 256 - 32 * len(blocks)), F32))
        phases.append(jnp.concatenate(parts, axis=1))
    state = jnp.concatenate(phases, axis=0)

    rows_p = n_chan // 2
    first_row = me_row * rows_p - rows_p
    own_at = rows_p * cols_p
    for s in range(steps_p):
        if s == steps_p - 1:
            state = pltpu.roll(state, state.shape[1] - 2 * cols_p, 1)[:, :128]
            first_row, own_at = first_row + 2, own_at - 2 * cols_p
        lane = iota2((1, state.shape[1]), 1)
        col, row = lax.rem(lane, cols_p), lax.div(lane, cols_p) + first_row
        mine_p = jnp.logical_and(lane >= own_at, lane < own_at + rows_p * cols_p)
        u = apply_mix(state, mix_p0[...] if s == 0 else mix_p1[s - 1], const_p[s])
        ua, updated, g = coupling(
            u,
            half_p,
            half_p,
            w1p_t.at[s],
            w2p_t.at[s],
            b2p.at[s],
            w3p.at[s],
            bias3_p[s],
            col >= 1,
            col <= cols_p - 2,
            row >= 1,
            row <= height // 2 - 2,
            jnp.logical_and(row >= 0, row < height // 2),
            cols_p,
            256,
            True,
        )
        state = jnp.concatenate([ua, updated], axis=0)
        partial = partial + folded(jnp.where(mine_p, log_sigmoid(g), 0.0))
    partial = partial + folded(jnp.where(mine_p, -0.5 * state * state, 0.0))
    ll_out[...] = jnp.sum(partial, axis=0, keepdims=True)
    pl.semaphore_wait(token_sem.at[2], rows_off(4))
    ll_copies = []
    for k in far_rows:
        peer = row_peers[k - 1]
        copy = pltpu.make_async_remote_copy(
            src_ref=ll_out,
            dst_ref=ll_in.at[n_rows - 1 - k],
            send_sem=ls_sem.at[k - 1],
            recv_sem=lr_sem.at[n_rows - 1 - k],
            device_id={"rows": peer},
            device_id_type=MESH,
        )
        copy.start()
        ll_copies.append(copy)

    latent_top[...] = state.T[own_at : own_at + rows_p * cols_p]
    for copy in back_copies:
        copy.wait_recv()
    for c in range(n_img):
        piece = back_in[c]
        latent_mid[half_m * c : half_m * c + 8] = piece[:, :width]
        latent_mid[half_m * c + 8 : half_m * (c + 1)] = piece[: half_m - 8, width : 2 * width]
    cells = height * width
    const = sum(
        (
            cells * (jnp.sum(gain_mid[...]) + jnp.sum(diag_mid[...])),
            (cells // 4) * (jnp.sum(gain_top[...]) + jnp.sum(diag_top[...])),
        )
    )
    for copy in ll_copies:
        copy.wait_recv()
    total = ll_out[...]
    for k in range(n_rows - 1):
        total = total + ll_in[k]
    scale = 1.0 / (c_mid * cells)
    loglik[...] = jnp.broadcast_to((jnp.sum(total) + const) * scale - 0.5 * log_two_pi, (1, 128))
    for copy in (*y_copies, *back_copies, *ll_copies):
        copy.wait_send()
    for copy, there in z_copies:
        pl.when(there)(copy.wait_send)
    for copy, d in k_copies:
        pl.when(has_row(d))(copy.wait_send)


def write_out(*refs):
    sem = refs[-1]
    copies = [pltpu.make_async_copy(refs[k], refs[3 + k], sem.at[k]) for k in range(3)]
    for copy in copies:
        copy.start()
    for copy in copies:
        copy.wait()


def body(
    images,
    shift_mid,
    gain_mid,
    lower_mid,
    upper_mid,
    diag_mid,
    first_mid,
    first_bias_mid,
    second_mid,
    second_bias_mid,
    third_mid,
    third_bias_mid,
    shift_top,
    gain_top,
    lower_top,
    upper_top,
    diag_top,
    first_top,
    first_bias_top,
    second_top,
    second_bias_top,
    third_top,
    third_bias_top,
):
    n_rows, n_chan = lax.axis_size("rows"), lax.axis_size("chan")
    n_img, c_mid, _, width = images.shape
    hid = second_mid.shape[1]
    steps_m, steps_p = shift_mid.shape[0], shift_top.shape[0]
    c_top = shift_top.shape[1]
    half_m, half_p = c_mid // 2, c_top // 2
    images = images.reshape(n_img, c_mid, width)
    third_mid = third_mid.transpose(0, 1, 3, 2).reshape(steps_m, 9 * c_mid, hid)
    third_top = third_top.transpose(0, 1, 3, 2).reshape(steps_p, 9 * c_top, hid)
    first_top = first_top.reshape(steps_p, 9 * half_p, hid)
    big = pl.BlockSpec(memory_space=pltpu.HBM)
    small = pl.BlockSpec(memory_space=pltpu.VMEM)
    rows_p = n_chan // 2
    vmem = pltpu.VMEM
    small_args = (shift_mid, gain_mid, lower_mid, upper_mid, diag_mid, first_bias_mid, second_bias_mid, third_bias_mid, shift_top, gain_top, lower_top, upper_top, diag_top, first_bias_top, second_bias_top, third_bias_top)
    dma = pltpu.SemaphoreType.DMA
    found = pl.pallas_call(
        functools.partial(kernel, n_rows, n_chan),
        out_shape=(
            vmem((n_img * half_m, width), F32),
            vmem((rows_p * width // 2, c_top), F32),
            vmem((1, 128), F32),
        ),
        in_specs=[big] * 23,
        out_specs=(small, small, small),
        scratch_shapes=[
            vmem((n_img, c_mid, width), F32),
            vmem((steps_m, 9, half_m, hid), BF16),
            vmem((steps_m, hid, hid), BF16),
            vmem((steps_m, 9 * c_mid, hid), BF16),
            vmem((steps_p, 9 * half_p, hid), BF16),
            vmem((steps_p, hid, hid), BF16),
            vmem((steps_p, 9 * c_top, hid), BF16),
            vmem((144, hid), F32),
            vmem((9 * half_p + 8, hid), F32),
            vmem((steps_m, hid, 144), BF16),
            vmem((steps_m, hid, hid), BF16),
            vmem((steps_p, hid, 9 * half_p + 8), BF16),
            vmem((steps_p, hid, hid), BF16),
            vmem((steps_m, hid, 128), F32),
            vmem((steps_p, hid, 128), F32),
            vmem((steps_m, 32, 96), BF16),
            vmem((c_top, 192), BF16),
            vmem((steps_p - 1, c_top, 144), BF16),
            vmem((steps_m, 32, 1), F32),
            vmem((steps_p, c_top, 1), F32),
            vmem((n_chan, 8, 128), F32),
            vmem((n_chan, 8, 128), F32),
            vmem((2, n_chan, 8, 128), F32),
            vmem((16, n_chan * width), BF16),
            vmem((2, 16, n_chan * width), BF16),
            vmem((n_chan, 8, 128), F32),
            vmem((n_chan, 8, 128), F32),
            vmem((1, 128), F32),
            vmem((n_rows - 1, 1, 128), F32),
            *(vmem(a.shape, a.dtype) for a in small_args),
            dma((6,)),
            dma(()),
            dma((len(small_args),)),
            dma((n_chan - 1,)),
            dma((n_chan - 1,)),
            dma((2, n_chan)),
            dma((2, n_chan)),
            dma((2,)),
            dma((2,)),
            dma((n_chan - 1,)),
            dma((n_chan - 1,)),
            dma((n_rows - 1,)),
            dma((n_rows - 1,)),
            pltpu.SemaphoreType.REGULAR((3,)),
        ],
        compiler_params=pltpu.CompilerParams(
            collective_id=0, has_side_effects=True, vmem_limit_bytes=67043328 - 100 * 1024
        ),
    )(
        images,
        shift_mid,
        gain_mid,
        lower_mid,
        upper_mid,
        diag_mid,
        first_mid,
        first_bias_mid,
        second_mid,
        second_bias_mid,
        third_mid,
        third_bias_mid,
        shift_top,
        gain_top,
        lower_top,
        upper_top,
        diag_top,
        first_top,
        first_bias_top,
        second_top,
        second_bias_top,
        third_top,
        third_bias_top,
    )
    latent_mid, latent_top, loglik = pl.pallas_call(
        write_out,
        out_shape=tuple(jax.ShapeDtypeStruct(x.shape, x.dtype) for x in found),
        in_specs=[small] * 3,
        out_specs=(pl.BlockSpec(memory_space=pltpu.HBM),) * 3,
        scratch_shapes=[dma((3,))],
        compiler_params=pltpu.CompilerParams(vmem_limit_bytes=1024 * 1024),
    )(*found)
    latent_mid = latent_mid.reshape(n_img, half_m, 1, width)
    latent_top = latent_top.reshape(1, rows_p, width // 2, c_top).transpose(0, 3, 1, 2)
    return latent_mid, latent_top, loglik[0, :1]


def solution(mesh):
    placed = (P("batch", None, ("rows", "chan"), None),) + (P(),) * 22
    return jax.shard_map(
        body,
        mesh=mesh,
        in_specs=placed,
        out_specs=(
            P("batch", None, ("rows", "chan"), None),
            P(("batch", "chan"), None, "rows", None),
            P(("batch", "chan")),
        ),
        check_vma=False,
    )
```

```python
import functools
import math

import jax
import jax.numpy as jnp
from jax import lax
from jax.experimental import pallas as pl
from jax.experimental.pallas import tpu as pltpu
from jax.sharding import PartitionSpec as P

MESH = pl.DeviceIdType.MESH
F32 = jnp.float32
BF16 = jnp.bfloat16
HI = lax.Precision.HIGHEST
log_two_pi = math.log(2.0 * math.pi)


def iota2(shape, dim):
    return lax.broadcasted_iota(jnp.int32, shape, dim)


def mixing(lower, upper, diag, gain, shift, spread, place, split_at):
    n = lower.shape[0]
    r, c = iota2((n, n), 0), iota2((n, n), 1)
    low = jnp.where(r > c, lower, jnp.where(r == c, 1.0, 0.0))
    up = jnp.where(c > r, upper, jnp.where(r == c, jnp.exp(diag), 0.0)) * jnp.exp(gain)
    both = jnp.dot(low, up, precision=HI, preferred_element_type=F32)
    if spread is not None:
        both = jnp.dot(spread, both, precision=HI, preferred_element_type=F32)
    const = jnp.sum(both * shift, axis=1, keepdims=True)
    wide = jnp.dot(both, place, precision=HI, preferred_element_type=F32)
    high = wide.astype(BF16).astype(F32)
    lane = iota2(wide.shape, 1)
    return jnp.where(lane < split_at, high, wide - high).astype(BF16), const


def column(row):
    n = row.shape[1]
    eye = iota2((n, n), 0) == iota2((n, n), 1)
    return jnp.sum(jnp.where(eye, jnp.broadcast_to(row, (n, n)), 0.0), axis=1, keepdims=True)


def apply_mix(state, mix, const):
    high = state.astype(BF16)
    low = (state - high.astype(F32)).astype(BF16)
    stacked = jnp.concatenate([high, low, high], axis=0)
    return jnp.dot(mix, stacked, preferred_element_type=F32) + const


def dot(w, x):
    if x.shape[1] > 256:
        return jnp.dot(w[...], x, preferred_element_type=F32)
    rows = w.shape[0]
    cut = rows // 16 // 2 * 16
    return jnp.concatenate(
        [
            jnp.dot(w[:cut], x, preferred_element_type=F32),
            jnp.dot(w[cut:], x, preferred_element_type=F32),
        ],
        axis=0,
    )


def shifted(x, by, ok):
    pieces = [pltpu.roll(x[:, at : at + 128], by, 1) for at in range(0, x.shape[1], 128)]
    return jnp.where(ok, jnp.concatenate(pieces, axis=1), 0.0)


def from_left(x, ok):
    return shifted(x, 1, ok)


def from_right(x, ok):
    return shifted(x, 127, ok)


def coupling(u, half, pad, w1t, w2t, bias2, w3, bias3, left_ok, right_ok, up_ok, down_ok, inside, cols, tile, extra):
    length = u.shape[1]
    ua, ub = u[:pad], u[pad : 2 * pad]
    q = jnp.where(inside, ua.astype(BF16).astype(F32), 0.0)
    sides = (from_left(q, left_ok), q, from_right(q, right_ok))
    above = [pltpu.roll(s, cols, 1) for s in sides]
    below = [pltpu.roll(s, length - cols, 1) for s in sides]
    stack = [*above, *sides, *below]
    if extra:
        stack.append(jnp.ones((8, length), F32))
    patches = jnp.concatenate(stack, axis=0).astype(BF16)
    pieces = []
    for at in range(0, length, tile):
        size = min(tile, length - at)
        h = dot(w1t, patches[:, at : at + size])
        h = jnp.maximum(h, 0.0).astype(BF16)
        h = dot(w2t, h)
        b = bias2[...]
        b = jnp.concatenate([b] * (size // 128), axis=1)
        h = jnp.maximum(h + b, 0.0).astype(BF16)
        pieces.append(dot(w3, h))
    taps = jnp.concatenate(pieces, axis=1) if len(pieces) > 1 else pieces[0]
    both = 2 * half
    rows = []
    for dr in range(3):
        a, b, c = (taps[(dr * 3 + dc) * both : (dr * 3 + dc + 1) * both] for dc in range(3))
        rows.append(
            b
            + from_left(a, left_ok)
            + from_right(c, right_ok)
        )
    out = (
        rows[1]
        + jnp.where(up_ok, pltpu.roll(rows[0], cols, 1), 0.0)
        + jnp.where(down_ok, pltpu.roll(rows[2], length - cols, 1), 0.0)
        + bias3
    )
    g, t = out[:half] + 2.0, out[half:]
    if pad > half:
        zeros = jnp.zeros((pad - half, length), F32)
        g, t = jnp.concatenate([g, zeros], axis=0), jnp.concatenate([t, zeros], axis=0)
    return ua, (ub + t) * jax.nn.sigmoid(g), g


def log_sigmoid(g):
    return jnp.minimum(g, 0.0) - jnp.log1p(jnp.exp(-jnp.abs(g)))


def kernel(
    n_rows,
    n_chan,
    images,
    shift_mid_h,
    gain_mid_h,
    lower_mid_h,
    upper_mid_h,
    diag_mid_h,
    first_mid,
    first_bias_mid_h,
    second_mid,
    second_bias_mid_h,
    third_mid,
    third_bias_mid_h,
    shift_top_h,
    gain_top_h,
    lower_top_h,
    upper_top_h,
    diag_top_h,
    first_top,
    first_bias_top_h,
    second_top,
    second_bias_top_h,
    third_top,
    third_bias_top_h,
    latent_mid,
    latent_top,
    loglik,
    img_v,
    w1m,
    w2m,
    w3m,
    w1p,
    w2p,
    w3p,
    w1f_m,
    w1f_p,
    w1m_t,
    w2m_t,
    w1p_t,
    w2p_t,
    b2m,
    b2p,
    mix_m,
    mix_p0,
    mix_p1,
    const_m,
    const_p,
    y_out,
    y_half,
    y_in,
    z_in,
    k_out,
    k_in,
    back_out,
    back_in,
    ll_out,
    ll_in,
    shift_mid,
    gain_mid,
    lower_mid,
    upper_mid,
    diag_mid,
    first_bias_mid,
    second_bias_mid,
    third_bias_mid,
    shift_top,
    gain_top,
    lower_top,
    upper_top,
    diag_top,
    first_bias_top,
    second_bias_top,
    third_bias_top,
    load_sem,
    image_sem,
    small_sem,
    ys_sem,
    yr_sem,
    zs_sem,
    zr_sem,
    ks_sem,
    kr_sem,
    bs_sem,
    br_sem,
    ls_sem,
    lr_sem,
    token_sem,
):
    me_row, me_chan = lax.axis_index("rows"), lax.axis_index("chan")
    steps_m, steps_p = shift_mid.shape[0], shift_top.shape[0]
    n_img, c_mid, width = img_v.shape
    halo = 2 * steps_m
    half_m = c_mid // 2
    c_top = shift_top.shape[1]
    half_p = c_top // 2

    def has_row(d):
        return jnp.logical_and(me_row + d >= 0, me_row + d < n_rows)

    def to_neighbours(src, dst, send_sem, recv_sem):
        copies = []
        for k, d in enumerate((1, -1)):
            copy = pltpu.make_async_remote_copy(
                src_ref=src,
                dst_ref=dst.at[k],
                send_sem=send_sem.at[k],
                recv_sem=recv_sem.at[k],
                device_id={"rows": lax.rem(me_row + d + n_rows, n_rows)},
                device_id_type=MESH,
            )
            pl.when(has_row(d))(copy.start)
            copies.append((copy, d))
        return copies

    def from_neighbours(copies):
        for copy, d in copies:
            pl.when(has_row(-d))(copy.wait_recv)

    def tell_rows(sem, by):
        for d in (by, -by):

            @pl.when(has_row(d))
            def _():
                pl.semaphore_signal(sem, inc=1, device_id={"rows": lax.rem(me_row + d + n_rows, n_rows)}, device_id_type=MESH)

    def rows_off(by):
        return has_row(by).astype(jnp.int32) + has_row(-by).astype(jnp.int32)

    image_load = pltpu.make_async_copy(images, img_v, image_sem)
    image_load.start()
    barrier = pltpu.get_barrier_semaphore()
    far = sorted(range(1, n_chan), key=lambda k: (-(k // 2 == 2), -(k > 1)))
    chan_peers = [me_chan ^ k for k in range(1, n_chan)]
    row_peers = [lax.rem(me_row + k, n_rows) for k in range(1, n_rows)]
    far_rows = sorted(range(1, n_rows), key=lambda k: -min(k, n_rows - k))
    for k in far:
        pl.semaphore_signal(barrier, inc=1, device_id={"chan": chan_peers[k - 1]}, device_id_type=MESH)
    for d in (1, -1):

        @pl.when(has_row(d))
        def _():
            row = lax.rem(me_row + d + n_rows, n_rows)
            for k in (*far, 0):
                pl.semaphore_signal(barrier, inc=1, device_id={"rows": row, "chan": me_chan ^ k}, device_id_type=MESH)


    loads = [
        pltpu.make_async_copy(src, dst, load_sem.at[k])
        for k, (src, dst) in enumerate(
            (
                (first_mid, w1m),
                (second_mid, w2m),
                (third_mid, w3m),
                (first_top, w1p),
                (second_top, w2p),
                (third_top, w3p),
            )
        )
    ]
    smalls = [
        pltpu.make_async_copy(src, dst, small_sem.at[k])
        for k, (src, dst) in enumerate(
            (
                (shift_mid_h, shift_mid),
                (gain_mid_h, gain_mid),
                (lower_mid_h, lower_mid),
                (upper_mid_h, upper_mid),
                (diag_mid_h, diag_mid),
                (first_bias_mid_h, first_bias_mid),
                (second_bias_mid_h, second_bias_mid),
                (third_bias_mid_h, third_bias_mid),
                (shift_top_h, shift_top),
                (gain_top_h, gain_top),
                (lower_top_h, lower_top),
                (upper_top_h, upper_top),
                (diag_top_h, diag_top),
                (first_bias_top_h, first_bias_top),
                (second_bias_top_h, second_bias_top),
                (third_bias_top_h, third_bias_top),
            )
        )
    ]
    for load in (*smalls, *loads):
        load.start()

    image_load.wait()
    for i in range(n_img):
        row = img_v[i]
        packed = [row[8 * k : 8 * k + 8] for k in range(c_mid // 8)]
        packed.append(jnp.zeros((8, 128 - width * (c_mid // 8)), F32))
        y_out[i] = jnp.concatenate(packed, axis=1)
        y_half[i] = y_out[i].astype(BF16)
    y_in[me_chan] = y_out[me_chan]

    pl.semaphore_wait(barrier, n_chan - 1 + n_chan * rows_off(1))
    tell_rows(token_sem.at[0], 1)
    y_copies = {
        c: pltpu.make_async_remote_copy(
            src_ref=y_out.at[me_chan ^ c],
            dst_ref=y_in.at[me_chan],
            send_sem=ys_sem.at[c - 1],
            recv_sem=yr_sem.at[c - 1],
            device_id={"chan": me_chan ^ c},
            device_id_type=MESH,
        )
        for c in far
    }
    z_copies = []
    for k, (d, needed) in enumerate(((1, me_chan >= n_chan - halo), (-1, me_chan < halo))):
        copies = {
            c: pltpu.make_async_remote_copy(
                src_ref=y_half.at[me_chan ^ c],
                dst_ref=z_in.at[k, me_chan],
                send_sem=zs_sem.at[k, c],
                recv_sem=zr_sem.at[k, me_chan],
                device_id={"rows": lax.rem(me_row + d + n_rows, n_rows), "chan": me_chan ^ c},
                device_id_type=MESH,
            )
            for c in (*far, 0)
        }
        z_copies.append((copies, jnp.logical_and(has_row(d), needed)))
    for group in (far[:2], far[2:] + [0]):
        for c in group:
            if c:
                y_copies[c].start()
        for copies, there in z_copies:

            @pl.when(there)
            def _():
                for c in group:
                    copies[c].start()

    y_copies = list(y_copies.values())
    z_copies = [(list(copies.values()), there) for copies, there in z_copies]

    for load in smalls:
        load.wait()
    spread = jnp.where(
        iota2((32, c_mid), 0)
        == iota2((32, c_mid), 1) + jnp.where(iota2((32, c_mid), 1) >= half_m, 16 - half_m, 0),
        1.0,
        0.0,
    )
    src, lane = iota2((c_mid, 96), 0), lax.rem(iota2((c_mid, 96), 1), 32)
    plain = jnp.where(src == lane, 1.0, 0.0)
    padded = jnp.where(src + jnp.where(src >= half_m, 16 - half_m, 0) == lane, 1.0, 0.0)
    for s in range(steps_m):
        mix, const = mixing(
            lower_mid[s],
            upper_mid[s],
            diag_mid[s : s + 1],
            gain_mid[s : s + 1],
            shift_mid[s : s + 1],
            spread,
            plain if s == 0 else padded,
            64,
        )
        mix_m[s] = mix
        const_m[s] = jnp.where(iota2((32, 1), 0) == half_m, 1.0, const)
    src, lane = iota2((c_top, 192), 0), lax.rem(iota2((c_top, 192), 1), 64)
    squeezed_place = jnp.where(
        jnp.logical_and(lax.rem(lane, 16) < half_m, src == 4 * lax.rem(lane, 16) + lax.div(lane, 16)), 1.0, 0.0
    )
    src, lane = iota2((c_top, 144), 0), lax.rem(iota2((c_top, 144), 1), 48)
    top_place = jnp.where(src == lane, 1.0, 0.0)
    for s in range(steps_p):
        mix, const = mixing(
            lower_top[s],
            upper_top[s],
            diag_top[s : s + 1],
            gain_top[s : s + 1],
            shift_top[s : s + 1],
            None,
            squeezed_place if s == 0 else top_place,
            128 if s == 0 else 96,
        )
        if s == 0:
            mix_p0[...] = mix
        else:
            mix_p1[s - 1] = mix
        const_p[s] = const

    def prepare_mid(s):
        w1f_m[...] = jnp.zeros_like(w1f_m)
        for t in range(9):
            w1f_m[16 * t : 16 * t + half_m] = w1m[s, t].astype(F32)
        w1f_m[64 + half_m : 65 + half_m] = first_bias_mid[s : s + 1].astype(F32)
        w1m_t[s] = w1f_m[...].T.astype(BF16)
        w2m_t[s] = w2m[s].T
        b2m[s] = jnp.broadcast_to(second_bias_mid[s : s + 1], (128, b2m.shape[1])).T

    def prepare_top(s):
        w1f_p[9 * half_p :] = jnp.zeros((8, w1f_p.shape[1]), F32)
        w1f_p[: 9 * half_p] = w1p[s].astype(F32)
        w1f_p[9 * half_p : 9 * half_p + 1] = first_bias_top[s : s + 1].astype(F32)
        w1p_t[s] = w1f_p[...].T.astype(BF16)
        w2p_t[s] = w2p[s].T
        b2p[s] = jnp.broadcast_to(second_bias_top[s : s + 1], (128, b2p.shape[1])).T

    for load in loads:
        load.wait()
    for s in range(steps_m):
        prepare_mid(s)
    for s in range(steps_p):
        prepare_top(s)
    bias3_m = [column(third_bias_mid[s : s + 1]) for s in range(steps_m)]
    bias3_p = [column(third_bias_top[s : s + 1]) for s in range(steps_p)]

    for copy in y_copies:
        copy.wait_recv()

    def block(rows):
        groups = [
            jnp.concatenate([r[:, width * k : width * (k + 1)] for r in rows], axis=1) for k in range(c_mid // 8)
        ]
        return jnp.concatenate([*groups, jnp.zeros((32 - c_mid, n_chan * width), F32)], axis=0)

    own = block([y_in[c] for c in range(n_chan)])
    pl.semaphore_wait(token_sem.at[0], rows_off(1))
    tell_rows(token_sem.at[1], 2)
    for k, (d, needed) in enumerate(((1, range(n_chan - halo, n_chan)), (-1, range(halo)))):

        @pl.when(has_row(-d))
        def _():
            for c in needed:
                pltpu.make_async_remote_copy(
                    src_ref=y_half.at[c],
                    dst_ref=z_in.at[k, c],
                    send_sem=zs_sem.at[k, c],
                    recv_sem=zr_sem.at[k, c],
                    device_id={"rows": lax.rem(me_row + d + n_rows, n_rows)},
                    device_id_type=MESH,
                ).wait_recv()

    zero = jnp.zeros_like(own)
    blank = jnp.zeros((8, 128), F32)
    state = jnp.concatenate(
        [
            jnp.where(has_row(-1), block([blank] * (n_chan - halo) + [z_in[0, c].astype(F32) for c in range(n_chan - halo, n_chan)]), zero),
            own,
            jnp.where(has_row(1), block([z_in[1, c].astype(F32) for c in range(halo)] + [blank] * (n_chan - halo)), zero),
        ],
        axis=1,
    )

    height = n_rows * n_chan
    partial = jnp.zeros((8, 128), F32)

    def folded(x):
        total = None
        for i in range(0, x.shape[0], 8):
            for j in range(0, x.shape[1], 128):
                piece = x[i : i + 8, j : j + 128]
                total = piece if total is None else total + piece
        return total

    first_row = me_row * n_chan - n_chan
    own_at = n_chan * width
    own_lanes = n_chan * width
    valid_m = iota2((16, own_lanes), 0) < half_m
    for s in range(steps_m):
        if s == 1:
            state = state[:, 4 * width : 20 * width]
            first_row = first_row + 4
            own_at = own_at - 4 * width
        length = state.shape[1]
        lane = iota2((1, length), 1)
        col, row = lax.rem(lane, width), lax.div(lane, width) + first_row
        u = apply_mix(state, mix_m[s], const_m[s])
        ua, updated, g = coupling(
            u,
            half_m,
            16,
            w1m_t.at[s],
            w2m_t.at[s],
            b2m.at[s],
            w3m.at[s],
            bias3_m[s],
            col >= 1,
            col <= width - 2,
            row >= 1,
            row <= height - 2,
            jnp.logical_and(row >= 0, row < height),
            width,
            512,
            False,
        )
        state = jnp.concatenate([ua, updated], axis=0)
        mine = g[:, own_at : own_at + own_lanes]
        partial = partial + folded(jnp.where(valid_m, log_sigmoid(mine), 0.0))
    kept = state[16:, own_at : own_at + own_lanes]
    k_out[...] = kept.astype(BF16)
    k_copies = to_neighbours(k_out, k_in, ks_sem, kr_sem)
    latent = jnp.where(valid_m, state[:16, own_at : own_at + own_lanes], 0.0)
    partial = partial + folded(-0.5 * latent * latent)

    for c in range(n_chan):
        piece = latent[:, width * c : width * (c + 1)]
        back_out[c] = jnp.concatenate([piece[:8], piece[8:], jnp.zeros((8, 128 - 2 * width), F32)], axis=1)
    back_in[me_chan] = back_out[me_chan]
    back_copies = []
    for k in far:
        peer = chan_peers[k - 1]
        copy = pltpu.make_async_remote_copy(
            src_ref=back_out.at[peer],
            dst_ref=back_in.at[me_chan],
            send_sem=bs_sem.at[k - 1],
            recv_sem=br_sem.at[k - 1],
            device_id={"chan": peer},
            device_id_type=MESH,
        )
        copy.start()
        back_copies.append(copy)

    cols_p = width // 2
    lane = iota2((16, 128), 1)
    phase, rest = lax.div(lane, 32), lax.rem(lane, 32)
    pick = (2 * lax.div(rest, cols_p) + lax.div(phase, 2)) * width + 2 * lax.rem(rest, cols_p) + lax.rem(phase, 2)
    pl.semaphore_wait(token_sem.at[1], rows_off(2))
    tell_rows(token_sem.at[2], 4)
    from_neighbours(k_copies)
    zero = jnp.zeros_like(kept)
    kept = jnp.concatenate(
        [
            jnp.where(has_row(-1), k_in[0].astype(F32), zero),
            kept,
            jnp.where(has_row(1), k_in[1].astype(F32), zero),
        ],
        axis=1,
    )
    blocks = [
        jnp.take_along_axis(kept[:, 128 * k : 128 * k + 128], pick, axis=1) for k in range(kept.shape[1] // 128)
    ]
    phases = []
    for p in range(4):
        parts = [b[:, 32 * p : 32 * p + 32] for b in blocks]
        parts.append(jnp.zeros((16, 256 - 32 * len(blocks)), F32))
        phases.append(jnp.concatenate(parts, axis=1))
    state = jnp.concatenate(phases, axis=0)

    rows_p = n_chan // 2
    first_row = me_row * rows_p - rows_p
    own_at = rows_p * cols_p
    for s in range(steps_p):
        if s == steps_p - 1:
            state = pltpu.roll(state, state.shape[1] - 2 * cols_p, 1)[:, :128]
            first_row, own_at = first_row + 2, own_at - 2 * cols_p
        lane = iota2((1, state.shape[1]), 1)
        col, row = lax.rem(lane, cols_p), lax.div(lane, cols_p) + first_row
        mine_p = jnp.logical_and(lane >= own_at, lane < own_at + rows_p * cols_p)
        u = apply_mix(state, mix_p0[...] if s == 0 else mix_p1[s - 1], const_p[s])
        ua, updated, g = coupling(
            u,
            half_p,
            half_p,
            w1p_t.at[s],
            w2p_t.at[s],
            b2p.at[s],
            w3p.at[s],
            bias3_p[s],
            col >= 1,
            col <= cols_p - 2,
            row >= 1,
            row <= height // 2 - 2,
            jnp.logical_and(row >= 0, row < height // 2),
            cols_p,
            256,
            True,
        )
        state = jnp.concatenate([ua, updated], axis=0)
        partial = partial + folded(jnp.where(mine_p, log_sigmoid(g), 0.0))
    partial = partial + folded(jnp.where(mine_p, -0.5 * state * state, 0.0))
    ll_out[...] = jnp.sum(partial, axis=0, keepdims=True)
    pl.semaphore_wait(token_sem.at[2], rows_off(4))
    ll_copies = []
    for k in far_rows:
        peer = row_peers[k - 1]
        copy = pltpu.make_async_remote_copy(
            src_ref=ll_out,
            dst_ref=ll_in.at[n_rows - 1 - k],
            send_sem=ls_sem.at[k - 1],
            recv_sem=lr_sem.at[n_rows - 1 - k],
            device_id={"rows": peer},
            device_id_type=MESH,
        )
        copy.start()
        ll_copies.append(copy)

    latent_top[...] = state.T[own_at : own_at + rows_p * cols_p]
    for copy in back_copies:
        copy.wait_recv()
    for c in range(n_img):
        piece = back_in[c]
        latent_mid[half_m * c : half_m * c + 8] = piece[:, :width]
        latent_mid[half_m * c + 8 : half_m * (c + 1)] = piece[: half_m - 8, width : 2 * width]
    cells = height * width
    const = sum(
        (
            cells * (jnp.sum(gain_mid[...]) + jnp.sum(diag_mid[...])),
            (cells // 4) * (jnp.sum(gain_top[...]) + jnp.sum(diag_top[...])),
        )
    )
    for copy in ll_copies:
        copy.wait_recv()
    total = ll_out[...]
    for k in range(n_rows - 1):
        total = total + ll_in[k]
    scale = 1.0 / (c_mid * cells)
    loglik[...] = jnp.broadcast_to((jnp.sum(total) + const) * scale - 0.5 * log_two_pi, (1, 128))
    for copy in (*y_copies, *back_copies, *ll_copies):
        copy.wait_send()
    for copies, there in z_copies:

        @pl.when(there)
        def _():
            for copy in copies:
                copy.wait_send()

    for copy, d in k_copies:
        pl.when(has_row(d))(copy.wait_send)


def write_out(*refs):
    sem = refs[-1]
    copies = [pltpu.make_async_copy(refs[k], refs[3 + k], sem.at[k]) for k in range(3)]
    for copy in copies:
        copy.start()
    for copy in copies:
        copy.wait()


def body(
    images,
    shift_mid,
    gain_mid,
    lower_mid,
    upper_mid,
    diag_mid,
    first_mid,
    first_bias_mid,
    second_mid,
    second_bias_mid,
    third_mid,
    third_bias_mid,
    shift_top,
    gain_top,
    lower_top,
    upper_top,
    diag_top,
    first_top,
    first_bias_top,
    second_top,
    second_bias_top,
    third_top,
    third_bias_top,
):
    n_rows, n_chan = lax.axis_size("rows"), lax.axis_size("chan")
    n_img, c_mid, _, width = images.shape
    hid = second_mid.shape[1]
    steps_m, steps_p = shift_mid.shape[0], shift_top.shape[0]
    c_top = shift_top.shape[1]
    half_m, half_p = c_mid // 2, c_top // 2
    images = images.reshape(n_img, c_mid, width)
    third_mid = third_mid.transpose(0, 1, 3, 2).reshape(steps_m, 9 * c_mid, hid)
    third_top = third_top.transpose(0, 1, 3, 2).reshape(steps_p, 9 * c_top, hid)
    first_top = first_top.reshape(steps_p, 9 * half_p, hid)
    big = pl.BlockSpec(memory_space=pltpu.HBM)
    small = pl.BlockSpec(memory_space=pltpu.VMEM)
    rows_p = n_chan // 2
    vmem = pltpu.VMEM
    small_args = (shift_mid, gain_mid, lower_mid, upper_mid, diag_mid, first_bias_mid, second_bias_mid, third_bias_mid, shift_top, gain_top, lower_top, upper_top, diag_top, first_bias_top, second_bias_top, third_bias_top)
    dma = pltpu.SemaphoreType.DMA
    found = pl.pallas_call(
        functools.partial(kernel, n_rows, n_chan),
        out_shape=(
            vmem((n_img * half_m, width), F32),
            vmem((rows_p * width // 2, c_top), F32),
            vmem((1, 128), F32),
        ),
        in_specs=[big] * 23,
        out_specs=(small, small, small),
        scratch_shapes=[
            vmem((n_img, c_mid, width), F32),
            vmem((steps_m, 9, half_m, hid), BF16),
            vmem((steps_m, hid, hid), BF16),
            vmem((steps_m, 9 * c_mid, hid), BF16),
            vmem((steps_p, 9 * half_p, hid), BF16),
            vmem((steps_p, hid, hid), BF16),
            vmem((steps_p, 9 * c_top, hid), BF16),
            vmem((144, hid), F32),
            vmem((9 * half_p + 8, hid), F32),
            vmem((steps_m, hid, 144), BF16),
            vmem((steps_m, hid, hid), BF16),
            vmem((steps_p, hid, 9 * half_p + 8), BF16),
            vmem((steps_p, hid, hid), BF16),
            vmem((steps_m, hid, 128), F32),
            vmem((steps_p, hid, 128), F32),
            vmem((steps_m, 32, 96), BF16),
            vmem((c_top, 192), BF16),
            vmem((steps_p - 1, c_top, 144), BF16),
            vmem((steps_m, 32, 1), F32),
            vmem((steps_p, c_top, 1), F32),
            vmem((n_chan, 8, 128), F32),
            vmem((n_chan, 8, 128), BF16),
            vmem((n_chan, 8, 128), F32),
            vmem((2, n_chan, 8, 128), BF16),
            vmem((16, n_chan * width), BF16),
            vmem((2, 16, n_chan * width), BF16),
            vmem((n_chan, 8, 128), F32),
            vmem((n_chan, 8, 128), F32),
            vmem((1, 128), F32),
            vmem((n_rows - 1, 1, 128), F32),
            *(vmem(a.shape, a.dtype) for a in small_args),
            dma((6,)),
            dma(()),
            dma((len(small_args),)),
            dma((n_chan - 1,)),
            dma((n_chan - 1,)),
            dma((2, n_chan)),
            dma((2, n_chan)),
            dma((2,)),
            dma((2,)),
            dma((n_chan - 1,)),
            dma((n_chan - 1,)),
            dma((n_rows - 1,)),
            dma((n_rows - 1,)),
            pltpu.SemaphoreType.REGULAR((3,)),
        ],
        compiler_params=pltpu.CompilerParams(
            collective_id=0, has_side_effects=True, vmem_limit_bytes=67043328 - 100 * 1024
        ),
    )(
        images,
        shift_mid,
        gain_mid,
        lower_mid,
        upper_mid,
        diag_mid,
        first_mid,
        first_bias_mid,
        second_mid,
        second_bias_mid,
        third_mid,
        third_bias_mid,
        shift_top,
        gain_top,
        lower_top,
        upper_top,
        diag_top,
        first_top,
        first_bias_top,
        second_top,
        second_bias_top,
        third_top,
        third_bias_top,
    )
    latent_mid, latent_top, loglik = pl.pallas_call(
        write_out,
        out_shape=tuple(jax.ShapeDtypeStruct(x.shape, x.dtype) for x in found),
        in_specs=[small] * 3,
        out_specs=(pl.BlockSpec(memory_space=pltpu.HBM),) * 3,
        scratch_shapes=[dma((3,))],
        compiler_params=pltpu.CompilerParams(vmem_limit_bytes=1024 * 1024),
    )(*found)
    latent_mid = latent_mid.reshape(n_img, half_m, 1, width)
    latent_top = latent_top.reshape(1, rows_p, width // 2, c_top).transpose(0, 3, 1, 2)
    return latent_mid, latent_top, loglik[0, :1]


def solution(mesh):
    placed = (P("batch", None, ("rows", "chan"), None),) + (P(),) * 22
    return jax.shard_map(
        body,
        mesh=mesh,
        in_specs=placed,
        out_specs=(
            P("batch", None, ("rows", "chan"), None),
            P(("batch", "chan"), None, "rows", None),
            P(("batch", "chan")),
        ),
        check_vma=False,
    )
```

```python
import functools
import math

import jax
import jax.numpy as jnp
from jax import lax
from jax.experimental import pallas as pl
from jax.experimental.pallas import tpu as pltpu
from jax.sharding import PartitionSpec as P

MESH = pl.DeviceIdType.MESH
F32 = jnp.float32
BF16 = jnp.bfloat16
HI = lax.Precision.HIGHEST
log_two_pi = math.log(2.0 * math.pi)


def iota2(shape, dim):
    return lax.broadcasted_iota(jnp.int32, shape, dim)


def mixing(lower, upper, diag, gain, shift, spread, place, split_at):
    n = lower.shape[0]
    r, c = iota2((n, n), 0), iota2((n, n), 1)
    low = jnp.where(r > c, lower, jnp.where(r == c, 1.0, 0.0))
    up = jnp.where(c > r, upper, jnp.where(r == c, jnp.exp(diag), 0.0)) * jnp.exp(gain)
    both = jnp.dot(low, up, precision=HI, preferred_element_type=F32)
    if spread is not None:
        both = jnp.dot(spread, both, precision=HI, preferred_element_type=F32)
    const = jnp.sum(both * shift, axis=1, keepdims=True)
    wide = jnp.dot(both, place, precision=HI, preferred_element_type=F32)
    high = wide.astype(BF16).astype(F32)
    lane = iota2(wide.shape, 1)
    return jnp.where(lane < split_at, high, wide - high).astype(BF16), const


def column(row):
    n = row.shape[1]
    eye = iota2((n, n), 0) == iota2((n, n), 1)
    return jnp.sum(jnp.where(eye, jnp.broadcast_to(row, (n, n)), 0.0), axis=1, keepdims=True)


def apply_mix(state, mix, const):
    high = state.astype(BF16)
    low = (state - high.astype(F32)).astype(BF16)
    stacked = jnp.concatenate([high, low, high], axis=0)
    return jnp.dot(mix, stacked, preferred_element_type=F32) + const


def dot(w, x):
    if x.shape[1] > 256:
        return jnp.dot(w[...], x, preferred_element_type=F32)
    rows = w.shape[0]
    cut = rows // 16 // 2 * 16
    return jnp.concatenate(
        [
            jnp.dot(w[:cut], x, preferred_element_type=F32),
            jnp.dot(w[cut:], x, preferred_element_type=F32),
        ],
        axis=0,
    )


def shifted(x, by, ok):
    pieces = [pltpu.roll(x[:, at : at + 128], by, 1) for at in range(0, x.shape[1], 128)]
    return jnp.where(ok, jnp.concatenate(pieces, axis=1), 0.0)


def from_left(x, ok):
    return shifted(x, 1, ok)


def from_right(x, ok):
    return shifted(x, 127, ok)


def coupling(u, half, pad, w1t, w2t, bias2, w3, bias3, left_ok, right_ok, up_ok, down_ok, inside, cols, tile, extra):
    length = u.shape[1]
    ua, ub = u[:pad], u[pad : 2 * pad]
    q = jnp.where(inside, ua.astype(BF16).astype(F32), 0.0)
    sides = (from_left(q, left_ok), q, from_right(q, right_ok))
    above = [pltpu.roll(s, cols, 1) for s in sides]
    below = [pltpu.roll(s, length - cols, 1) for s in sides]
    stack = [*above, *sides, *below]
    if extra:
        stack.append(jnp.ones((8, length), F32))
    patches = jnp.concatenate(stack, axis=0).astype(BF16)
    pieces = []
    for at in range(0, length, tile):
        size = min(tile, length - at)
        h = dot(w1t, patches[:, at : at + size])
        h = jnp.maximum(h, 0.0).astype(BF16)
        h = dot(w2t, h)
        b = bias2[...]
        b = jnp.concatenate([b] * (size // 128), axis=1)
        h = jnp.maximum(h + b, 0.0).astype(BF16)
        pieces.append(dot(w3, h))
    taps = jnp.concatenate(pieces, axis=1) if len(pieces) > 1 else pieces[0]
    both = 2 * half
    rows = []
    for dr in range(3):
        a, b, c = (taps[(dr * 3 + dc) * both : (dr * 3 + dc + 1) * both] for dc in range(3))
        rows.append(
            b
            + from_left(a, left_ok)
            + from_right(c, right_ok)
        )
    out = (
        rows[1]
        + jnp.where(up_ok, pltpu.roll(rows[0], cols, 1), 0.0)
        + jnp.where(down_ok, pltpu.roll(rows[2], length - cols, 1), 0.0)
        + bias3
    )
    g, t = out[:half] + 2.0, out[half:]
    if pad > half:
        zeros = jnp.zeros((pad - half, length), F32)
        g, t = jnp.concatenate([g, zeros], axis=0), jnp.concatenate([t, zeros], axis=0)
    return ua, (ub + t) * jax.nn.sigmoid(g), g


def log_sigmoid(g):
    return jnp.minimum(g, 0.0) - jnp.log(1.0 + jnp.exp(-jnp.abs(g)))


def kernel(
    n_rows,
    n_chan,
    images,
    shift_mid_h,
    gain_mid_h,
    lower_mid_h,
    upper_mid_h,
    diag_mid_h,
    first_mid,
    first_bias_mid_h,
    second_mid,
    second_bias_mid_h,
    third_mid,
    third_bias_mid_h,
    shift_top_h,
    gain_top_h,
    lower_top_h,
    upper_top_h,
    diag_top_h,
    first_top,
    first_bias_top_h,
    second_top,
    second_bias_top_h,
    third_top,
    third_bias_top_h,
    latent_mid,
    latent_top,
    loglik,
    img_v,
    w1m,
    w2m,
    w3m,
    w1p,
    w2p,
    w3p,
    w1f_m,
    w1f_p,
    w1m_t,
    w2m_t,
    w1p_t,
    w2p_t,
    b2m,
    b2p,
    mix_m,
    mix_p0,
    mix_p1,
    const_m,
    const_p,
    y_out,
    y_half,
    y_in,
    z_in,
    k_out,
    k_in,
    back_out,
    back_in,
    ll_out,
    ll_in,
    shift_mid,
    gain_mid,
    lower_mid,
    upper_mid,
    diag_mid,
    first_bias_mid,
    second_bias_mid,
    third_bias_mid,
    shift_top,
    gain_top,
    lower_top,
    upper_top,
    diag_top,
    first_bias_top,
    second_bias_top,
    third_bias_top,
    load_sem,
    image_sem,
    small_sem,
    ys_sem,
    yr_sem,
    zs_sem,
    zr_sem,
    ks_sem,
    kr_sem,
    bs_sem,
    br_sem,
    ls_sem,
    lr_sem,
    token_sem,
):
    me_row, me_chan = lax.axis_index("rows"), lax.axis_index("chan")
    steps_m, steps_p = shift_mid.shape[0], shift_top.shape[0]
    n_img, c_mid, width = img_v.shape
    halo = 2 * steps_m
    half_m = c_mid // 2
    c_top = shift_top.shape[1]
    half_p = c_top // 2

    def has_row(d):
        return jnp.logical_and(me_row + d >= 0, me_row + d < n_rows)

    def to_neighbours(src, dst, send_sem, recv_sem):
        copies = []
        for k, d in enumerate((1, -1)):
            copy = pltpu.make_async_remote_copy(
                src_ref=src,
                dst_ref=dst.at[k],
                send_sem=send_sem.at[k],
                recv_sem=recv_sem.at[k],
                device_id={"rows": lax.rem(me_row + d + n_rows, n_rows)},
                device_id_type=MESH,
            )
            pl.when(has_row(d))(copy.start)
            copies.append((copy, d))
        return copies

    def from_neighbours(copies):
        for copy, d in copies:
            pl.when(has_row(-d))(copy.wait_recv)

    def tell_rows(sem, by):
        for d in (by, -by):

            @pl.when(has_row(d))
            def _():
                pl.semaphore_signal(sem, inc=1, device_id={"rows": lax.rem(me_row + d + n_rows, n_rows)}, device_id_type=MESH)

    def rows_off(by):
        return has_row(by).astype(jnp.int32) + has_row(-by).astype(jnp.int32)

    image_load = pltpu.make_async_copy(images, img_v, image_sem)
    image_load.start()
    barrier = pltpu.get_barrier_semaphore()
    far = sorted(range(1, n_chan), key=lambda k: (-(k // 2 == 2), -(k > 1)))
    chan_peers = [me_chan ^ k for k in range(1, n_chan)]

    def tell_block(d, group):
        @pl.when(has_row(d))
        def _():
            for k in group:
                pl.semaphore_signal(
                    barrier, inc=1, device_id={"rows": me_row + d, "chan": me_chan ^ k}, device_id_type=MESH
                )

    def tell_chan(group):
        for k in group:
            pl.semaphore_signal(barrier, inc=1, device_id={"chan": me_chan ^ k}, device_id_type=MESH)

    near = [0, *(k for k in range(1, n_chan) if k // 2 == 0)]
    rest = [k for k in far if k not in near]
    tell_block(-1, near)
    tell_block(1, near)
    tell_chan(far)
    tell_block(-1, rest)
    tell_block(1, rest)

    loads = [
        pltpu.make_async_copy(src, dst, load_sem.at[k])
        for k, (src, dst) in enumerate(
            (
                (first_mid, w1m),
                (second_mid, w2m),
                (third_mid, w3m),
                (first_top, w1p),
                (second_top, w2p),
                (third_top, w3p),
            )
        )
    ]
    smalls = [
        pltpu.make_async_copy(src, dst, small_sem.at[k])
        for k, (src, dst) in enumerate(
            (
                (shift_mid_h, shift_mid),
                (gain_mid_h, gain_mid),
                (lower_mid_h, lower_mid),
                (upper_mid_h, upper_mid),
                (diag_mid_h, diag_mid),
                (first_bias_mid_h, first_bias_mid),
                (second_bias_mid_h, second_bias_mid),
                (third_bias_mid_h, third_bias_mid),
                (shift_top_h, shift_top),
                (gain_top_h, gain_top),
                (lower_top_h, lower_top),
                (upper_top_h, upper_top),
                (diag_top_h, diag_top),
                (first_bias_top_h, first_bias_top),
                (second_bias_top_h, second_bias_top),
                (third_bias_top_h, third_bias_top),
            )
        )
    ]
    for load in (*smalls, *loads):
        load.start()

    image_load.wait()
    for i in range(n_img):
        row = img_v[i]
        packed = [row[8 * k : 8 * k + 8] for k in range(c_mid // 8)]
        packed.append(jnp.zeros((8, 128 - width * (c_mid // 8)), F32))
        y_out[i] = jnp.concatenate(packed, axis=1)
        y_half[i] = y_out[i].astype(BF16)
    y_in[me_chan] = y_out[me_chan]

    for load in smalls:
        load.wait()
    src, lane = iota2((c_top, 192), 0), lax.rem(iota2((c_top, 192), 1), 64)
    squeezed_place = jnp.where(
        jnp.logical_and(lax.rem(lane, 16) < half_m, src == 4 * lax.rem(lane, 16) + lax.div(lane, 16)), 1.0, 0.0
    )
    src, lane = iota2((c_top, 144), 0), lax.rem(iota2((c_top, 144), 1), 48)
    top_place = jnp.where(src == lane, 1.0, 0.0)
    for s in range(steps_p):
        mix, const = mixing(
            lower_top[s],
            upper_top[s],
            diag_top[s : s + 1],
            gain_top[s : s + 1],
            shift_top[s : s + 1],
            None,
            squeezed_place if s == 0 else top_place,
            128 if s == 0 else 96,
        )
        if s == 0:
            mix_p0[...] = mix
        else:
            mix_p1[s - 1] = mix
        const_p[s] = const

    pl.semaphore_wait(barrier, n_chan - 1 + n_chan * rows_off(1))
    tell_rows(token_sem.at[0], 1)
    y_copies = {
        c: pltpu.make_async_remote_copy(
            src_ref=y_out.at[me_chan ^ c],
            dst_ref=y_in.at[me_chan],
            send_sem=ys_sem.at[c - 1],
            recv_sem=yr_sem.at[c - 1],
            device_id={"chan": me_chan ^ c},
            device_id_type=MESH,
        )
        for c in far
    }
    z_copies = []
    for k, (d, needed) in enumerate(((1, me_chan >= n_chan - halo), (-1, me_chan < halo))):
        copies = {
            c: pltpu.make_async_remote_copy(
                src_ref=y_half.at[me_chan ^ c],
                dst_ref=z_in.at[k, me_chan],
                send_sem=zs_sem.at[k, c],
                recv_sem=zr_sem.at[k, me_chan],
                device_id={"rows": lax.rem(me_row + d + n_rows, n_rows), "chan": me_chan ^ c},
                device_id_type=MESH,
            )
            for c in (*far, 0)
        }
        z_copies.append((copies, jnp.logical_and(has_row(d), needed)))
    for group in (far[:2], far[2:] + [0]):
        for c in group:
            if c:
                y_copies[c].start()
        for copies, there in z_copies:

            @pl.when(there)
            def _():
                for c in group:
                    copies[c].start()

    y_copies = list(y_copies.values())
    z_copies = [(list(copies.values()), there) for copies, there in z_copies]

    spread = jnp.where(
        iota2((32, c_mid), 0)
        == iota2((32, c_mid), 1) + jnp.where(iota2((32, c_mid), 1) >= half_m, 16 - half_m, 0),
        1.0,
        0.0,
    )
    src, lane = iota2((c_mid, 96), 0), lax.rem(iota2((c_mid, 96), 1), 32)
    plain = jnp.where(src == lane, 1.0, 0.0)
    padded = jnp.where(src + jnp.where(src >= half_m, 16 - half_m, 0) == lane, 1.0, 0.0)
    for s in range(steps_m):
        mix, const = mixing(
            lower_mid[s],
            upper_mid[s],
            diag_mid[s : s + 1],
            gain_mid[s : s + 1],
            shift_mid[s : s + 1],
            spread,
            plain if s == 0 else padded,
            64,
        )
        mix_m[s] = mix
        const_m[s] = jnp.where(iota2((32, 1), 0) == half_m, 1.0, const)

    def prepare_mid(s):
        w1f_m[...] = jnp.zeros_like(w1f_m)
        for t in range(9):
            w1f_m[16 * t : 16 * t + half_m] = w1m[s, t].astype(F32)
        w1f_m[64 + half_m : 65 + half_m] = first_bias_mid[s : s + 1].astype(F32)
        w1m_t[s] = w1f_m[...].T.astype(BF16)
        w2m_t[s] = w2m[s].T
        b2m[s] = jnp.broadcast_to(second_bias_mid[s : s + 1], (128, b2m.shape[1])).T

    def prepare_top(s):
        w1f_p[9 * half_p :] = jnp.zeros((8, w1f_p.shape[1]), F32)
        w1f_p[: 9 * half_p] = w1p[s].astype(F32)
        w1f_p[9 * half_p : 9 * half_p + 1] = first_bias_top[s : s + 1].astype(F32)
        w1p_t[s] = w1f_p[...].T.astype(BF16)
        w2p_t[s] = w2p[s].T
        b2p[s] = jnp.broadcast_to(second_bias_top[s : s + 1], (128, b2p.shape[1])).T

    for load in loads:
        load.wait()
    for s in range(steps_m):
        prepare_mid(s)
    for s in range(steps_p):
        prepare_top(s)
    bias3_m = [column(third_bias_mid[s : s + 1]) for s in range(steps_m)]
    bias3_p = [column(third_bias_top[s : s + 1]) for s in range(steps_p)]

    for copy in y_copies:
        copy.wait_recv()

    def block(rows):
        groups = [
            jnp.concatenate([r[:, width * k : width * (k + 1)] for r in rows], axis=1) for k in range(c_mid // 8)
        ]
        return jnp.concatenate([*groups, jnp.zeros((32 - c_mid, n_chan * width), F32)], axis=0)

    own = block([y_in[c] for c in range(n_chan)])
    pl.semaphore_wait(token_sem.at[0], rows_off(1))
    tell_rows(token_sem.at[1], 2)
    for k, (d, needed) in enumerate(((1, range(n_chan - halo, n_chan)), (-1, range(halo)))):

        @pl.when(has_row(-d))
        def _():
            for c in needed:
                pltpu.make_async_remote_copy(
                    src_ref=y_half.at[c],
                    dst_ref=z_in.at[k, c],
                    send_sem=zs_sem.at[k, c],
                    recv_sem=zr_sem.at[k, c],
                    device_id={"rows": lax.rem(me_row + d + n_rows, n_rows)},
                    device_id_type=MESH,
                ).wait_recv()

    zero = jnp.zeros_like(own)
    blank = jnp.zeros((8, 128), F32)
    state = jnp.concatenate(
        [
            jnp.where(has_row(-1), block([blank] * (n_chan - halo) + [z_in[0, c].astype(F32) for c in range(n_chan - halo, n_chan)]), zero),
            own,
            jnp.where(has_row(1), block([z_in[1, c].astype(F32) for c in range(halo)] + [blank] * (n_chan - halo)), zero),
        ],
        axis=1,
    )

    height = n_rows * n_chan
    partial = jnp.zeros((8, 128), F32)

    def folded(x):
        total = None
        for i in range(0, x.shape[0], 8):
            for j in range(0, x.shape[1], 128):
                piece = x[i : i + 8, j : j + 128]
                total = piece if total is None else total + piece
        return total

    first_row = me_row * n_chan - n_chan
    own_at = n_chan * width
    own_lanes = n_chan * width
    valid_m = iota2((16, own_lanes), 0) < half_m
    for s in range(steps_m):
        if s == 1:
            state = state[:, 4 * width : 20 * width]
            first_row = first_row + 4
            own_at = own_at - 4 * width
        length = state.shape[1]
        lane = iota2((1, length), 1)
        col, row = lax.rem(lane, width), lax.div(lane, width) + first_row
        u = apply_mix(state, mix_m[s], const_m[s])
        ua, updated, g = coupling(
            u,
            half_m,
            16,
            w1m_t.at[s],
            w2m_t.at[s],
            b2m.at[s],
            w3m.at[s],
            bias3_m[s],
            col >= 1,
            col <= width - 2,
            row >= 1,
            row <= height - 2,
            jnp.logical_and(row >= 0, row < height),
            width,
            512,
            False,
        )
        state = jnp.concatenate([ua, updated], axis=0)
        mine = g[:, own_at : own_at + own_lanes]
        if s < steps_m - 1:
            partial = partial + folded(jnp.where(valid_m, log_sigmoid(mine), 0.0))
    kept = state[16:, own_at : own_at + own_lanes]
    k_out[...] = kept.astype(BF16)
    k_copies = to_neighbours(k_out, k_in, ks_sem, kr_sem)
    partial = partial + folded(jnp.where(valid_m, log_sigmoid(mine), 0.0))
    latent = jnp.where(valid_m, state[:16, own_at : own_at + own_lanes], 0.0)
    partial = partial + folded(-0.5 * latent * latent)

    for c in range(n_chan):
        piece = latent[:, width * c : width * (c + 1)]
        back_out[c] = jnp.concatenate([piece[:8], piece[8:], jnp.zeros((8, 128 - 2 * width), F32)], axis=1)
    back_in[me_chan] = back_out[me_chan]
    back_copies = []
    for k in far:
        peer = chan_peers[k - 1]
        copy = pltpu.make_async_remote_copy(
            src_ref=back_out.at[peer],
            dst_ref=back_in.at[me_chan],
            send_sem=bs_sem.at[k - 1],
            recv_sem=br_sem.at[k - 1],
            device_id={"chan": peer},
            device_id_type=MESH,
        )
        copy.start()
        back_copies.append(copy)

    cols_p = width // 2
    lane = iota2((16, 128), 1)
    phase, rest = lax.div(lane, 32), lax.rem(lane, 32)
    pick = (2 * lax.div(rest, cols_p) + lax.div(phase, 2)) * width + 2 * lax.rem(rest, cols_p) + lax.rem(phase, 2)
    pl.semaphore_wait(token_sem.at[1], rows_off(2))
    tell_rows(token_sem.at[2], 4)
    from_neighbours(k_copies)
    zero = jnp.zeros_like(kept)
    kept = jnp.concatenate(
        [
            jnp.where(has_row(-1), k_in[0].astype(F32), zero),
            kept,
            jnp.where(has_row(1), k_in[1].astype(F32), zero),
        ],
        axis=1,
    )
    blocks = [
        jnp.take_along_axis(kept[:, 128 * k : 128 * k + 128], pick, axis=1) for k in range(kept.shape[1] // 128)
    ]
    phases = []
    for p in range(4):
        parts = [b[:, 32 * p : 32 * p + 32] for b in blocks]
        parts.append(jnp.zeros((16, 256 - 32 * len(blocks)), F32))
        phases.append(jnp.concatenate(parts, axis=1))
    state = jnp.concatenate(phases, axis=0)

    rows_p = n_chan // 2
    first_row = me_row * rows_p - rows_p
    own_at = rows_p * cols_p
    for s in range(steps_p):
        if s == steps_p - 1:
            state = pltpu.roll(state, state.shape[1] - 2 * cols_p, 1)[:, :128]
            first_row, own_at = first_row + 2, own_at - 2 * cols_p
        lane = iota2((1, state.shape[1]), 1)
        col, row = lax.rem(lane, cols_p), lax.div(lane, cols_p) + first_row
        mine_p = jnp.logical_and(lane >= own_at, lane < own_at + rows_p * cols_p)
        u = apply_mix(state, mix_p0[...] if s == 0 else mix_p1[s - 1], const_p[s])
        ua, updated, g = coupling(
            u,
            half_p,
            half_p,
            w1p_t.at[s],
            w2p_t.at[s],
            b2p.at[s],
            w3p.at[s],
            bias3_p[s],
            col >= 1,
            col <= cols_p - 2,
            row >= 1,
            row <= height // 2 - 2,
            jnp.logical_and(row >= 0, row < height // 2),
            cols_p,
            256,
            True,
        )
        state = jnp.concatenate([ua, updated], axis=0)
        partial = partial + folded(jnp.where(mine_p, log_sigmoid(g), 0.0))
    partial = partial + folded(jnp.where(mine_p, -0.5 * state * state, 0.0))
    ll_out[...] = jnp.sum(partial, axis=0, keepdims=True)
    pl.semaphore_wait(token_sem.at[2], rows_off(4))
    row_peers = [lax.rem(me_row + k, n_rows) for k in range(1, n_rows)]
    far_rows = sorted(range(1, n_rows), key=lambda k: -min(k, n_rows - k))
    ll_copies = []
    for k in far_rows:
        peer = row_peers[k - 1]
        copy = pltpu.make_async_remote_copy(
            src_ref=ll_out,
            dst_ref=ll_in.at[n_rows - 1 - k],
            send_sem=ls_sem.at[k - 1],
            recv_sem=lr_sem.at[n_rows - 1 - k],
            device_id={"rows": peer},
            device_id_type=MESH,
        )
        copy.start()
        ll_copies.append(copy)

    latent_top[...] = state.T[own_at : own_at + rows_p * cols_p]
    for copy in back_copies:
        copy.wait_recv()
    for c in range(n_img):
        piece = back_in[c]
        latent_mid[half_m * c : half_m * c + 8] = piece[:, :width]
        latent_mid[half_m * c + 8 : half_m * (c + 1)] = piece[: half_m - 8, width : 2 * width]
    cells = height * width
    const = sum(
        (
            cells * (jnp.sum(gain_mid[...]) + jnp.sum(diag_mid[...])),
            (cells // 4) * (jnp.sum(gain_top[...]) + jnp.sum(diag_top[...])),
        )
    )
    for copy in ll_copies:
        copy.wait_recv()
    total = ll_out[...]
    for k in range(n_rows - 1):
        total = total + ll_in[k]
    scale = 1.0 / (c_mid * cells)
    loglik[...] = jnp.broadcast_to((jnp.sum(total) + const) * scale - 0.5 * log_two_pi, (1, 128))
    for copy in (*y_copies, *back_copies, *ll_copies):
        copy.wait_send()
    for copies, there in z_copies:

        @pl.when(there)
        def _():
            for copy in copies:
                copy.wait_send()

    for copy, d in k_copies:
        pl.when(has_row(d))(copy.wait_send)


def write_out(*refs):
    sem = refs[-1]
    copies = [pltpu.make_async_copy(refs[k], refs[3 + k], sem.at[k]) for k in range(3)]
    for copy in copies:
        copy.start()
    for copy in copies:
        copy.wait()


def body(
    images,
    shift_mid,
    gain_mid,
    lower_mid,
    upper_mid,
    diag_mid,
    first_mid,
    first_bias_mid,
    second_mid,
    second_bias_mid,
    third_mid,
    third_bias_mid,
    shift_top,
    gain_top,
    lower_top,
    upper_top,
    diag_top,
    first_top,
    first_bias_top,
    second_top,
    second_bias_top,
    third_top,
    third_bias_top,
):
    n_rows, n_chan = lax.axis_size("rows"), lax.axis_size("chan")
    n_img, c_mid, _, width = images.shape
    hid = second_mid.shape[1]
    steps_m, steps_p = shift_mid.shape[0], shift_top.shape[0]
    c_top = shift_top.shape[1]
    half_m, half_p = c_mid // 2, c_top // 2
    images = images.reshape(n_img, c_mid, width)
    third_mid = third_mid.transpose(0, 1, 3, 2).reshape(steps_m, 9 * c_mid, hid)
    third_top = third_top.transpose(0, 1, 3, 2).reshape(steps_p, 9 * c_top, hid)
    first_top = first_top.reshape(steps_p, 9 * half_p, hid)
    big = pl.BlockSpec(memory_space=pltpu.HBM)
    small = pl.BlockSpec(memory_space=pltpu.VMEM)
    rows_p = n_chan // 2
    vmem = pltpu.VMEM
    small_args = (shift_mid, gain_mid, lower_mid, upper_mid, diag_mid, first_bias_mid, second_bias_mid, third_bias_mid, shift_top, gain_top, lower_top, upper_top, diag_top, first_bias_top, second_bias_top, third_bias_top)
    dma = pltpu.SemaphoreType.DMA
    found = pl.pallas_call(
        functools.partial(kernel, n_rows, n_chan),
        out_shape=(
            vmem((n_img * half_m, width), F32),
            vmem((rows_p * width // 2, c_top), F32),
            vmem((1, 128), F32),
        ),
        in_specs=[big] * 23,
        out_specs=(small, small, small),
        scratch_shapes=[
            vmem((n_img, c_mid, width), F32),
            vmem((steps_m, 9, half_m, hid), BF16),
            vmem((steps_m, hid, hid), BF16),
            vmem((steps_m, 9 * c_mid, hid), BF16),
            vmem((steps_p, 9 * half_p, hid), BF16),
            vmem((steps_p, hid, hid), BF16),
            vmem((steps_p, 9 * c_top, hid), BF16),
            vmem((144, hid), F32),
            vmem((9 * half_p + 8, hid), F32),
            vmem((steps_m, hid, 144), BF16),
            vmem((steps_m, hid, hid), BF16),
            vmem((steps_p, hid, 9 * half_p + 8), BF16),
            vmem((steps_p, hid, hid), BF16),
            vmem((steps_m, hid, 128), F32),
            vmem((steps_p, hid, 128), F32),
            vmem((steps_m, 32, 96), BF16),
            vmem((c_top, 192), BF16),
            vmem((steps_p - 1, c_top, 144), BF16),
            vmem((steps_m, 32, 1), F32),
            vmem((steps_p, c_top, 1), F32),
            vmem((n_chan, 8, 128), F32),
            vmem((n_chan, 8, 128), BF16),
            vmem((n_chan, 8, 128), F32),
            vmem((2, n_chan, 8, 128), BF16),
            vmem((16, n_chan * width), BF16),
            vmem((2, 16, n_chan * width), BF16),
            vmem((n_chan, 8, 128), F32),
            vmem((n_chan, 8, 128), F32),
            vmem((1, 128), F32),
            vmem((n_rows - 1, 1, 128), F32),
            *(vmem(a.shape, a.dtype) for a in small_args),
            dma((6,)),
            dma(()),
            dma((len(small_args),)),
            dma((n_chan - 1,)),
            dma((n_chan - 1,)),
            dma((2, n_chan)),
            dma((2, n_chan)),
            dma((2,)),
            dma((2,)),
            dma((n_chan - 1,)),
            dma((n_chan - 1,)),
            dma((n_rows - 1,)),
            dma((n_rows - 1,)),
            pltpu.SemaphoreType.REGULAR((3,)),
        ],
        compiler_params=pltpu.CompilerParams(
            collective_id=0, has_side_effects=True, vmem_limit_bytes=67043328 - 100 * 1024
        ),
    )(
        images,
        shift_mid,
        gain_mid,
        lower_mid,
        upper_mid,
        diag_mid,
        first_mid,
        first_bias_mid,
        second_mid,
        second_bias_mid,
        third_mid,
        third_bias_mid,
        shift_top,
        gain_top,
        lower_top,
        upper_top,
        diag_top,
        first_top,
        first_bias_top,
        second_top,
        second_bias_top,
        third_top,
        third_bias_top,
    )
    latent_mid, latent_top, loglik = pl.pallas_call(
        write_out,
        out_shape=tuple(jax.ShapeDtypeStruct(x.shape, x.dtype) for x in found),
        in_specs=[small] * 3,
        out_specs=(pl.BlockSpec(memory_space=pltpu.HBM),) * 3,
        scratch_shapes=[dma((3,))],
        compiler_params=pltpu.CompilerParams(vmem_limit_bytes=1024 * 1024),
    )(*found)
    latent_mid = latent_mid.reshape(n_img, half_m, 1, width)
    latent_top = latent_top.reshape(1, rows_p, width // 2, c_top).transpose(0, 3, 1, 2)
    return latent_mid, latent_top, loglik[0, :1]


def solution(mesh):
    placed = (P("batch", None, ("rows", "chan"), None),) + (P(),) * 22
    return jax.shard_map(
        body,
        mesh=mesh,
        in_specs=placed,
        out_specs=(
            P("batch", None, ("rows", "chan"), None),
            P(("batch", "chan"), None, "rows", None),
            P(("batch", "chan")),
        ),
        check_vma=False,
    )
```

```python
import functools
import math

import jax
import jax.numpy as jnp
from jax import lax
from jax.experimental import pallas as pl
from jax.experimental.pallas import tpu as pltpu
from jax.sharding import PartitionSpec as P

MESH = pl.DeviceIdType.MESH
F32 = jnp.float32
BF16 = jnp.bfloat16
HI = lax.Precision.HIGHEST
log_two_pi = math.log(2.0 * math.pi)


def iota2(shape, dim):
    return lax.broadcasted_iota(jnp.int32, shape, dim)


def mixing(lower, upper, diag, gain, shift, spread, place, split_at):
    n = lower.shape[0]
    r, c = iota2((n, n), 0), iota2((n, n), 1)
    low = jnp.where(r > c, lower, jnp.where(r == c, 1.0, 0.0))
    up = jnp.where(c > r, upper, jnp.where(r == c, jnp.exp(diag), 0.0)) * jnp.exp(gain)
    both = jnp.dot(low, up, precision=HI, preferred_element_type=F32)
    if spread is not None:
        both = jnp.dot(spread, both, precision=HI, preferred_element_type=F32)
    const = jnp.sum(both * shift, axis=1, keepdims=True)
    wide = jnp.dot(both, place, precision=HI, preferred_element_type=F32)
    high = wide.astype(BF16).astype(F32)
    lane = iota2(wide.shape, 1)
    return jnp.where(lane < split_at, high, wide - high).astype(BF16), const


def column(row):
    n = row.shape[1]
    eye = iota2((n, n), 0) == iota2((n, n), 1)
    return jnp.sum(jnp.where(eye, jnp.broadcast_to(row, (n, n)), 0.0), axis=1, keepdims=True)


def apply_mix(state, mix, const):
    high = state.astype(BF16)
    low = (state - high.astype(F32)).astype(BF16)
    stacked = jnp.concatenate([high, low, high], axis=0)
    return jnp.dot(mix, stacked, preferred_element_type=F32) + const


def dot(w, x):
    if x.shape[1] > 256:
        return jnp.dot(w[...], x, preferred_element_type=F32)
    rows = w.shape[0]
    cut = rows // 16 // 2 * 16
    return jnp.concatenate(
        [
            jnp.dot(w[:cut], x, preferred_element_type=F32),
            jnp.dot(w[cut:], x, preferred_element_type=F32),
        ],
        axis=0,
    )


def shifted(x, by, ok):
    pieces = [pltpu.roll(x[:, at : at + 128], by, 1) for at in range(0, x.shape[1], 128)]
    return jnp.where(ok, jnp.concatenate(pieces, axis=1), 0.0)


def from_left(x, ok):
    return shifted(x, 1, ok)


def from_right(x, ok):
    return shifted(x, 127, ok)


def coupling(u, half, pad, w1t, w2t, bias2, w3, bias3, left_ok, right_ok, up_ok, down_ok, inside, cols, tile, extra):
    length = u.shape[1]
    ua, ub = u[:pad], u[pad : 2 * pad]
    q = jnp.where(inside, ua.astype(BF16).astype(F32), 0.0)
    sides = (from_left(q, left_ok), q, from_right(q, right_ok))
    above = [pltpu.roll(s, cols, 1) for s in sides]
    below = [pltpu.roll(s, length - cols, 1) for s in sides]
    stack = [*above, *sides, *below]
    if extra:
        stack.append(jnp.ones((8, length), F32))
    patches = jnp.concatenate(stack, axis=0).astype(BF16)
    pieces = []
    for at in range(0, length, tile):
        size = min(tile, length - at)
        h = dot(w1t, patches[:, at : at + size])
        h = jnp.maximum(h, 0.0).astype(BF16)
        h = dot(w2t, h)
        b = bias2[...]
        b = jnp.concatenate([b] * (size // 128), axis=1)
        h = jnp.maximum(h + b, 0.0).astype(BF16)
        pieces.append(dot(w3, h))
    taps = jnp.concatenate(pieces, axis=1) if len(pieces) > 1 else pieces[0]
    both = 2 * half
    rows = []
    for dr in range(3):
        a, b, c = (taps[(dr * 3 + dc) * both : (dr * 3 + dc + 1) * both] for dc in range(3))
        rows.append(
            b
            + from_left(a, left_ok)
            + from_right(c, right_ok)
        )
    out = (
        rows[1]
        + jnp.where(up_ok, pltpu.roll(rows[0], cols, 1), 0.0)
        + jnp.where(down_ok, pltpu.roll(rows[2], length - cols, 1), 0.0)
        + bias3
    )
    g, t = out[:half] + 2.0, out[half:]
    if pad > half:
        zeros = jnp.zeros((pad - half, length), F32)
        g, t = jnp.concatenate([g, zeros], axis=0), jnp.concatenate([t, zeros], axis=0)
    return ua, (ub + t) * jax.nn.sigmoid(g), g


def log_sigmoid(g):
    return jnp.minimum(g, 0.0) - jnp.log(1.0 + jnp.exp(-jnp.abs(g)))


def kernel(
    n_rows,
    n_chan,
    images,
    shift_mid_h,
    gain_mid_h,
    lower_mid_h,
    upper_mid_h,
    diag_mid_h,
    first_mid,
    first_bias_mid_h,
    second_mid,
    second_bias_mid_h,
    third_mid,
    third_bias_mid_h,
    shift_top_h,
    gain_top_h,
    lower_top_h,
    upper_top_h,
    diag_top_h,
    first_top,
    first_bias_top_h,
    second_top,
    second_bias_top_h,
    third_top,
    third_bias_top_h,
    latent_mid,
    latent_top,
    loglik,
    img_v,
    w1m,
    w2m,
    w3m,
    w1p,
    w2p,
    w3p,
    w1f_m,
    w1f_p,
    w1m_t,
    w2m_t,
    w1p_t,
    w2p_t,
    b2m,
    b2p,
    mix_m,
    mix_p0,
    mix_p1,
    const_m,
    const_p,
    y_out,
    y_half,
    y_in,
    z_in,
    k_out,
    k_in,
    back_out,
    back_in,
    ll_out,
    ll_in,
    shift_mid,
    gain_mid,
    lower_mid,
    upper_mid,
    diag_mid,
    first_bias_mid,
    second_bias_mid,
    third_bias_mid,
    shift_top,
    gain_top,
    lower_top,
    upper_top,
    diag_top,
    first_bias_top,
    second_bias_top,
    third_bias_top,
    load_sem,
    image_sem,
    small_sem,
    ys_sem,
    yr_sem,
    zs_sem,
    zr_sem,
    ks_sem,
    kr_sem,
    bs_sem,
    br_sem,
    ls_sem,
    lr_sem,
    token_sem,
):
    me_row, me_chan = lax.axis_index("rows"), lax.axis_index("chan")
    steps_m, steps_p = shift_mid.shape[0], shift_top.shape[0]
    n_img, c_mid, width = img_v.shape
    halo = 2 * steps_m
    half_m = c_mid // 2
    c_top = shift_top.shape[1]
    half_p = c_top // 2

    def has_row(d):
        return jnp.logical_and(me_row + d >= 0, me_row + d < n_rows)

    def to_neighbours(src, dst, send_sem, recv_sem):
        copies = []
        for k, d in enumerate((1, -1)):
            copy = pltpu.make_async_remote_copy(
                src_ref=src,
                dst_ref=dst.at[k],
                send_sem=send_sem.at[k],
                recv_sem=recv_sem.at[k],
                device_id={"rows": lax.rem(me_row + d + n_rows, n_rows)},
                device_id_type=MESH,
            )
            pl.when(has_row(d))(copy.start)
            copies.append((copy, d))
        return copies

    def from_neighbours(copies):
        for copy, d in copies:
            pl.when(has_row(-d))(copy.wait_recv)

    def tell_rows(sem, by):
        for d in (by, -by):

            @pl.when(has_row(d))
            def _():
                pl.semaphore_signal(sem, inc=1, device_id={"rows": lax.rem(me_row + d + n_rows, n_rows)}, device_id_type=MESH)

    def rows_off(by):
        return has_row(by).astype(jnp.int32) + has_row(-by).astype(jnp.int32)

    image_load = pltpu.make_async_copy(images, img_v, image_sem)
    image_load.start()
    barrier = pltpu.get_barrier_semaphore()
    far = sorted(range(1, n_chan), key=lambda k: (-(k // 2 == 2), -(k > 1)))
    chan_peers = [me_chan ^ k for k in range(1, n_chan)]

    def tell_block(d, group):
        @pl.when(has_row(d))
        def _():
            for k in group:
                pl.semaphore_signal(
                    barrier, inc=1, device_id={"rows": me_row + d, "chan": me_chan ^ k}, device_id_type=MESH
                )

    def tell_chan(group):
        for k in group:
            pl.semaphore_signal(barrier, inc=1, device_id={"chan": me_chan ^ k}, device_id_type=MESH)

    near = [0, *(k for k in range(1, n_chan) if k // 2 == 0)]
    rest = [k for k in far if k not in near]
    tell_block(-1, near)
    tell_block(1, near)
    tell_chan(far)
    tell_block(-1, rest)
    tell_block(1, rest)

    loads = [
        pltpu.make_async_copy(src, dst, load_sem.at[k])
        for k, (src, dst) in enumerate(
            (
                (first_mid, w1m),
                (second_mid, w2m),
                (third_mid, w3m),
                (first_top, w1p),
                (second_top, w2p),
                (third_top, w3p),
            )
        )
    ]
    smalls = [
        pltpu.make_async_copy(src, dst, small_sem.at[k])
        for k, (src, dst) in enumerate(
            (
                (shift_mid_h, shift_mid),
                (gain_mid_h, gain_mid),
                (lower_mid_h, lower_mid),
                (upper_mid_h, upper_mid),
                (diag_mid_h, diag_mid),
                (first_bias_mid_h, first_bias_mid),
                (second_bias_mid_h, second_bias_mid),
                (third_bias_mid_h, third_bias_mid),
                (shift_top_h, shift_top),
                (gain_top_h, gain_top),
                (lower_top_h, lower_top),
                (upper_top_h, upper_top),
                (diag_top_h, diag_top),
                (first_bias_top_h, first_bias_top),
                (second_bias_top_h, second_bias_top),
                (third_bias_top_h, third_bias_top),
            )
        )
    ]
    for load in (*smalls, *loads):
        load.start()

    image_load.wait()
    for i in range(n_img):
        row = img_v[i]
        packed = [row[8 * k : 8 * k + 8] for k in range(c_mid // 8)]
        packed.append(jnp.zeros((8, 128 - width * (c_mid // 8)), F32))
        y_out[i] = jnp.concatenate(packed, axis=1)
        y_half[i] = y_out[i].astype(BF16)
    y_in[me_chan] = y_out[me_chan]

    pl.semaphore_wait(barrier, n_chan - 1 + n_chan * rows_off(1))
    tell_rows(token_sem.at[0], 1)
    y_copies = {
        c: pltpu.make_async_remote_copy(
            src_ref=y_out.at[me_chan ^ c],
            dst_ref=y_in.at[me_chan],
            send_sem=ys_sem.at[c - 1],
            recv_sem=yr_sem.at[c - 1],
            device_id={"chan": me_chan ^ c},
            device_id_type=MESH,
        )
        for c in far
    }
    z_copies = []
    for k, (d, needed) in enumerate(((1, me_chan >= n_chan - halo), (-1, me_chan < halo))):
        copies = {
            c: pltpu.make_async_remote_copy(
                src_ref=y_half.at[me_chan ^ c],
                dst_ref=z_in.at[k, me_chan],
                send_sem=zs_sem.at[k, c],
                recv_sem=zr_sem.at[k, me_chan],
                device_id={"rows": lax.rem(me_row + d + n_rows, n_rows), "chan": me_chan ^ c},
                device_id_type=MESH,
            )
            for c in (*far, 0)
        }
        z_copies.append((copies, jnp.logical_and(has_row(d), needed)))
    for group in (far[:2], far[2:] + [0]):
        for c in group:
            if c:
                y_copies[c].start()
        for copies, there in z_copies:

            @pl.when(there)
            def _():
                for c in group:
                    copies[c].start()

    y_copies = list(y_copies.values())
    z_copies = [(list(copies.values()), there) for copies, there in z_copies]

    for load in smalls:
        load.wait()
    spread = jnp.where(
        iota2((32, c_mid), 0)
        == iota2((32, c_mid), 1) + jnp.where(iota2((32, c_mid), 1) >= half_m, 16 - half_m, 0),
        1.0,
        0.0,
    )
    src, lane = iota2((c_mid, 96), 0), lax.rem(iota2((c_mid, 96), 1), 32)
    plain = jnp.where(src == lane, 1.0, 0.0)
    padded = jnp.where(src + jnp.where(src >= half_m, 16 - half_m, 0) == lane, 1.0, 0.0)
    for s in range(steps_m):
        mix, const = mixing(
            lower_mid[s],
            upper_mid[s],
            diag_mid[s : s + 1],
            gain_mid[s : s + 1],
            shift_mid[s : s + 1],
            spread,
            plain if s == 0 else padded,
            64,
        )
        mix_m[s] = mix
        const_m[s] = jnp.where(iota2((32, 1), 0) == half_m, 1.0, const)

    src, lane = iota2((c_top, 192), 0), lax.rem(iota2((c_top, 192), 1), 64)
    squeezed_place = jnp.where(
        jnp.logical_and(lax.rem(lane, 16) < half_m, src == 4 * lax.rem(lane, 16) + lax.div(lane, 16)), 1.0, 0.0
    )
    src, lane = iota2((c_top, 144), 0), lax.rem(iota2((c_top, 144), 1), 48)
    top_place = jnp.where(src == lane, 1.0, 0.0)
    for s in range(steps_p):
        mix, const = mixing(
            lower_top[s],
            upper_top[s],
            diag_top[s : s + 1],
            gain_top[s : s + 1],
            shift_top[s : s + 1],
            None,
            squeezed_place if s == 0 else top_place,
            128 if s == 0 else 96,
        )
        if s == 0:
            mix_p0[...] = mix
        else:
            mix_p1[s - 1] = mix
        const_p[s] = const

    def prepare_mid(s):
        w1f_m[...] = jnp.zeros_like(w1f_m)
        for t in range(9):
            w1f_m[16 * t : 16 * t + half_m] = w1m[s, t].astype(F32)
        w1f_m[64 + half_m : 65 + half_m] = first_bias_mid[s : s + 1].astype(F32)
        w1m_t[s] = w1f_m[...].T.astype(BF16)
        w2m_t[s] = w2m[s].T
        b2m[s] = jnp.broadcast_to(second_bias_mid[s : s + 1], (128, b2m.shape[1])).T

    def prepare_top(s):
        w1f_p[9 * half_p :] = jnp.zeros((8, w1f_p.shape[1]), F32)
        w1f_p[: 9 * half_p] = w1p[s].astype(F32)
        w1f_p[9 * half_p : 9 * half_p + 1] = first_bias_top[s : s + 1].astype(F32)
        w1p_t[s] = w1f_p[...].T.astype(BF16)
        w2p_t[s] = w2p[s].T
        b2p[s] = jnp.broadcast_to(second_bias_top[s : s + 1], (128, b2p.shape[1])).T

    for load in loads:
        load.wait()
    for s in range(steps_m):
        prepare_mid(s)
    for s in range(steps_p):
        prepare_top(s)
    bias3_m = [column(third_bias_mid[s : s + 1]) for s in range(steps_m)]
    bias3_p = [column(third_bias_top[s : s + 1]) for s in range(steps_p)]

    for copy in y_copies:
        copy.wait_recv()

    def block(rows):
        groups = [
            jnp.concatenate([r[:, width * k : width * (k + 1)] for r in rows], axis=1) for k in range(c_mid // 8)
        ]
        return jnp.concatenate([*groups, jnp.zeros((32 - c_mid, n_chan * width), F32)], axis=0)

    own = block([y_in[c] for c in range(n_chan)])
    pl.semaphore_wait(token_sem.at[0], rows_off(1))
    tell_rows(token_sem.at[1], 2)
    for k, (d, needed) in enumerate(((1, range(n_chan - halo, n_chan)), (-1, range(halo)))):

        @pl.when(has_row(-d))
        def _():
            for c in needed:
                pltpu.make_async_remote_copy(
                    src_ref=y_half.at[c],
                    dst_ref=z_in.at[k, c],
                    send_sem=zs_sem.at[k, c],
                    recv_sem=zr_sem.at[k, c],
                    device_id={"rows": lax.rem(me_row + d + n_rows, n_rows)},
                    device_id_type=MESH,
                ).wait_recv()

    zero = jnp.zeros_like(own)
    blank = jnp.zeros((8, 128), F32)
    state = jnp.concatenate(
        [
            jnp.where(has_row(-1), block([blank] * (n_chan - halo) + [z_in[0, c].astype(F32) for c in range(n_chan - halo, n_chan)]), zero),
            own,
            jnp.where(has_row(1), block([z_in[1, c].astype(F32) for c in range(halo)] + [blank] * (n_chan - halo)), zero),
        ],
        axis=1,
    )

    height = n_rows * n_chan
    partial = jnp.zeros((8, 128), F32)

    def folded(x):
        total = None
        for i in range(0, x.shape[0], 8):
            for j in range(0, x.shape[1], 128):
                piece = x[i : i + 8, j : j + 128]
                total = piece if total is None else total + piece
        return total

    first_row = me_row * n_chan - n_chan
    own_at = n_chan * width
    own_lanes = n_chan * width
    valid_m = iota2((16, own_lanes), 0) < half_m
    for s in range(steps_m):
        if s == 1:
            state = state[:, 4 * width : 20 * width]
            first_row = first_row + 4
            own_at = own_at - 4 * width
        length = state.shape[1]
        lane = iota2((1, length), 1)
        col, row = lax.rem(lane, width), lax.div(lane, width) + first_row
        u = apply_mix(state, mix_m[s], const_m[s])
        ua, updated, g = coupling(
            u,
            half_m,
            16,
            w1m_t.at[s],
            w2m_t.at[s],
            b2m.at[s],
            w3m.at[s],
            bias3_m[s],
            col >= 1,
            col <= width - 2,
            row >= 1,
            row <= height - 2,
            jnp.logical_and(row >= 0, row < height),
            width,
            512,
            False,
        )
        state = jnp.concatenate([ua, updated], axis=0)
        mine = g[:, own_at : own_at + own_lanes]
        if s < steps_m - 1:
            partial = partial + folded(jnp.where(valid_m, log_sigmoid(mine), 0.0))
    kept = state[16:, own_at : own_at + own_lanes]
    k_out[...] = kept.astype(BF16)
    k_copies = to_neighbours(k_out, k_in, ks_sem, kr_sem)
    partial = partial + folded(jnp.where(valid_m, log_sigmoid(mine), 0.0))
    latent = jnp.where(valid_m, state[:16, own_at : own_at + own_lanes], 0.0)
    partial = partial + folded(-0.5 * latent * latent)

    for c in range(n_chan):
        piece = latent[:, width * c : width * (c + 1)]
        back_out[c] = jnp.concatenate([piece[:8], piece[8:], jnp.zeros((8, 128 - 2 * width), F32)], axis=1)
    back_in[me_chan] = back_out[me_chan]
    back_copies = []
    for k in far:
        peer = chan_peers[k - 1]
        copy = pltpu.make_async_remote_copy(
            src_ref=back_out.at[peer],
            dst_ref=back_in.at[me_chan],
            send_sem=bs_sem.at[k - 1],
            recv_sem=br_sem.at[k - 1],
            device_id={"chan": peer},
            device_id_type=MESH,
        )
        copy.start()
        back_copies.append(copy)

    cols_p = width // 2
    lane = iota2((16, 128), 1)
    phase, rest = lax.div(lane, 32), lax.rem(lane, 32)
    pick = (2 * lax.div(rest, cols_p) + lax.div(phase, 2)) * width + 2 * lax.rem(rest, cols_p) + lax.rem(phase, 2)
    pl.semaphore_wait(token_sem.at[1], rows_off(2))
    tell_rows(token_sem.at[2], 4)
    from_neighbours(k_copies)
    zero = jnp.zeros_like(kept)
    kept = jnp.concatenate(
        [
            jnp.where(has_row(-1), k_in[0].astype(F32), zero),
            kept,
            jnp.where(has_row(1), k_in[1].astype(F32), zero),
        ],
        axis=1,
    )
    blocks = [
        jnp.take_along_axis(kept[:, 128 * k : 128 * k + 128], pick, axis=1) for k in range(kept.shape[1] // 128)
    ]
    phases = []
    for p in range(4):
        parts = [b[:, 32 * p : 32 * p + 32] for b in blocks]
        parts.append(jnp.zeros((16, 256 - 32 * len(blocks)), F32))
        phases.append(jnp.concatenate(parts, axis=1))
    state = jnp.concatenate(phases, axis=0)

    rows_p = n_chan // 2
    first_row = me_row * rows_p - rows_p
    own_at = rows_p * cols_p
    for s in range(steps_p):
        if s == steps_p - 1:
            state = pltpu.roll(state, state.shape[1] - 2 * cols_p, 1)[:, :128]
            first_row, own_at = first_row + 2, own_at - 2 * cols_p
        lane = iota2((1, state.shape[1]), 1)
        col, row = lax.rem(lane, cols_p), lax.div(lane, cols_p) + first_row
        mine_p = jnp.logical_and(lane >= own_at, lane < own_at + rows_p * cols_p)
        u = apply_mix(state, mix_p0[...] if s == 0 else mix_p1[s - 1], const_p[s])
        ua, updated, g = coupling(
            u,
            half_p,
            half_p,
            w1p_t.at[s],
            w2p_t.at[s],
            b2p.at[s],
            w3p.at[s],
            bias3_p[s],
            col >= 1,
            col <= cols_p - 2,
            row >= 1,
            row <= height // 2 - 2,
            jnp.logical_and(row >= 0, row < height // 2),
            cols_p,
            256,
            True,
        )
        state = jnp.concatenate([ua, updated], axis=0)
        partial = partial + folded(jnp.where(mine_p, log_sigmoid(g), 0.0))
    partial = partial + folded(jnp.where(mine_p, -0.5 * state * state, 0.0))
    ll_out[...] = jnp.sum(partial, axis=0, keepdims=True)
    pl.semaphore_wait(token_sem.at[2], rows_off(4))
    row_peers = [lax.rem(me_row + k, n_rows) for k in range(1, n_rows)]
    far_rows = sorted(range(1, n_rows), key=lambda k: -min(k, n_rows - k))
    ll_copies = []
    for k in far_rows:
        peer = row_peers[k - 1]
        copy = pltpu.make_async_remote_copy(
            src_ref=ll_out,
            dst_ref=ll_in.at[n_rows - 1 - k],
            send_sem=ls_sem.at[k - 1],
            recv_sem=lr_sem.at[n_rows - 1 - k],
            device_id={"rows": peer},
            device_id_type=MESH,
        )
        copy.start()
        ll_copies.append(copy)

    latent_top[...] = state.T[own_at : own_at + rows_p * cols_p]
    for copy in back_copies:
        copy.wait_recv()
    for c in range(n_img):
        piece = back_in[c]
        latent_mid[half_m * c : half_m * c + 8] = piece[:, :width]
        latent_mid[half_m * c + 8 : half_m * (c + 1)] = piece[: half_m - 8, width : 2 * width]
    cells = height * width
    const = sum(
        (
            cells * (jnp.sum(gain_mid[...]) + jnp.sum(diag_mid[...])),
            (cells // 4) * (jnp.sum(gain_top[...]) + jnp.sum(diag_top[...])),
        )
    )
    for copy in (*y_copies, *back_copies, *ll_copies):
        copy.wait_send()
    for copies, there in z_copies:

        @pl.when(there)
        def _():
            for copy in copies:
                copy.wait_send()

    for copy, d in k_copies:
        pl.when(has_row(d))(copy.wait_send)
    for copy in ll_copies:
        copy.wait_recv()
    total = ll_out[...]
    for k in range(n_rows - 1):
        total = total + ll_in[k]
    scale = 1.0 / (c_mid * cells)
    loglik[...] = jnp.broadcast_to((jnp.sum(total) + const) * scale - 0.5 * log_two_pi, (1, 128))


def write_out(*refs):
    sem = refs[-1]
    copies = [pltpu.make_async_copy(refs[k], refs[3 + k], sem.at[k]) for k in range(3)]
    for copy in copies:
        copy.start()
    for copy in copies:
        copy.wait()


def body(
    images,
    shift_mid,
    gain_mid,
    lower_mid,
    upper_mid,
    diag_mid,
    first_mid,
    first_bias_mid,
    second_mid,
    second_bias_mid,
    third_mid,
    third_bias_mid,
    shift_top,
    gain_top,
    lower_top,
    upper_top,
    diag_top,
    first_top,
    first_bias_top,
    second_top,
    second_bias_top,
    third_top,
    third_bias_top,
):
    n_rows, n_chan = lax.axis_size("rows"), lax.axis_size("chan")
    n_img, c_mid, _, width = images.shape
    hid = second_mid.shape[1]
    steps_m, steps_p = shift_mid.shape[0], shift_top.shape[0]
    c_top = shift_top.shape[1]
    half_m, half_p = c_mid // 2, c_top // 2
    images = images.reshape(n_img, c_mid, width)
    third_mid = third_mid.transpose(0, 1, 3, 2).reshape(steps_m, 9 * c_mid, hid)
    third_top = third_top.transpose(0, 1, 3, 2).reshape(steps_p, 9 * c_top, hid)
    first_top = first_top.reshape(steps_p, 9 * half_p, hid)
    big = pl.BlockSpec(memory_space=pltpu.HBM)
    small = pl.BlockSpec(memory_space=pltpu.VMEM)
    rows_p = n_chan // 2
    vmem = pltpu.VMEM
    small_args = (shift_mid, gain_mid, lower_mid, upper_mid, diag_mid, first_bias_mid, second_bias_mid, third_bias_mid, shift_top, gain_top, lower_top, upper_top, diag_top, first_bias_top, second_bias_top, third_bias_top)
    dma = pltpu.SemaphoreType.DMA
    found = pl.pallas_call(
        functools.partial(kernel, n_rows, n_chan),
        out_shape=(
            vmem((n_img * half_m, width), F32),
            vmem((rows_p * width // 2, c_top), F32),
            vmem((1, 128), F32),
        ),
        in_specs=[big] * 23,
        out_specs=(small, small, small),
        scratch_shapes=[
            vmem((n_img, c_mid, width), F32),
            vmem((steps_m, 9, half_m, hid), BF16),
            vmem((steps_m, hid, hid), BF16),
            vmem((steps_m, 9 * c_mid, hid), BF16),
            vmem((steps_p, 9 * half_p, hid), BF16),
            vmem((steps_p, hid, hid), BF16),
            vmem((steps_p, 9 * c_top, hid), BF16),
            vmem((144, hid), F32),
            vmem((9 * half_p + 8, hid), F32),
            vmem((steps_m, hid, 144), BF16),
            vmem((steps_m, hid, hid), BF16),
            vmem((steps_p, hid, 9 * half_p + 8), BF16),
            vmem((steps_p, hid, hid), BF16),
            vmem((steps_m, hid, 128), F32),
            vmem((steps_p, hid, 128), F32),
            vmem((steps_m, 32, 96), BF16),
            vmem((c_top, 192), BF16),
            vmem((steps_p - 1, c_top, 144), BF16),
            vmem((steps_m, 32, 1), F32),
            vmem((steps_p, c_top, 1), F32),
            vmem((n_chan, 8, 128), F32),
            vmem((n_chan, 8, 128), BF16),
            vmem((n_chan, 8, 128), F32),
            vmem((2, n_chan, 8, 128), BF16),
            vmem((16, n_chan * width), BF16),
            vmem((2, 16, n_chan * width), BF16),
            vmem((n_chan, 8, 128), F32),
            vmem((n_chan, 8, 128), F32),
            vmem((1, 128), F32),
            vmem((n_rows - 1, 1, 128), F32),
            *(vmem(a.shape, a.dtype) for a in small_args),
            dma((6,)),
            dma(()),
            dma((len(small_args),)),
            dma((n_chan - 1,)),
            dma((n_chan - 1,)),
            dma((2, n_chan)),
            dma((2, n_chan)),
            dma((2,)),
            dma((2,)),
            dma((n_chan - 1,)),
            dma((n_chan - 1,)),
            dma((n_rows - 1,)),
            dma((n_rows - 1,)),
            pltpu.SemaphoreType.REGULAR((3,)),
        ],
        compiler_params=pltpu.CompilerParams(
            collective_id=0, has_side_effects=True, vmem_limit_bytes=67043328 - 100 * 1024
        ),
    )(
        images,
        shift_mid,
        gain_mid,
        lower_mid,
        upper_mid,
        diag_mid,
        first_mid,
        first_bias_mid,
        second_mid,
        second_bias_mid,
        third_mid,
        third_bias_mid,
        shift_top,
        gain_top,
        lower_top,
        upper_top,
        diag_top,
        first_top,
        first_bias_top,
        second_top,
        second_bias_top,
        third_top,
        third_bias_top,
    )
    latent_mid, latent_top, loglik = pl.pallas_call(
        write_out,
        out_shape=tuple(jax.ShapeDtypeStruct(x.shape, x.dtype) for x in found),
        in_specs=[small] * 3,
        out_specs=(pl.BlockSpec(memory_space=pltpu.HBM),) * 3,
        scratch_shapes=[dma((3,))],
        compiler_params=pltpu.CompilerParams(vmem_limit_bytes=1024 * 1024),
    )(*found)
    latent_mid = latent_mid.reshape(n_img, half_m, 1, width)
    latent_top = latent_top.reshape(1, rows_p, width // 2, c_top).transpose(0, 3, 1, 2)
    return latent_mid, latent_top, loglik[0, :1]


def solution(mesh):
    placed = (P("batch", None, ("rows", "chan"), None),) + (P(),) * 22
    return jax.shard_map(
        body,
        mesh=mesh,
        in_specs=placed,
        out_specs=(
            P("batch", None, ("rows", "chan"), None),
            P(("batch", "chan"), None, "rows", None),
            P(("batch", "chan")),
        ),
        check_vma=False,
    )
```
